32 devices in a mesh: client: 4 (over z), tensor: 4 (over x, core), sdata: 2 (over y).
Axes of the slice: x: 2, y: 2, z: 4, core: 2. Of those that a mesh axis runs over, the one named last changes fastest.
Arguments:
- client_input: bfloat16 [3072, 2048], P(('client', 'sdata')), may hold values from -6 to 6
- client_gain: bfloat16 [4, 2048], P('client'), may hold values from 0.5 to 1.5
- query_weight: bfloat16 [4, 2048, 2048], P('client', None, 'tensor'), as said below
- key_weight: bfloat16 [4, 2048, 512], P('client', None, 'tensor'), as said below
- client_value_weight: bfloat16 [4, 2048, 512], P('client', None, 'tensor'), may hold values from -0.125 to 0.125
- output_weight: bfloat16 [4, 2048, 2048], P('client', None, 'tensor'), may hold values from -0.125 to 0.125
- server_gain: bfloat16 [2, 2048], P('sdata'), may hold values from 0.5 to 1.5
- server_gate: bfloat16 [2, 2048, 4096], P('sdata', None, 'tensor'), may hold values from -0.125 to 0.125
- server_up: bfloat16 [2, 2048, 4096], P('sdata', None, 'tensor'), may hold values from -0.125 to 0.125
- server_down: bfloat16 [2, 4096, 2048], P('sdata', 'tensor'), may hold values from -0.09375 to 0.09375
- upstream: bfloat16 [3072, 2048], P(('client', 'sdata')), may hold values from -6 to 6
- assignment: int32 [4], replicated, may hold values from 0 to 1, as said below
Outputs:
- query_update: bfloat16 [2048, 2048], P(('client', 'sdata'), 'tensor')
- key_update: bfloat16 [2048, 512], P(('client', 'sdata'), 'tensor')
- value_update: bfloat16 [2048, 512], P(('client', 'sdata'), 'tensor')
- output_update: bfloat16 [2048, 2048], P(('client', 'sdata'), 'tensor')
The draws below stay inside these ranges and needn't reach their ends.
Inputs may be any that keep to these rules, and one draw needn't show every extreme that they name: `assignment`: each of the 2 server groups is named by exactly 2 clients. `query_weight`: independent entries with a spread of about 2048 ** -0.5. `key_weight`: entries with a spread of about 2048 ** -0.5 or more.
All inputs are finite; a program needn't handle non-finite values.
Results may differ from the reference program's by a relative error of at most 0.038.
The reference program's roundings to bfloat16 on the way count: a program that leaves them out, or rounds other values in their place, can miss the bound.
Values may be sent and summed in bfloat16 or wider, within the bound.
A program may use at most 128 MiB of HBM per device.

```python
import math
import jax
import jax.numpy as jnp
from jax import lax

MODEL_WIDTH = 2048
HEAD_DIM = 64
FF = 4096
LEN = 384
CLIENT_TOTAL = 4
GROUPS = 2
TOKENS = 3072
QUERY_FEATURES = 2048
KEY_FEATURES = 512


def weights_pair(key):
    scaling_factor = MODEL_WIDTH ** (-0.5)
    query_matrix = jnp.clip(jax.random.normal(jax.random.fold_in(key, 11), (CLIENT_TOTAL, MODEL_WIDTH, QUERY_FEATURES), jnp.float32), -4.0, 4.0) * scaling_factor
    client_key_matrix = jnp.clip(jax.random.normal(jax.random.fold_in(key, 12), (CLIENT_TOTAL, MODEL_WIDTH, KEY_FEATURES), jnp.float32), -4.0, 4.0) * scaling_factor
    return (query_matrix, client_key_matrix)


def draw_query_weight(key, part):
    return weights_pair(key)[0].astype(jnp.bfloat16)


def draw_key_weight(key, part):
    return weights_pair(key)[1].astype(jnp.bfloat16)


def draw_assignment(key, part):
    scores = jax.random.randint(jax.random.fold_in(key, 4099), (CLIENT_TOTAL,), 0, 1 << 20) * CLIENT_TOTAL + jnp.arange(CLIENT_TOTAL)
    order = jnp.argsort(scores, stable=True)
    return (order % GROUPS).astype(jnp.int32)


def strengthened(entries, own_key, source, target, shards_of, factor):
    def block_of(axis_at):
        return (jnp.arange(entries.shape[axis_at]) // (entries.shape[axis_at] // shards_of)).reshape((-1,) + (1,) * (entries.ndim - 1 - axis_at))

    near = jax.random.permutation(own_key, shards_of)[block_of(target)]
    far = (block_of(target) + shards_of // 2) % shards_of
    return jnp.where((block_of(source) == near) | (block_of(source) == far), factor * entries, entries)


def level_of(key, shape, pieces, least, largest):
    def one(dim, parts):
        steps = jax.random.uniform(jax.random.fold_in(jax.random.fold_in(key, 6), dim), (parts,), jnp.float32, least / len(pieces), largest / len(pieces))
        return jnp.repeat(jnp.exp(steps), shape[dim] // parts).reshape((-1,) + (1,) * (len(shape) - dim - 1))

    level = one(*pieces[0])
    for cut in pieces[1:]:
        level = level * one(*cut)
    return level


def noise(rng, shape, deviation, most, pieces=(), kind=jnp.bfloat16):
    array = jax.random.normal(rng, shape, jnp.float32) * deviation
    if len(pieces) > 0:
        array = level_of(rng, shape, pieces, -0.22, 0.18) * array
    return jnp.clip(array, min=-most, max=most).astype(kind)


def noise_with(stream_key, shape, scale, limit, pieces, heavy, held_as=jnp.bfloat16):
    array = scale * jax.random.normal(stream_key, shape, jnp.float32)
    if pieces:
        array = array * level_of(stream_key, shape, pieces, -0.22, 0.18)
    return jnp.clip(strengthened(array, jax.random.fold_in(stream_key, 3), *heavy), -limit, limit).astype(held_as)


def setup_inputs(seed: int = 0) -> dict:
    streams_of = jax.random.split(jax.random.key(seed), 13)
    return {
        "client_input": noise_with(streams_of[0], (TOKENS, MODEL_WIDTH), 1.0, 6.0, ((0, 8),), (0, 1, 8, 2.0)),
        "client_gain": jnp.clip(1.0 + 0.1 * jax.random.normal(streams_of[1], (CLIENT_TOTAL, MODEL_WIDTH), jnp.float32), 0.5, 1.5).astype(jnp.bfloat16),
        "query_weight": draw_query_weight(jax.random.fold_in(streams_of[12], 71), 0),
        "key_weight": draw_key_weight(jax.random.fold_in(streams_of[12], 71), 0),
        "client_value_weight": noise(streams_of[4], (CLIENT_TOTAL, MODEL_WIDTH, KEY_FEATURES), MODEL_WIDTH ** -0.5, 0.125, ((0, 4), (2, 4))),
        "output_weight": noise(streams_of[5], (CLIENT_TOTAL, MODEL_WIDTH, QUERY_FEATURES), QUERY_FEATURES ** -0.5, 0.125, ((0, 4), (2, 4))),
        "server_gain": jnp.clip(1.0 + 0.1 * jax.random.normal(streams_of[6], (GROUPS, MODEL_WIDTH), jnp.float32), 0.5, 1.5).astype(jnp.bfloat16),
        "server_gate": noise(streams_of[7], (GROUPS, MODEL_WIDTH, FF), MODEL_WIDTH ** -0.5, 0.125, ((0, 2), (2, 4))),
        "server_up": noise(streams_of[8], (GROUPS, MODEL_WIDTH, FF), MODEL_WIDTH ** -0.5, 0.125, ((0, 2), (2, 4))),
        "server_down": noise(streams_of[9], (GROUPS, FF, MODEL_WIDTH), FF ** -0.5, 0.09375, ((0, 2), (1, 4))),
        "upstream": noise(streams_of[10], (TOKENS, MODEL_WIDTH), 1.0, 6.0, ((0, 8),)),
        "assignment": draw_assignment(jax.random.fold_in(streams_of[12], 71), 0),
    }


def rotary_tables(length):
    halfway = HEAD_DIM // 2
    positions = jnp.arange(length).astype(jnp.float32)
    exponents = jnp.arange(halfway).astype(jnp.float32) * (2.0 / HEAD_DIM)
    frequencies = jnp.exp(-math.log(500000.0) * exponents)
    angles = positions[:, None] * frequencies[None, :]
    cosine_table = jnp.concatenate([jnp.cos(angles), jnp.cos(angles)], 1)
    sine_table = jnp.concatenate([jnp.sin(angles), jnp.sin(angles)], 1)
    return (cosine_table, sine_table)

def rotary(heads_in, cosine_table, sine_table):
    halfway = heads_in.shape[-1] // 2
    turned = jnp.concatenate([-heads_in[..., halfway:], heads_in[..., :halfway]], -1)
    return heads_in * cosine_table[:, None, :] + turned * sine_table[:, None, :]

def normalize(rows_in, gain):
    rows_float = rows_in.astype(jnp.float32)
    inv_rms = lax.rsqrt(lax.optimization_barrier(jnp.mean(rows_float * rows_float, -1, keepdims=True)) + 1e-05)
    return (rows_float * inv_rms * gain.astype(jnp.float32)).astype(jnp.bfloat16)

def attention_part(normed, query_matrix, client_key_matrix, value_matrix, output_matrix):
    length = normed.shape[0]
    query_count = query_matrix.shape[1] // HEAD_DIM
    shared_count = client_key_matrix.shape[1] // HEAD_DIM
    group_size = query_count // shared_count
    cosine_table, sine_table = rotary_tables(length)
    queries = jnp.dot(normed, query_matrix, preferred_element_type=jnp.float32).reshape(length, query_count, HEAD_DIM)
    queries = rotary(queries, cosine_table, sine_table).astype(jnp.bfloat16).reshape(length, shared_count, group_size, HEAD_DIM)
    key_heads = jnp.dot(normed, client_key_matrix, preferred_element_type=jnp.float32).reshape(length, shared_count, HEAD_DIM)
    key_heads = rotary(key_heads, cosine_table, sine_table).astype(jnp.bfloat16)
    value_heads = jnp.dot(normed, value_matrix, preferred_element_type=jnp.float32).astype(jnp.bfloat16).reshape(length, shared_count, HEAD_DIM)
    scores = jnp.einsum('qgrd,kgd->grqk', queries.astype(jnp.float32), key_heads.astype(jnp.float32)) * HEAD_DIM ** (-0.5)
    row_ids = lax.broadcasted_iota(jnp.int32, (length, length), 0)
    col_ids = lax.broadcasted_iota(jnp.int32, (length, length), 1)
    scores = jnp.where(col_ids <= row_ids, scores, -1e+30)
    highest = lax.stop_gradient(lax.optimization_barrier(jnp.max(scores, -1, keepdims=True)))
    exponent = jnp.exp(scores - highest)
    weights = (exponent / lax.optimization_barrier(jnp.sum(exponent, -1, keepdims=True))).astype(jnp.bfloat16)
    context = jnp.einsum('grqk,kgd->qgrd', weights.astype(jnp.float32), value_heads.astype(jnp.float32))
    context = context.astype(jnp.bfloat16).reshape(length, query_count * HEAD_DIM)
    return lax.dot_general(context, output_matrix, (((1,), (1,)), ((), ())), preferred_element_type=jnp.float32)

def server_pull(rows_in, upstream_rows, gain, gate_matrix, up_matrix, down_matrix):
    rows_float = rows_in.astype(jnp.float32)
    inv_rms = lax.rsqrt(lax.optimization_barrier(jnp.mean(rows_float * rows_float, -1, keepdims=True)) + 1e-05)
    gain_float = gain.astype(jnp.float32)
    server_normed = (rows_float * inv_rms * gain_float).astype(jnp.bfloat16)
    gate_value = jnp.dot(server_normed, gate_matrix, preferred_element_type=jnp.float32)
    up_value = jnp.dot(server_normed, up_matrix, preferred_element_type=jnp.float32)
    pulled = lax.dot_general(upstream_rows, down_matrix, (((1,), (1,)), ((), ())), preferred_element_type=jnp.float32)
    sigmoid_gate = jax.nn.sigmoid(gate_value)
    gate_grad = (pulled * up_value * sigmoid_gate * (1.0 + gate_value * (1.0 - sigmoid_gate))).astype(jnp.bfloat16)
    up_grad = (pulled * gate_value * sigmoid_gate).astype(jnp.bfloat16)
    normed_grad = lax.dot_general(gate_grad, gate_matrix, (((1,), (1,)), ((), ())), preferred_element_type=jnp.float32)
    normed_grad = normed_grad + lax.dot_general(up_grad, up_matrix, (((1,), (1,)), ((), ())), preferred_element_type=jnp.float32)
    weighted = normed_grad * gain_float
    return inv_rms * weighted - rows_float * inv_rms ** 3 * lax.optimization_barrier(jnp.mean(weighted * rows_float, -1, keepdims=True))

def reference(client_input, client_gain, query_weight, key_weight, client_value_weight, output_weight, server_gain, server_gate, server_up, server_down, upstream, assignment):
    sequences = client_input.reshape(CLIENT_TOTAL * GROUPS, LEN, MODEL_WIDTH)
    upstream_seqs = upstream.reshape(CLIENT_TOTAL * GROUPS, LEN, MODEL_WIDTH)

    def one_sequence(totals, index_seq):
        owner_client = index_seq // GROUPS
        group_index = assignment[owner_client]
        rows_in = sequences[index_seq]
        upstream_rows = upstream_seqs[index_seq]
        normed = normalize(rows_in, client_gain[owner_client])

        def client_part(query_matrix, client_key_matrix, value_matrix, output_matrix):
            return attention_part(normed, query_matrix, client_key_matrix, value_matrix, output_matrix)
        attended, pullback = jax.vjp(client_part, query_weight[owner_client], key_weight[owner_client], client_value_weight[owner_client], output_weight[owner_client])
        cut_input = (rows_in.astype(jnp.float32) + attended).astype(jnp.bfloat16)
        pulled = server_pull(cut_input, upstream_rows, server_gain[group_index], server_gate[group_index], server_up[group_index], server_down[group_index])
        cut_grad = (upstream_rows.astype(jnp.float32) + pulled).astype(jnp.bfloat16)
        gradients = pullback(cut_grad.astype(jnp.float32))
        updated = tuple((total + grad_item.astype(jnp.bfloat16).astype(jnp.float32) for total, grad_item in zip(totals, gradients)))
        return (updated, None)
    start_offsets = (jnp.zeros((MODEL_WIDTH, QUERY_FEATURES), jnp.float32), jnp.zeros((MODEL_WIDTH, KEY_FEATURES), jnp.float32), jnp.zeros((MODEL_WIDTH, KEY_FEATURES), jnp.float32), jnp.zeros((MODEL_WIDTH, QUERY_FEATURES), jnp.float32))
    totals, unused = lax.scan(one_sequence, start_offsets, jnp.arange(CLIENT_TOTAL * GROUPS).astype(jnp.int32))
    query_total, key_total, value_total, output_total = totals
    return ((query_total / CLIENT_TOTAL).astype(jnp.bfloat16), (key_total / CLIENT_TOTAL).astype(jnp.bfloat16), (value_total / CLIENT_TOTAL).astype(jnp.bfloat16), (output_total / CLIENT_TOTAL).astype(jnp.bfloat16))
```

```python
from functools import partial
import math

import jax
import jax.numpy as jnp
from jax import lax
from jax.experimental import pallas as pl
from jax.experimental.pallas import tpu as pltpu
from jax.sharding import PartitionSpec as P

HEAD_DIM = 64
MESH = pl.DeviceIdType.MESH
CORES = 2
LANES = 128
BF16 = jnp.bfloat16
F32 = jnp.float32


def lane_tile(flag_ref=None):
    return lax.broadcasted_iota(jnp.int32, (1, LANES), 1)


def swap_halves(tile):
    low = lax.rem(lane_tile(), HEAD_DIM) < HEAD_DIM // 2
    ahead = pltpu.roll(tile, LANES - HEAD_DIM // 2, 1)
    behind = pltpu.roll(tile, HEAD_DIM // 2, 1)
    return jnp.where(low, ahead, behind)


def paired(tile, at):
    low = lane_tile() < HEAD_DIM
    moved = pltpu.roll(tile, HEAD_DIM, 1)
    first, second = (tile, moved) if at == 0 else (moved, tile)
    zero = jnp.zeros_like(tile)
    return jnp.where(low, first, zero).astype(BF16), jnp.where(low, zero, second).astype(BF16)


CROSSED = (((1,), (1,)), ((), ()))
TALL = (((0,), (0,)), ((), ()))


def forward_kernel(
    kv_count, sends_half,
    rows_ref, gain_ref, cosine_ref, sine_ref, query_hbm, key_hbm, value_hbm, output_hbm,
    normed_out, theirs_out, query_out, key_out, value_out, context_out, weights_out, attended_out,
    query_mat, key_mat, value_mat, output_mat, scores, key_pair, value_turn, sems,
):
    length = rows_ref.shape[0]
    copies = []
    for i, (source, target) in enumerate(
        ((query_hbm, query_mat), (key_hbm, key_mat), (value_hbm, value_mat), (output_hbm, output_mat))
    ):
        copies.append(pltpu.make_async_copy(source, target, sems.at[i]))
        copies[-1].start()
    rows_float = rows_ref[...].astype(F32)
    inv_rms = lax.rsqrt(jnp.mean(rows_float * rows_float, -1, keepdims=True) + 1e-05)
    normed_out[...] = (rows_float * inv_rms * gain_ref[...].astype(F32)).astype(BF16)
    if sends_half:
        blocks, unused, wide = theirs_out.shape
        other = 1 - lax.axis_index("sdata")
        for d in range(blocks):
            theirs_out[d] = normed_out[:, pl.ds(pl.multiple_of((2 * d + other) * wide, wide), wide)]
    normed = normed_out[...]

    def turn(tile):
        return tile * cosine_ref[...] + swap_halves(tile) * sine_ref[...]

    copies[0].wait()
    wide = 2 * LANES
    for at in range(0, query_mat.shape[1], wide):
        part = jnp.dot(normed, query_mat[:, at : at + wide], preferred_element_type=F32)
        for side in (0, LANES):
            query_out[:, at + side : at + side + LANES] = turn(part[:, side : side + LANES]).astype(BF16)
    copies[1].wait()
    keys = turn(jnp.dot(normed, key_mat[...], preferred_element_type=F32)).astype(BF16)
    key_out[...] = keys
    copies[2].wait()
    values = jnp.dot(normed, value_mat[...], preferred_element_type=F32).astype(BF16)
    value_out[...] = values
    keys_float, values_float = keys.astype(F32), values.astype(F32)
    values_turned = values_float.T.astype(BF16)
    value_turn[...] = jnp.zeros_like(value_turn)
    for g in range(kv_count):
        key_pair[g, :length], key_pair[g, length:] = paired(keys_float, g)
        mine = values_turned[g * HEAD_DIM : (g + 1) * HEAD_DIM]
        value_turn[g, :HEAD_DIM, :length] = mine
        value_turn[g, HEAD_DIM:, length:] = mine
    tiles = query_mat.shape[1] // LANES
    step = LANES
    for t in range(tiles):
        g = t * kv_count // tiles
        scores[...] = lax.dot_general(
            key_pair[g], query_out[:, t * LANES : (t + 1) * LANES], CROSSED, preferred_element_type=F32
        )
        for head in range(2):
            base = head * length
            for i in range(0, length, step):
                deep = i + step
                block = scores[base : base + deep, i : i + step] * HEAD_DIM ** (-0.5)
                key_ids = lax.broadcasted_iota(jnp.int32, (deep, step), 0)
                query_ids = lax.broadcasted_iota(jnp.int32, (deep, step), 1) + i
                block = jnp.where(key_ids <= query_ids, block, -1e30)
                exponent = jnp.exp(block - jnp.max(block, 0, keepdims=True))
                share = 1.0 / jnp.sum(exponent, 0, keepdims=True)
                weights_out[t, base : base + deep, i : i + step] = (exponent * share).astype(BF16)
                if deep < length:
                    weights_out[t, base + deep : base + length, i : i + step] = jnp.zeros(
                        (length - deep, step), BF16
                    )
        turned_context = jnp.dot(value_turn[g], weights_out[t], preferred_element_type=F32)
        context_out[:, t * LANES : (t + 1) * LANES] = turned_context.T.astype(BF16)
    copies[3].wait()
    context = context_out[...]
    wide = next(b for b in (512, 256, 128) if attended_out.shape[1] % b == 0)
    for at in range(0, attended_out.shape[1], wide):
        attended_out[:, at : at + wide] = lax.dot_general(
            context, output_mat[at : at + wide, :], CROSSED, preferred_element_type=F32
        ).astype(BF16)


def forward(rows_in, gain, tables, matrices, kv_count, blocks):
    length, breadth = rows_in.shape
    features, shared = matrices[0].shape[1], matrices[1].shape[1]
    tiles = features // LANES
    rows = breadth // (2 * blocks)
    sends_half = rows % LANES == 0
    shape = lambda *sizes: jax.ShapeDtypeStruct(sizes, BF16)
    theirs = shape(blocks, length, rows) if sends_half else shape(16, LANES)
    return pl.pallas_call(
        partial(forward_kernel, kv_count, sends_half),
        out_shape=(
            shape(length, breadth), theirs, shape(length, features), shape(length, shared),
            shape(length, shared), shape(length, features), shape(tiles, 2 * length, length),
            shape(length, breadth),
        ),
        in_specs=[VMEM_SPEC] * 4 + [ANY_SPEC] * 4,
        out_specs=(VMEM_SPEC,) * 8,
        scratch_shapes=[pltpu.VMEM(m.shape, BF16) for m in matrices]
        + [
            pltpu.VMEM((2 * length, length), F32),
            pltpu.VMEM((kv_count, 2 * length, LANES), BF16),
            pltpu.VMEM((kv_count, LANES, 2 * length), BF16),
            pltpu.SemaphoreType.DMA((4,)),
        ],
        compiler_params=pltpu.CompilerParams(vmem_limit_bytes=48 * 2**20),
        name="forward",
    )(rows_in, gain, *tables, *matrices)


def server_kernel(
    rows_ref, upstream_ref, gain_ref, gate_ref, up_ref, down_ref, out_ref, normed_ref, total_ref
):
    step = pl.program_id(0)

    def inverse_rms(rows_float):
        return lax.rsqrt(jnp.mean(rows_float * rows_float, -1, keepdims=True) + 1e-05)

    @pl.when(step == 0)
    def _():
        rows_float = rows_ref[...].astype(F32)
        normed_ref[...] = (
            rows_float * inverse_rms(rows_float) * gain_ref[...].astype(F32)
        ).astype(BF16)

    gate, up = gate_ref[...], up_ref[...]
    crossed = (((1,), (1,)), ((), ()))
    gate_value = jnp.dot(normed_ref[...], gate, preferred_element_type=F32)
    up_value = jnp.dot(normed_ref[...], up, preferred_element_type=F32)
    pulled = lax.dot_general(
        upstream_ref[...], down_ref[...], crossed, preferred_element_type=F32
    )
    sigmoid_gate = jax.nn.sigmoid(gate_value)
    gate_grad = (
        pulled * up_value * sigmoid_gate * (1.0 + gate_value * (1.0 - sigmoid_gate))
    ).astype(BF16)
    up_grad = (pulled * gate_value * sigmoid_gate).astype(BF16)
    normed_grad = lax.dot_general(
        gate_grad, gate, crossed, preferred_element_type=F32
    ) + lax.dot_general(up_grad, up, crossed, preferred_element_type=F32)

    @pl.when(step == 0)
    def _():
        total_ref[...] = normed_grad

    @pl.when(step > 0)
    def _():
        total_ref[...] += normed_grad

    @pl.when(step == pl.num_programs(0) - 1)
    def _():
        rows_float = rows_ref[...].astype(F32)
        inv_rms = inverse_rms(rows_float)
        weighted = total_ref[...] * gain_ref[...].astype(F32)
        out_ref[...] = (
            inv_rms * weighted
            - rows_float * inv_rms**3 * jnp.mean(weighted * rows_float, -1, keepdims=True)
        ).astype(BF16)


def server_pull(rows_in, upstream_rows, gain, gate_matrix, up_matrix, down_matrix):
    length, breadth = rows_in.shape
    hidden = gate_matrix.shape[1]
    block = next(b for b in (256, 128, hidden) if hidden % b == 0)
    whole = pl.BlockSpec((length, breadth), lambda i: (0, 0))
    tall = pl.BlockSpec((breadth, block), lambda i: (0, i))
    return pl.pallas_call(
        server_kernel,
        grid=(hidden // block,),
        out_shape=jax.ShapeDtypeStruct((length, breadth), BF16),
        in_specs=[
            whole,
            whole,
            pl.BlockSpec((1, breadth), lambda i: (0, 0)),
            tall,
            tall,
            pl.BlockSpec((block, breadth), lambda i: (i, 0)),
        ],
        out_specs=whole,
        scratch_shapes=[pltpu.VMEM((length, breadth), BF16), pltpu.VMEM((length, breadth), F32)],
        compiler_params=pltpu.CompilerParams(vmem_limit_bytes=48 * 2**20),
        name="server_pull",
    )(rows_in, upstream_rows, gain[None], gate_matrix, up_matrix, down_matrix)


def greet(others):
    barrier = pltpu.get_barrier_semaphore()
    for other in others:
        pl.semaphore_signal(barrier, inc=1, device_id=other, device_id_type=MESH)
    pl.semaphore_wait(barrier, len(others))


def send(source, target, send_sem, recv_sem, device):
    copy = pltpu.make_async_remote_copy(
        src_ref=source,
        dst_ref=target,
        send_sem=send_sem,
        recv_sem=recv_sem,
        device_id=device,
        device_id_type=MESH,
    )
    copy.start()
    return copy


def place():
    tensor_at = lax.axis_index("tensor")
    return tensor_at // CORES, lax.rem(tensor_at, CORES)


def turned(index, step, count):
    return lax.rem(index + step, count)


def columns_of(chip, core, width):
    return pl.ds(pl.multiple_of((chip * CORES + core) * width, width), width)


def partners(chips, client_count, group_count):
    chip, core = place()
    client, group = lax.axis_index("client"), lax.axis_index("sdata")
    others = [{"tensor": chip * CORES + 1 - core}]
    others += [{"tensor": turned(chip, k, chips) * CORES + core} for k in range(1, chips)]
    others += [{"client": turned(client, k, client_count)} for k in range(1, client_count)]
    others += [{"sdata": turned(group, k, group_count)} for k in range(1, group_count)]
    return others


class ShareSum:
    def __init__(self, part, pair, relay, landed, sems, chunks, chips):
        self.part, self.pair, self.relay, self.landed = part, pair, relay, landed
        self.pair_send, self.pair_recv, self.chip_send, self.chip_recv = sems
        self.chips, self.width = chips, part.shape[-1] // (CORES * chips)
        self.chip, self.core = place()
        self.copies = []
        self.pair_copies = {}
        self.chip_copies = {}
        for n, q in enumerate(chunks):
            for k in list(range(1, chips)) + [0]:
                to = turned(self.chip, k, chips)
                copy = send(
                    part.at[q, :, columns_of(to, 1 - self.core, self.width)],
                    pair.at[k, q],
                    self.pair_send.at[k, n],
                    self.pair_recv.at[k, n],
                    {"tensor": self.chip * CORES + 1 - self.core},
                )
                self.pair_copies[k, n] = copy
        for n, q in enumerate(chunks):
            for k in range(1, chips):
                to = turned(self.chip, k, chips)
                self.pair_copies[k, n].wait_recv()
                relay[k, q] = (
                    part[q, :, columns_of(to, self.core, self.width)].astype(F32)
                    + pair[k, q].astype(F32)
                ).astype(BF16)
                self.chip_copies[k, n] = send(
                    relay.at[k, q],
                    landed.at[k, q],
                    self.chip_send.at[k, n],
                    self.chip_recv.at[k, n],
                    {"tensor": to * CORES + self.core},
                )

    def get(self, n, q):
        self.pair_copies[0, n].wait_recv()
        total = self.part[q, :, columns_of(self.chip, self.core, self.width)].astype(
            F32
        ) + self.pair[0, q].astype(F32)
        for k in range(1, self.chips):
            self.chip_copies[k, n].wait_recv()
            total = total + self.landed[k, q].astype(F32)
        return total

    def finish(self):
        for copy in list(self.pair_copies.values()) + list(self.chip_copies.values()):
            copy.wait_send()


class Widen:
    def __init__(self, out, sems, chips):
        self.out, self.chips = out, chips
        self.chip_send, self.chip_recv, self.pair_send, self.pair_recv = sems
        self.chip, self.core = place()
        self.width = out.shape[-1] // (CORES * chips)
        self.started, self.forwarded, self.chip_copies = [], [], {}

    def pair_copy(self, source, k, n, q):
        cols = columns_of(turned(self.chip, self.chips - k, self.chips), self.core, self.width)
        self.forwarded.append(
            send(
                source,
                self.out.at[q, :, cols],
                self.pair_send.at[k, n],
                self.pair_recv.at[k, n],
                {"tensor": self.chip * CORES + 1 - self.core},
            )
        )

    def start(self, source, n, q):
        cols = columns_of(self.chip, self.core, self.width)
        for k in range(1, self.chips):
            self.chip_copies[k, n] = send(
                source,
                self.out.at[q, :, cols],
                self.chip_send.at[k, n],
                self.chip_recv.at[k, n],
                {"tensor": turned(self.chip, k, self.chips) * CORES + self.core},
            )
        self.pair_copy(source, 0, n, q)
        self.out[q, :, cols] = source[...]

    def forward(self, n, q):
        for k in range(1, self.chips):
            self.chip_copies[k, n].wait_recv()
            cols = columns_of(turned(self.chip, self.chips - k, self.chips), self.core, self.width)
            self.pair_copy(self.out.at[q, :, cols], k, n, q)

    def finish(self):
        for copy in self.forwarded:
            copy.wait_recv()
        for copy in self.forwarded + list(self.chip_copies.values()):
            copy.wait_send()


def out_kernel(
    chips, client_count, group_count,
    order, part, inputs, upstream,
    cut_out, up_out, up_own,
    pair, relay, landed, cut_from, cut_at, up_at, cut_put, up_put, cut_own,
    tp_sems, z_sems, y_sems, wide_sems,
):
    client, group = lax.axis_index("client"), lax.axis_index("sdata")
    chip, core = place()
    share = client_count // group_count
    width = part.shape[-1] // (CORES * chips)
    cols = columns_of(chip, core, width)
    greet(partners(chips, client_count, group_count))
    steps = list(range(1, client_count)) + [0]
    targets = [turned(client, k, client_count) for k in steps]
    up_z = []
    sums = ShareSum(part, pair, relay, landed, [tp_sems.at[i] for i in range(4)], targets, chips)
    for k in range(1, client_count):
        to = turned(client, k, client_count)
        up_z.append(
            send(
                upstream.at[to, :, cols], up_at.at[client],
                z_sems.at[0, k], z_sems.at[1, k], {"client": to},
            )
        )
    up_at[client] = upstream[client, :, cols]
    cut_z = []
    for n, (k, to) in enumerate(zip(steps, targets)):
        block = (sums.get(n, to) + inputs[to, :, cols].astype(F32)).astype(BF16)
        if k == 0:
            cut_at[client] = block
        else:
            cut_from[k] = block
            cut_z.append(
                send(
                    cut_from.at[k], cut_at.at[client],
                    z_sems.at[2, k], z_sems.at[3, k], {"client": to},
                )
            )
    widens = [
        Widen(up_out, [wide_sems.at[i] for i in range(4)], chips),
        Widen(cut_out, [wide_sems.at[i] for i in range(4, 8)], chips),
    ]
    rounds = []
    for which, (z_copies, at, put, own) in enumerate(
        ((up_z, up_at, up_put, up_own), (cut_z, cut_at, cut_put, cut_own))
    ):
        for copy in z_copies:
            copy.wait_recv()
        y_copies = []
        for d in range(1, group_count):
            to = turned(group, d, group_count)
            for i in range(share):
                put[d, i] = at[order[to * share + i]]
                y_copies.append(
                    (
                        send(
                            put.at[d, i], own.at[group * share + i],
                            y_sems.at[2 * which, d, i], y_sems.at[2 * which + 1, d, i],
                            {"sdata": to},
                        ),
                        turned(group, group_count - d, group_count) * share + i,
                    )
                )
        n = 0
        for i in range(share):
            q = group * share + i
            own[q] = at[order[group * share + i]]
            widens[which].start(own.at[q], n, q)
            rounds.append((which, n, q))
            n += 1
        for copy, q in y_copies:
            copy.wait_recv()
            widens[which].start(own.at[q], n, q)
            rounds.append((which, n, q))
            n += 1
        for copy, q in y_copies:
            copy.wait_send()
    for which, n, q in rounds:
        widens[which].forward(n, q)
    for widen in widens:
        widen.finish()
    sums.finish()
    for copy in up_z + cut_z:
        copy.wait_send()


def back_kernel(
    chips, client_count, group_count,
    inverse, part, up_own,
    grad_out,
    pair, relay, landed, y_from, y_at, z_from, own,
    tp_sems, y_sems, z_sems, wide_sems,
):
    client, group = lax.axis_index("client"), lax.axis_index("sdata")
    share = client_count // group_count
    greet(partners(chips, client_count, group_count))
    steps = [(d, i) for d in list(range(1, group_count)) + [0] for i in range(share)]
    chunks = [turned(group, d, group_count) * share + i for d, i in steps]
    sums = ShareSum(part, pair, relay, landed, [tp_sems.at[i] for i in range(4)], chunks, chips)
    y_copies = []
    for n, ((d, i), q) in enumerate(zip(steps, chunks)):
        block = (sums.get(n, q) + up_own[q].astype(F32)).astype(BF16)
        if d == 0:
            y_at[group * share + i] = block
        else:
            y_from[d, i] = block
            y_copies.append(
                send(
                    y_from.at[d, i], y_at.at[group * share + i],
                    y_sems.at[0, d, i], y_sems.at[1, d, i],
                    {"sdata": turned(group, d, group_count)},
                )
            )
    for copy in y_copies:
        copy.wait_recv()
    widen = Widen(grad_out, [wide_sems.at[i] for i in range(4)], chips)
    z_copies = []
    for k in list(range(1, client_count)):
        to = turned(client, k, client_count)
        z_from[k] = y_at[inverse[to]]
        z_copies.append(
            send(
                z_from.at[k], own.at[client], z_sems.at[0, k], z_sems.at[1, k], {"client": to}
            )
        )
    own[client] = y_at[inverse[client]]
    widen.start(own.at[client], 0, client)
    for k, copy in enumerate(z_copies, 1):
        copy.wait_recv()
        source = turned(client, client_count - k, client_count)
        widen.start(own.at[source], k, source)
    for k in range(client_count):
        widen.forward(k, turned(client, client_count - k, client_count))
    widen.finish()
    sums.finish()
    for copy in y_copies + z_copies:
        copy.wait_send()


class Chain:
    def __init__(self, own, forth, back, sems, count):
        self.own, self.forth, self.back, self.count = own, forth, back, count
        self.sems = sems
        self.at = lax.axis_index("client")

    def copy(self, way, j, d):
        landing = self.forth if way == 0 else self.back
        to = self.at + 1 if way == 0 else self.at - 1
        return pltpu.make_async_remote_copy(
            src_ref=self.own.at[d],
            dst_ref=landing.at[j],
            send_sem=self.sems.at[2 * way, j],
            recv_sem=self.sems.at[2 * way + 1, j],
            device_id={"client": lax.rem(to + self.count, self.count)},
            device_id_type=MESH,
        )

    def legs(self):
        for j in range(self.count - 1):
            for way in (0, 1):
                d = self.count - 1 - j if way == 0 else j
                end = 0 if way == 0 else self.count - 1
                beyond = self.at < d if way == 0 else self.at > d
                yield way, j, d, end, beyond

    def open(self, d, way):
        j = self.count - 1 - d if way == 0 else d
        if j < self.count - 1:
            end = 0 if way == 0 else self.count - 1

            @pl.when(self.at == end)
            def _():
                self.copy(way, j, d).start()

    def relay(self):
        for way, j, d, end, beyond in self.legs():
            landing = self.forth if way == 0 else self.back

            @pl.when(beyond & (self.at != end))
            def _(way=way, j=j, d=d, landing=landing):
                self.copy(way, j, d).wait_recv()
                self.own[d] = (self.own[d].astype(F32) + landing[j].astype(F32)).astype(BF16)
                self.copy(way, j, d).start()

    def total(self, out_refs):
        last = self.count - 1
        for way, end, j in ((0, 0, last - self.at), (1, last, self.at)):
            landing = self.forth if way == 0 else self.back

            @pl.when(self.at != end)
            def _(way=way, j=j, landing=landing):
                self.copy(way, j, 0).wait_recv()
                self.own[self.at] = (
                    self.own[self.at].astype(F32) + landing[j].astype(F32)
                ).astype(BF16)

        result = (self.own[self.at].astype(F32) * (1.0 / self.count)).astype(BF16)
        at = 0
        for out in out_refs:
            out[...] = result[:, at : at + out.shape[1]]
            at += out.shape[1]

    def finish(self):
        for way, j, d, end, beyond in self.legs():

            @pl.when(beyond)
            def _(way=way, j=j, d=d):
                self.copy(way, j, d).wait_send()


def learn_kernel(
    kv_count, count, aligned,
    cut_ref, output_ref, query_ref, key_ref, value_ref, context_ref, weights_ref, normed_ref,
    far_normed, far_context, cosine_ref, sine_ref, *refs,
):
    if not aligned:
        near_cut, give_cut, near_normed, refs = refs[0], refs[1], refs[2], refs[3:]
    query_out, key_out, value_out, output_out = refs[:4]
    (
        pulled, pair, key_turn, value_pair, weight_grad, score_grad, query_grad, shared_grad,
        far_cut, far_query, far_shared,
        output_own, output_forth, output_back, shared_own, shared_forth, shared_back,
        query_own, query_forth, query_back,
        cut_sems, core_sems, give_sems, output_sems, shared_sems, query_sems,
    ) = refs[4:]
    length = cut_ref.shape[0]
    rows = far_cut.shape[2]
    client, group = lax.axis_index("client"), lax.axis_index("sdata")
    tensor_at = lax.axis_index("tensor")
    core = lax.rem(tensor_at, CORES)
    sibling = {"tensor": tensor_at + 1 - 2 * core}
    across = {"sdata": 1 - group}
    ahead = {"client": lax.rem(client + 1, count)}
    behind = {"client": lax.rem(client + count - 1, count)}
    greet([sibling, across, ahead, behind])
    order = []
    for j in range((count + 1) // 2):
        order += [count - 1 - j, j]

    def columns(d, side):
        return pl.ds(pl.multiple_of((2 * d + side) * rows, rows), rows)

    def cut_copy(n, d):
        source = cut_ref.at[:, columns(d, 1 - group)] if aligned else give_cut.at[d]
        return pltpu.make_async_remote_copy(
            src_ref=source, dst_ref=far_cut.at[d],
            send_sem=cut_sems.at[0, n], recv_sem=cut_sems.at[1, n],
            device_id=across, device_id_type=MESH,
        )

    def core_copy(n, d):
        return pltpu.make_async_remote_copy(
            src_ref=far_cut.at[d], dst_ref=far_cut.at[d],
            send_sem=core_sems.at[0, n], recv_sem=core_sems.at[1, n],
            device_id=sibling, device_id_type=MESH,
        )

    halves = count // CORES
    picks = [order[CORES * n] + core * (order[CORES * n + 1] - order[CORES * n]) for n in range(halves)]
    others = [
        order[CORES * n + 1] + core * (order[CORES * n] - order[CORES * n + 1]) for n in range(halves)
    ]
    for n in range(halves):
        cut_copy(n, picks[n]).start()

    width = 2 * LANES if query_ref.shape[1] % (2 * LANES) == 0 else LANES
    for at in range(0, query_ref.shape[1], width):
        pulled[:, at : at + width] = jnp.dot(
            cut_ref[...], output_ref[:, at : at + width], preferred_element_type=F32
        ).astype(BF16)
    keys_float, values_float = key_ref[...].astype(F32), value_ref[...].astype(F32)
    keys_turned = keys_float.T.astype(BF16)
    key_turn[...] = jnp.zeros_like(key_turn)
    score_grad[...] = jnp.zeros_like(score_grad)
    for g in range(kv_count):
        value_pair[g, :length], value_pair[g, length:] = paired(values_float, g)
        mine = keys_turned[g * HEAD_DIM : (g + 1) * HEAD_DIM]
        key_turn[g, :HEAD_DIM, :length] = mine
        key_turn[g, HEAD_DIM:, length:] = mine

    def unturn(tile):
        return tile * cosine_ref[...] - swap_halves(tile) * sine_ref[...]

    tiles = query_ref.shape[1] // LANES
    low = lane_tile() < HEAD_DIM
    key_sum, value_sum = [None] * kv_count, [None] * kv_count
    for t in range(tiles):
        g = t * kv_count // tiles
        span = slice(t * LANES, (t + 1) * LANES)
        weight_grad[...] = lax.dot_general(
            value_pair[g], pulled[:, span], CROSSED, preferred_element_type=F32
        )
        for head in range(2):
            base = head * length
            for i in range(0, length, LANES):
                deep = i + LANES
                grad = weight_grad[base : base + deep, i : i + LANES].astype(BF16).astype(F32)
                weight = weights_ref[t, base : base + deep, i : i + LANES].astype(F32)
                both = grad * weight
                drift = jnp.sum(both, 0, keepdims=True)
                score_grad[base : base + deep, i : i + LANES] = (
                    (both - weight * drift) * HEAD_DIM ** (-0.5)
                ).astype(BF16)
        back_query = jnp.dot(key_turn[g], score_grad[...], preferred_element_type=F32)
        query_grad[:, span] = unturn(back_query.T.astype(BF16).astype(F32)).astype(BF16)
        back_key = jnp.dot(score_grad[...], query_ref[:, span], preferred_element_type=F32)
        back_value = jnp.dot(weights_ref[t], pulled[:, span], preferred_element_type=F32)
        first = key_sum[g] is None
        key_sum[g] = back_key if first else key_sum[g] + back_key
        value_sum[g] = back_value if first else value_sum[g] + back_value

    def folded(sums):
        whole = None
        for g, both in enumerate(sums):
            upper, lower = both[:length], both[length:]
            if g == 0:
                whole = upper + pltpu.roll(lower, HEAD_DIM, 1)
            else:
                whole = jnp.where(low, whole, pltpu.roll(upper, HEAD_DIM, 1) + lower)
        return whole.astype(BF16)

    shared_grad[:, :LANES] = unturn(folded(key_sum).astype(F32)).astype(BF16)
    shared_grad[:, LANES:] = folded(value_sum)

    def give(source, target, i):
        return pltpu.make_async_remote_copy(
            src_ref=source, dst_ref=target, send_sem=give_sems.at[0, i], recv_sem=give_sems.at[1, i],
            device_id=across, device_id_type=MESH,
        )

    gifts = [give(shared_grad, far_shared, 0), give(query_grad, far_query, 1)]
    for gift in gifts:
        gift.start()
    chains = [
        Chain(output_own, output_forth, output_back, output_sems, count),
        Chain(shared_own, shared_forth, shared_back, shared_sems, count),
        Chain(query_own, query_forth, query_back, query_sems, count),
    ]

    def near(d, from_cut):
        if aligned:
            return (cut_ref if from_cut else normed_ref)[:, columns(d, group)]
        return near_cut[d] if from_cut else near_normed[d]

    def product(chain, d, left, right, far_left, far_right):
        chain.own[d] = (
            lax.dot_general(left, right, TALL, preferred_element_type=F32)
            + lax.dot_general(far_left, far_right, TALL, preferred_element_type=F32)
        ).astype(BF16)

    for n in range(halves):
        cut_copy(n, picks[n]).wait_recv()
        core_copy(n, picks[n]).start()
        core_copy(n, others[n]).wait_recv()
        for i in range(CORES):
            d = order[CORES * n + i]
            product(chains[0], d, near(d, True), context_ref[...], far_cut[d], far_context[...])
            for way in (0, 1):
                chains[0].open(d, way)

    def spread(chain, grad, far_grad):
        for d in order:
            product(chain, d, near(d, False), grad[...], far_normed[d], far_grad[...])
            for way in (0, 1):
                chain.open(d, way)

    gifts[0].wait_recv()
    spread(chains[1], shared_grad, far_shared)
    chains[0].relay()
    gifts[1].wait_recv()
    spread(chains[2], query_grad, far_query)
    chains[1].relay()
    chains[2].relay()
    chains[0].total([output_out])
    chains[1].total([key_out, value_out])
    chains[2].total([query_out])
    for n in range(halves):
        cut_copy(n, picks[n]).wait_send()
        core_copy(n, picks[n]).wait_send()
    for gift in gifts:
        gift.wait_send()
    for chain in chains:
        chain.finish()


def learn(cut_grad, output_matrix, saved, normed, far_normed, far_context, tables, kv_count):
    unused, count, group_count = axis_counts()
    queries, keys, values, context, weights = saved
    length, breadth = cut_grad.shape
    features = queries.shape[1]
    rows = breadth // (count * group_count)
    aligned = rows % LANES == 0
    dma = pltpu.SemaphoreType.DMA
    shape = lambda *sizes: jax.ShapeDtypeStruct(sizes, BF16)
    vmem = lambda *sizes: pltpu.VMEM(sizes, BF16)
    operands = [cut_grad, output_matrix, queries, keys, values, context, weights, normed]
    operands += [far_normed, far_context, *tables]
    if not aligned:
        group = lax.axis_index("sdata")
        operands += [
            half_of(cut_grad, count, group), half_of(cut_grad, count, 1 - group),
            half_of(normed, count, group),
        ]
    chain = lambda wide: [
        vmem(count, rows, wide), vmem(count - 1, rows, wide), vmem(count - 1, rows, wide)
    ]
    return pl.pallas_call(
        partial(learn_kernel, kv_count, count, aligned),
        out_shape=(
            shape(rows, features), shape(rows, LANES), shape(rows, LANES), shape(rows, features)
        ),
        in_specs=[VMEM_SPEC] * len(operands),
        out_specs=(VMEM_SPEC,) * 4,
        scratch_shapes=[
            vmem(length, features), vmem(16, LANES), vmem(kv_count, LANES, 2 * length),
            vmem(kv_count, 2 * length, LANES), pltpu.VMEM((2 * length, length), F32),
            vmem(2 * length, length), vmem(length, features), vmem(length, 2 * LANES),
            vmem(count, length, rows), vmem(length, features), vmem(length, 2 * LANES),
        ]
        + chain(features) + chain(2 * LANES) + chain(features)
        + [dma((2, count // CORES)), dma((2, count // CORES)), dma((2, 2))]
        + [dma((4, count - 1))] * 3,
        compiler_params=params(3),
        name="learn",
    )(*operands)


def half_of(array, count, side):
    blocks = array.reshape(array.shape[0], count, 2, -1)
    return lax.dynamic_index_in_dim(blocks, side, 2, False).transpose(1, 0, 2)


def across_groups(array):
    count = lax.axis_size("sdata")
    return lax.ppermute(array, "sdata", [(g, (g + 1) % count) for g in range(count)])


def tables_of(length):
    halfway = HEAD_DIM // 2
    lanes = jnp.arange(LANES) % HEAD_DIM
    frequencies = jnp.exp(-math.log(500000.0) * (2.0 / HEAD_DIM) * (lanes % halfway).astype(F32))
    angles = jnp.arange(length).astype(F32)[:, None] * frequencies[None, :]
    sign = jnp.where(lanes < halfway, -1.0, 1.0)
    return jnp.cos(angles), jnp.sin(angles) * sign[None, :]


def widened(matrix):
    return jnp.pad(matrix, ((0, 0), (0, LANES - matrix.shape[1])))


VMEM_SPEC = pl.BlockSpec(memory_space=pltpu.VMEM)
ANY_SPEC = pl.BlockSpec(memory_space=pl.ANY)
SMEM_SPEC = pl.BlockSpec(memory_space=pltpu.SMEM)


def params(number):
    return pltpu.CompilerParams(
        collective_id=number, has_side_effects=True, vmem_limit_bytes=48 * 2**20
    )


def axis_counts():
    return lax.axis_size("tensor") // CORES, lax.axis_size("client"), lax.axis_size("sdata")


def relay_out(order, attended, rows_in, upstream):
    chips, client_count, group_count = axis_counts()
    length, breadth = rows_in.shape
    chunk, width = length // client_count, breadth // (CORES * chips)
    share = client_count // group_count
    full = (client_count, chunk, breadth)
    own = (client_count, chunk, width)
    dma = pltpu.SemaphoreType.DMA
    vmem = lambda shape: pltpu.VMEM(shape, BF16)
    cut, up, up_own = pl.pallas_call(
        partial(out_kernel, chips, client_count, group_count),
        out_shape=(
            jax.ShapeDtypeStruct(full, BF16),
            jax.ShapeDtypeStruct(full, BF16),
            jax.ShapeDtypeStruct(own, BF16),
        ),
        in_specs=[SMEM_SPEC, VMEM_SPEC, VMEM_SPEC, VMEM_SPEC],
        out_specs=(VMEM_SPEC,) * 3,
        scratch_shapes=[
            vmem((chips,) + own), vmem((chips,) + own), vmem((chips,) + own),
            vmem(own), vmem(own), vmem(own),
            vmem((group_count, share, chunk, width)), vmem((group_count, share, chunk, width)),
            vmem(own),
            dma((4, chips, client_count)), dma((4, client_count)),
            dma((4, group_count, share)), dma((8, chips, client_count)),
        ],
        compiler_params=params(1),
        name="relay_out",
    )(order, attended.reshape(full), rows_in.reshape(full), upstream.reshape(full))
    return cut.reshape(length, breadth), up.reshape(length, breadth), up_own


def relay_back(inverse, pulled, up_own):
    chips, client_count, group_count = axis_counts()
    length, breadth = pulled.shape
    chunk, width = length // client_count, breadth // (CORES * chips)
    share = client_count // group_count
    full = (client_count, chunk, breadth)
    own = (client_count, chunk, width)
    dma = pltpu.SemaphoreType.DMA
    vmem = lambda shape: pltpu.VMEM(shape, BF16)
    grad = pl.pallas_call(
        partial(back_kernel, chips, client_count, group_count),
        out_shape=jax.ShapeDtypeStruct(full, BF16),
        in_specs=[SMEM_SPEC, VMEM_SPEC, VMEM_SPEC],
        out_specs=VMEM_SPEC,
        scratch_shapes=[
            vmem((chips,) + own), vmem((chips,) + own), vmem((chips,) + own),
            vmem((group_count, share, chunk, width)), vmem(own), vmem(own), vmem(own),
            dma((4, chips, client_count)), dma((2, group_count, share)),
            dma((2, client_count)), dma((4, chips, client_count)),
        ],
        compiler_params=params(2),
        name="relay_back",
    )(inverse, pulled.reshape(full), up_own)
    return grad.reshape(length, breadth)


def local(
    client_input,
    client_gain,
    query_weight,
    key_weight,
    client_value_weight,
    output_weight,
    server_gain,
    server_gate,
    server_up,
    server_down,
    upstream,
    assignment,
):
    client_count = lax.axis_size("client")
    shared = key_weight.shape[2]
    kv_count = shared // HEAD_DIM
    tables = tables_of(client_input.shape[0])
    matrices = [
        query_weight[0], widened(key_weight[0]), widened(client_value_weight[0]), output_weight[0]
    ]
    normed, theirs, *saved, attended = forward(
        client_input, client_gain, tables, matrices, kv_count, client_count
    )
    if theirs.ndim == 2:
        theirs = half_of(normed, client_count, 1 - lax.axis_index("sdata"))
    far_normed = across_groups(theirs)
    ids = jnp.arange(client_count).astype(jnp.int32)
    ahead = (assignment[None, :] < assignment[:, None]) | (
        (assignment[None, :] == assignment[:, None]) & (ids[None, :] < ids[:, None])
    )
    inverse = jnp.sum(ahead.astype(jnp.int32), 1)
    group_order = jnp.sum(jnp.where(inverse[None, :] == ids[:, None], ids[None, :], 0), 1)
    cut_rows, up_rows, up_own = relay_out(group_order, attended, client_input, upstream)
    context, cut_rows = lax.optimization_barrier((saved[3], cut_rows))
    far_context = across_groups(context)
    pulled = server_pull(
        cut_rows, up_rows, server_gain[0], server_gate[0], server_up[0], server_down[0]
    )
    arriving_grad = relay_back(inverse, pulled, up_own)
    query_update, key_update, value_update, output_update = learn(
        arriving_grad, output_weight[0], saved, normed, far_normed, far_context, tables, kv_count
    )
    return (query_update, key_update[:, :shared], value_update[:, :shared], output_update)


def solution(mesh):
    placed = (
        P(("client", "sdata"), None),
        P("client", None),
        P("client", None, "tensor"),
        P("client", None, "tensor"),
        P("client", None, "tensor"),
        P("client", None, "tensor"),
        P("sdata", None),
        P("sdata", None, "tensor"),
        P("sdata", None, "tensor"),
        P("sdata", "tensor", None),
        P(("client", "sdata"), None),
        P(),
    )
    return jax.shard_map(
        local,
        mesh=mesh,
        in_specs=placed,
        out_specs=(
            P(("client", "sdata"), "tensor"),
            P(("client", "sdata"), "tensor"),
            P(("client", "sdata"), "tensor"),
            P(("client", "sdata"), "tensor"),
        ),
        check_vma=False,
    )
```

```python
from functools import partial
import math

import jax
import jax.numpy as jnp
from jax import lax
from jax.experimental import pallas as pl
from jax.experimental.pallas import tpu as pltpu
from jax.sharding import PartitionSpec as P

HEAD_DIM = 64
MESH = pl.DeviceIdType.MESH
CORES = 2
LANES = 128
BF16 = jnp.bfloat16
F32 = jnp.float32


def lane_tile(flag_ref=None):
    return lax.broadcasted_iota(jnp.int32, (1, LANES), 1)


def swap_halves(tile):
    low = lax.rem(lane_tile(), HEAD_DIM) < HEAD_DIM // 2
    ahead = pltpu.roll(tile, LANES - HEAD_DIM // 2, 1)
    behind = pltpu.roll(tile, HEAD_DIM // 2, 1)
    return jnp.where(low, ahead, behind)


def paired(tile, at):
    low = lane_tile() < HEAD_DIM
    moved = pltpu.roll(tile, HEAD_DIM, 1)
    first, second = (tile, moved) if at == 0 else (moved, tile)
    zero = jnp.zeros_like(tile)
    return jnp.where(low, first, zero).astype(BF16), jnp.where(low, zero, second).astype(BF16)


CROSSED = (((1,), (1,)), ((), ()))
TALL = (((0,), (0,)), ((), ()))


VMEM_SPEC = pl.BlockSpec(memory_space=pltpu.VMEM)
ANY_SPEC = pl.BlockSpec(memory_space=pl.ANY)
SMEM_SPEC = pl.BlockSpec(memory_space=pltpu.SMEM)


def params(number):
    return pltpu.CompilerParams(
        collective_id=number, has_side_effects=True, vmem_limit_bytes=48 * 2**20
    )


def axis_counts():
    return lax.axis_size("tensor") // CORES, lax.axis_size("client"), lax.axis_size("sdata")


def greet(others):
    barrier = pltpu.get_barrier_semaphore()
    for other in others:
        pl.semaphore_signal(barrier, inc=1, device_id=other, device_id_type=MESH)
    pl.semaphore_wait(barrier, len(others))


def send(source, target, send_sem, recv_sem, device):
    copy = pltpu.make_async_remote_copy(
        src_ref=source,
        dst_ref=target,
        send_sem=send_sem,
        recv_sem=recv_sem,
        device_id=device,
        device_id_type=MESH,
    )
    copy.start()
    return copy


def place():
    tensor_at = lax.axis_index("tensor")
    return tensor_at // CORES, lax.rem(tensor_at, CORES)


def turned(index, step, count):
    return lax.rem(index + step, count)


def columns_of(chip, core, width):
    return pl.ds(pl.multiple_of((chip * CORES + core) * width, width), width)


def partners(chips, client_count, group_count):
    chip, core = place()
    client, group = lax.axis_index("client"), lax.axis_index("sdata")
    others = [{"tensor": chip * CORES + 1 - core}]
    others += [{"tensor": turned(chip, k, chips) * CORES + core} for k in range(1, chips)]
    others += [{"client": turned(client, k, client_count)} for k in range(1, client_count)]
    others += [{"sdata": turned(group, k, group_count)} for k in range(1, group_count)]
    return others


class ShareSum:
    def __init__(self, part, pair, relay, landed, sems, pieces, chips):
        self.part, self.pair, self.relay, self.landed = part, pair, relay, landed
        self.pair_send, self.pair_recv, self.chip_send, self.chip_recv = sems
        self.chips, self.width = chips, part.shape[-1] // (CORES * chips)
        self.chip, self.core = place()
        self.pair_copies = {}
        self.chip_copies = {}
        for n, (q, rows) in enumerate(pieces):
            for k in list(range(1, chips)) + [0]:
                to = turned(self.chip, k, chips)
                self.pair_copies[k, n] = send(
                    part.at[q, rows, columns_of(to, 1 - self.core, self.width)],
                    pair.at[k, q, rows],
                    self.pair_send.at[k, n],
                    self.pair_recv.at[k, n],
                    {"tensor": self.chip * CORES + 1 - self.core},
                )
        for n, (q, rows) in enumerate(pieces):
            for k in range(1, chips):
                to = turned(self.chip, k, chips)
                self.pair_copies[k, n].wait_recv()
                relay[k, q, rows] = (
                    part[q, rows, columns_of(to, self.core, self.width)].astype(F32)
                    + pair[k, q, rows].astype(F32)
                ).astype(BF16)
                self.chip_copies[k, n] = send(
                    relay.at[k, q, rows],
                    landed.at[k, q, rows],
                    self.chip_send.at[k, n],
                    self.chip_recv.at[k, n],
                    {"tensor": to * CORES + self.core},
                )

    def get(self, n, piece):
        q, rows = piece
        self.pair_copies[0, n].wait_recv()
        total = self.part[q, rows, columns_of(self.chip, self.core, self.width)].astype(
            F32
        ) + self.pair[0, q, rows].astype(F32)
        for k in range(1, self.chips):
            self.chip_copies[k, n].wait_recv()
            total = total + self.landed[k, q, rows].astype(F32)
        return total

    def finish(self):
        for copy in list(self.pair_copies.values()) + list(self.chip_copies.values()):
            copy.wait_send()


class Widen:
    def __init__(self, out, sems, chips):
        self.out, self.chips = out, chips
        self.chip_send, self.chip_recv, self.pair_send, self.pair_recv = sems
        self.chip, self.core = place()
        self.width = out.shape[-1] // (CORES * chips)
        self.forwarded, self.chip_copies = [], {}

    def spot(self, piece, k):
        q, rows = piece
        at = turned(self.chip, self.chips - k, self.chips)
        return q, rows, columns_of(at, self.core, self.width)

    def pair_copy(self, source, k, n, piece):
        self.forwarded.append(
            send(
                source,
                self.out.at[self.spot(piece, k)],
                self.pair_send.at[k, n],
                self.pair_recv.at[k, n],
                {"tensor": self.chip * CORES + 1 - self.core},
            )
        )

    def start(self, source, n, piece):
        spot = self.spot(piece, 0)
        for k in range(1, self.chips):
            self.chip_copies[k, n] = send(
                source,
                self.out.at[spot],
                self.chip_send.at[k, n],
                self.chip_recv.at[k, n],
                {"tensor": turned(self.chip, k, self.chips) * CORES + self.core},
            )
        self.pair_copy(source, 0, n, piece)
        self.out[spot] = source[...]

    def forward(self, n, piece):
        for k in range(1, self.chips):
            self.chip_copies[k, n].wait_recv()
            self.pair_copy(self.out.at[self.spot(piece, k)], k, n, piece)

    def finish(self):
        for copy in self.forwarded:
            copy.wait_recv()
        for copy in self.forwarded + list(self.chip_copies.values()):
            copy.wait_send()


PARTS = 2


def parts_of(chunk):
    parts = PARTS if chunk % (16 * PARTS) == 0 else 1
    return [slice(p * chunk // parts, (p + 1) * chunk // parts) for p in range(parts)]


def out_kernel(
    chips, client_count, group_count,
    order, part, inputs, up_at,
    cut_out, up_own,
    pair, relay, landed, cut_from, up_put, cut_put, cut_own,
    tp_sems, z_sems, y_sems, up_sems, wide_sems, *cut_at,
):
    client, group = lax.axis_index("client"), lax.axis_index("sdata")
    chip, core = place()
    share = client_count // group_count
    chunk = part.shape[1]
    width = part.shape[-1] // (CORES * chips)
    cols = columns_of(chip, core, width)
    greet(partners(chips, client_count, group_count))
    parts = parts_of(chunk)
    steps = list(range(1, client_count)) + [0]
    pieces = [(turned(client, k, client_count), rows) for rows in parts for k in steps]
    sums = ShareSum(part, pair, relay, landed, [tp_sems.at[i] for i in range(4)], pieces, chips)
    up_copies = []
    for d in range(1, group_count):
        to = turned(group, d, group_count)
        for i in range(share):
            up_put[d, i] = up_at[order[to * share + i]]
            up_copies.append(
                send(
                    up_put.at[d, i], up_own.at[group * share + i],
                    up_sems.at[0, d, i], up_sems.at[1, d, i], {"sdata": to},
                )
            )
    for i in range(share):
        up_own[group * share + i] = up_at[order[group * share + i]]
    cut_z = []
    for n, piece in enumerate(pieces):
        p, k = n // client_count, steps[n % client_count]
        to, rows = piece
        block = (sums.get(n, piece) + inputs[to, rows, cols].astype(F32)).astype(BF16)
        if k == 0:
            cut_at[p][client] = block
        else:
            cut_from[k, rows] = block
            cut_z.append(
                (
                    p,
                    send(
                        cut_from.at[k, rows], cut_at[p].at[client],
                        z_sems.at[0, p, k], z_sems.at[1, p, k], {"client": to},
                    ),
                )
            )
    widen = Widen(cut_out, [wide_sems.at[i] for i in range(4)], chips)
    rounds, y_copies = [], []

    def widen_piece(q, rows):
        widen.start(cut_own.at[q, rows], len(rounds), (q, rows))
        rounds.append((q, rows))

    for p, rows in enumerate(parts):
        for which, copy in cut_z:
            if which == p:
                copy.wait_recv()
        for d in range(1, group_count):
            to = turned(group, d, group_count)
            for i in range(share):
                cut_put[d, i, rows] = cut_at[p][order[to * share + i]]
                y_copies.append(
                    (
                        send(
                            cut_put.at[d, i, rows], cut_own.at[group * share + i, rows],
                            y_sems.at[0, p, d, i], y_sems.at[1, p, d, i], {"sdata": to},
                        ),
                        turned(group, group_count - d, group_count) * share + i,
                        rows,
                    )
                )
        for i in range(share):
            q = group * share + i
            cut_own[q, rows] = cut_at[p][order[group * share + i]]
            widen_piece(q, rows)
    for copy, q, rows in y_copies:
        copy.wait_recv()
        widen_piece(q, rows)
    for n, piece in enumerate(rounds):
        widen.forward(n, piece)
    widen.finish()
    sums.finish()
    for copy in up_copies:
        copy.wait_recv()
    for copy in up_copies + [c for unused, c in cut_z] + [c for c, unused, also in y_copies]:
        copy.wait_send()


def back_kernel(
    chips, client_count, group_count,
    inverse, part, up_own,
    grad_out,
    pair, relay, landed, y_from, z_from, own,
    tp_sems, y_sems, z_sems, wide_sems, *y_at,
):
    client, group = lax.axis_index("client"), lax.axis_index("sdata")
    share = client_count // group_count
    greet(partners(chips, client_count, group_count))
    parts = parts_of(part.shape[1])
    steps = [(d, i) for d in list(range(1, group_count)) + [0] for i in range(share)]
    pieces = [
        (turned(group, d, group_count) * share + i, rows) for rows in parts for d, i in steps
    ]
    sums = ShareSum(part, pair, relay, landed, [tp_sems.at[i] for i in range(4)], pieces, chips)
    y_copies = []
    for n, piece in enumerate(pieces):
        p, (d, i) = n // len(steps), steps[n % len(steps)]
        q, rows = piece
        block = (sums.get(n, piece) + up_own[q, rows].astype(F32)).astype(BF16)
        if d == 0:
            y_at[p][group * share + i] = block
        else:
            y_from[d, i, rows] = block
            y_copies.append(
                (
                    p,
                    send(
                        y_from.at[d, i, rows], y_at[p].at[group * share + i],
                        y_sems.at[0, p, d, i], y_sems.at[1, p, d, i],
                        {"sdata": turned(group, d, group_count)},
                    ),
                )
            )
    widen = Widen(grad_out, [wide_sems.at[i] for i in range(4)], chips)
    z_copies, rounds = [], []

    def widen_piece(q, rows):
        widen.start(own.at[q, rows], len(rounds), (q, rows))
        rounds.append((q, rows))

    for p, rows in enumerate(parts):
        for which, copy in y_copies:
            if which == p:
                copy.wait_recv()
        for k in range(1, client_count):
            to = turned(client, k, client_count)
            z_from[k, rows] = y_at[p][inverse[to]]
            z_copies.append(
                (
                    send(
                        z_from.at[k, rows], own.at[client, rows],
                        z_sems.at[0, p, k], z_sems.at[1, p, k], {"client": to},
                    ),
                    turned(client, client_count - k, client_count),
                    rows,
                )
            )
        own[client, rows] = y_at[p][inverse[client]]
        widen_piece(client, rows)
    for copy, source, rows in z_copies:
        copy.wait_recv()
        widen_piece(source, rows)
    for n, piece in enumerate(rounds):
        widen.forward(n, piece)
    widen.finish()
    sums.finish()
    for copy in [c for unused, c in y_copies] + [c for c, unused, also in z_copies]:
        copy.wait_send()


def forward_kernel(
    kv_count, sends_half, chips, count,
    rows_hbm, gain_ref, cosine_hbm, sine_hbm, upstream_hbm,
    query_hbm, key_hbm, value_hbm, output_hbm,
    normed_out, far_out, query_out, key_out, value_out, context_out, weights_out, attended_out, up_out,
    rows_ref, cosine_ref, sine_ref,
    query_mat, key_mat, value_mat, output_mat, scores, key_pair, value_turn, theirs,
    sems, z_sems, y_sems,
):
    length = rows_ref.shape[0]
    client, group = lax.axis_index("client"), lax.axis_index("sdata")
    chip, core = place()
    chunk, width = up_out.shape[1:]
    moves = (
        (rows_hbm, rows_ref), (cosine_hbm, cosine_ref), (sine_hbm, sine_ref),
        (query_hbm, query_mat), (key_hbm, key_mat), (value_hbm, value_mat), (output_hbm, output_mat),
        (upstream_hbm.at[client, :, columns_of(chip, core, width)], up_out.at[client]),
    )
    copies = []
    for i, (source, target) in enumerate(moves):
        copies.append(pltpu.make_async_copy(source, target, sems.at[i]))
        copies[-1].start()
    greet(
        [{"client": turned(client, k, count)} for k in range(1, count)]
        + ([{"sdata": 1 - group}] if sends_half else [])
    )
    sent = []
    for k in range(1, count):
        to = turned(client, k, count)
        sent.append(
            send(
                upstream_hbm.at[to, :, columns_of(chip, core, width)], up_out.at[client],
                z_sems.at[0, k], z_sems.at[1, k], {"client": to},
            )
        )
    copies[0].wait()
    rows_float = rows_ref[...].astype(F32)
    inv_rms = lax.rsqrt(jnp.mean(rows_float * rows_float, -1, keepdims=True) + 1e-05)
    normed_out[...] = (rows_float * inv_rms * gain_ref[...].astype(F32)).astype(BF16)
    if sends_half:
        wide = far_out.shape[2]
        for n in range(count // CORES):
            d = CORES * n + core
            at = pl.ds(pl.multiple_of((2 * d + 1 - group) * wide, wide), wide)
            theirs[n] = normed_out[:, at]
            sent.append(
                send(
                    theirs.at[n], far_out.at[n], y_sems.at[0, n], y_sems.at[1, n],
                    {"sdata": 1 - group},
                )
            )
    normed = normed_out[...]
    copies[1].wait()
    copies[2].wait()

    def turn(tile):
        return tile * cosine_ref[...] + swap_halves(tile) * sine_ref[...]

    copies[3].wait()
    wide = 2 * LANES
    for at in range(0, query_mat.shape[1], wide):
        part = jnp.dot(normed, query_mat[:, at : at + wide], preferred_element_type=F32)
        for side in (0, LANES):
            query_out[:, at + side : at + side + LANES] = turn(part[:, side : side + LANES]).astype(BF16)
    copies[4].wait()
    keys = turn(jnp.dot(normed, key_mat[...], preferred_element_type=F32)).astype(BF16)
    key_out[...] = keys
    copies[5].wait()
    values = jnp.dot(normed, value_mat[...], preferred_element_type=F32).astype(BF16)
    value_out[...] = values
    keys_float, values_float = keys.astype(F32), values.astype(F32)
    values_turned = values_float.T.astype(BF16)
    value_turn[...] = jnp.zeros_like(value_turn)
    for g in range(kv_count):
        key_pair[g, :length], key_pair[g, length:] = paired(keys_float, g)
        mine = values_turned[g * HEAD_DIM : (g + 1) * HEAD_DIM]
        value_turn[g, :HEAD_DIM, :length] = mine
        value_turn[g, HEAD_DIM:, length:] = mine
    tiles = query_mat.shape[1] // LANES
    step = LANES
    for t in range(tiles):
        g = t * kv_count // tiles
        scores[...] = lax.dot_general(
            key_pair[g], query_out[:, t * LANES : (t + 1) * LANES], CROSSED, preferred_element_type=F32
        )
        for head in range(2):
            base = head * length
            for i in range(0, length, step):
                deep = i + step
                block = scores[base : base + deep, i : i + step] * HEAD_DIM ** (-0.5)
                key_ids = lax.broadcasted_iota(jnp.int32, (deep, step), 0)
                query_ids = lax.broadcasted_iota(jnp.int32, (deep, step), 1) + i
                block = jnp.where(key_ids <= query_ids, block, -1e30)
                exponent = jnp.exp(block - jnp.max(block, 0, keepdims=True))
                share = 1.0 / jnp.sum(exponent, 0, keepdims=True)
                weights_out[t, base : base + deep, i : i + step] = (exponent * share).astype(BF16)
                if deep < length:
                    weights_out[t, base + deep : base + length, i : i + step] = jnp.zeros(
                        (length - deep, step), BF16
                    )
        turned_context = jnp.dot(value_turn[g], weights_out[t], preferred_element_type=F32)
        context_out[:, t * LANES : (t + 1) * LANES] = turned_context.T.astype(BF16)
    copies[6].wait()
    context = context_out[...]
    wide = next(b for b in (512, 256, 128) if attended_out.shape[1] % b == 0)
    for at in range(0, attended_out.shape[1], wide):
        attended_out[:, at : at + wide] = lax.dot_general(
            context, output_mat[at : at + wide, :], CROSSED, preferred_element_type=F32
        ).astype(BF16)
    copies[7].wait()
    for copy in sent:
        copy.wait_recv()
    for copy in sent:
        copy.wait_send()


def forward(rows_in, gain, tables, upstream, matrices, kv_count):
    chips, count, unused = axis_counts()
    length, breadth = rows_in.shape
    features, shared = matrices[0].shape[1], matrices[1].shape[1]
    tiles = features // LANES
    rows = breadth // (2 * count)
    sends_half = rows % LANES == 0
    shape = lambda *sizes: jax.ShapeDtypeStruct(sizes, BF16)
    half = (count // CORES, length, rows) if sends_half else (16, LANES)
    chunk, width = length // count, breadth // (CORES * chips)
    dma = pltpu.SemaphoreType.DMA
    return pl.pallas_call(
        partial(forward_kernel, kv_count, sends_half, chips, count),
        out_shape=(
            shape(length, breadth), shape(*half), shape(length, features), shape(length, shared),
            shape(length, shared), shape(length, features), shape(tiles, 2 * length, length),
            shape(length, breadth), shape(count, chunk, width),
        ),
        in_specs=[ANY_SPEC, VMEM_SPEC] + [ANY_SPEC] * 7,
        out_specs=(VMEM_SPEC,) * 9,
        scratch_shapes=[pltpu.VMEM(rows_in.shape, BF16)]
        + [pltpu.VMEM(table.shape, F32) for table in tables]
        + [pltpu.VMEM(m.shape, BF16) for m in matrices]
        + [
            pltpu.VMEM((2 * length, length), F32),
            pltpu.VMEM((kv_count, 2 * length, LANES), BF16),
            pltpu.VMEM((kv_count, LANES, 2 * length), BF16),
            pltpu.VMEM(half, BF16),
            dma((8,)), dma((2, count)), dma((2, count)),
        ],
        compiler_params=params(4),
        name="forward",
    )(rows_in, gain, *tables, upstream.reshape(count, chunk, breadth), *matrices)


def server_kernel(
    chips, shares,
    rows_ref, own_ref, gain_ref, context_ref, half_ref, gate_hbm, up_hbm, down_hbm,
    out_ref, far_context, far_normed,
    up_all, normed_ref, gate_value, up_value, gate_grad, up_grad, weighted_ref,
    gate_ref, up_ref, down_ref, load_sems, wide_sems, far_sems, core_sems, local_sems,
):
    length, breadth = rows_ref.shape
    hidden = gate_ref.shape[1]
    block = next(b for b in (512, 256, 128, hidden) if hidden % b == 0)
    spans = [slice(at, at + block) for at in range(0, hidden, block)]

    def loads(i, which):
        source, target = ((gate_hbm, gate_ref), (up_hbm, up_ref), (down_hbm, down_ref))[which]
        at = (spans[i], slice(None)) if which == 2 else (slice(None), spans[i])
        return pltpu.make_async_copy(source.at[at], target.at[at], load_sems.at[which, i])

    for which in range(3):
        for i in range(len(spans)):
            loads(i, which).start()
    group = lax.axis_index("sdata")
    chip, core = place()
    sibling = {"tensor": chip * CORES + 1 - core}
    greet(
        [sibling, {"sdata": 1 - group}]
        + [{"tensor": turned(chip, k, chips) * CORES + core} for k in range(1, chips)]
    )
    widen = Widen(up_all, [wide_sems.at[i] for i in range(4)], chips)
    count = own_ref.shape[0]
    for q in range(count):
        widen.start(own_ref.at[q], q, (q, slice(None)))
    others = [
        send(context_ref, far_context, far_sems.at[0], far_sems.at[1], {"sdata": 1 - group})
    ]
    kept = []
    for n in range(shares):
        d = CORES * n + core
        others.append(
            send(half_ref.at[n], far_normed.at[d], core_sems.at[0, n], core_sems.at[1, n], sibling)
        )
        kept.append(pltpu.make_async_copy(half_ref.at[n], far_normed.at[d], local_sems.at[n]))
        kept[-1].start()
    rows_float = rows_ref[...].astype(F32)
    gain = gain_ref[...].astype(F32)
    inv_rms = lax.rsqrt(jnp.mean(rows_float * rows_float, -1, keepdims=True) + 1e-05)
    normed_ref[...] = (rows_float * inv_rms * gain).astype(BF16)
    for i, span in enumerate(spans):
        loads(i, 0).wait()
        gate_value[:, span] = jnp.dot(normed_ref[...], gate_ref[:, span], preferred_element_type=F32)
        loads(i, 1).wait()
        up_value[:, span] = jnp.dot(normed_ref[...], up_ref[:, span], preferred_element_type=F32)
    for q in range(count):
        widen.forward(q, (q, slice(None)))
    widen.finish()
    upstream = up_all[...].reshape(length, breadth)
    for i, span in enumerate(spans):
        loads(i, 2).wait()
        pulled = lax.dot_general(upstream, down_ref[span], CROSSED, preferred_element_type=F32)
        gate, up = gate_value[:, span], up_value[:, span]
        sigmoid_gate = jax.nn.sigmoid(gate)
        gate_grad[:, span] = (
            pulled * up * sigmoid_gate * (1.0 + gate * (1.0 - sigmoid_gate))
        ).astype(BF16)
        up_grad[:, span] = (pulled * gate * sigmoid_gate).astype(BF16)
    step = next(b for b in (256, 128, breadth) if breadth % b == 0)
    lean = jnp.zeros((length, 1), F32)
    for at in range(0, breadth, step):
        span = slice(at, at + step)
        weighted = (
            lax.dot_general(gate_grad[...], gate_ref[span], CROSSED, preferred_element_type=F32)
            + lax.dot_general(up_grad[...], up_ref[span], CROSSED, preferred_element_type=F32)
        ) * gain_ref[:, span].astype(F32)
        weighted_ref[:, span] = weighted
        lean = lean + jnp.sum(weighted * rows_ref[:, span].astype(F32), -1, keepdims=True)
    pull = inv_rms**3 * (lean * (1.0 / breadth))
    out_ref[...] = (inv_rms * weighted_ref[...] - rows_ref[...].astype(F32) * pull).astype(BF16)
    for copy in others:
        copy.wait_recv()
    for copy in others:
        copy.wait_send()
    for copy in kept:
        copy.wait()


def server_pull(rows_in, up_own, gain, context, half, gate_matrix, up_matrix, down_matrix):
    chips, count, unused = axis_counts()
    length, breadth = rows_in.shape
    hidden = gate_matrix.shape[1]
    shares = half.shape[0] if half.ndim == 3 else 0
    full = (count,) + half.shape[1:] if shares else half.shape
    dma = pltpu.SemaphoreType.DMA
    vmem = lambda *sizes: pltpu.VMEM(sizes, BF16)
    wide = lambda *sizes: pltpu.VMEM(sizes, F32)
    return pl.pallas_call(
        partial(server_kernel, chips, shares),
        out_shape=(
            jax.ShapeDtypeStruct((length, breadth), BF16),
            jax.ShapeDtypeStruct(context.shape, BF16),
            jax.ShapeDtypeStruct(full, BF16),
        ),
        in_specs=[VMEM_SPEC] * 5 + [ANY_SPEC] * 3,
        out_specs=(VMEM_SPEC,) * 3,
        scratch_shapes=[
            vmem(count, length // count, breadth), vmem(length, breadth),
            wide(length, hidden), wide(length, hidden), vmem(length, hidden), vmem(length, hidden),
            wide(length, breadth),
            vmem(breadth, hidden), vmem(breadth, hidden), vmem(hidden, breadth),
            dma((3, hidden // LANES)), dma((4, chips, count)), dma((2,)), dma((2, count)),
            dma((count,)),
        ],
        compiler_params=params(5),
        name="server_pull",
    )(rows_in, up_own, gain[None], context, half, gate_matrix, up_matrix, down_matrix)


class Chain:
    def __init__(self, own, forth, back, sems, count):
        self.own, self.forth, self.back, self.count = own, forth, back, count
        self.sems = sems
        self.at = lax.axis_index("client")

    def copy(self, way, j, d):
        landing = self.forth if way == 0 else self.back
        to = self.at + 1 if way == 0 else self.at - 1
        return pltpu.make_async_remote_copy(
            src_ref=self.own.at[d],
            dst_ref=landing.at[j],
            send_sem=self.sems.at[2 * way, j],
            recv_sem=self.sems.at[2 * way + 1, j],
            device_id={"client": lax.rem(to + self.count, self.count)},
            device_id_type=MESH,
        )

    def legs(self):
        for j in range(self.count - 1):
            for way in (0, 1):
                d = self.count - 1 - j if way == 0 else j
                end = 0 if way == 0 else self.count - 1
                beyond = self.at < d if way == 0 else self.at > d
                yield way, j, d, end, beyond

    def open(self, d, way):
        j = self.count - 1 - d if way == 0 else d
        if j < self.count - 1:
            end = 0 if way == 0 else self.count - 1

            @pl.when(self.at == end)
            def _():
                self.copy(way, j, d).start()

    def relay(self):
        near = self.at < self.count // 2
        legs = list(self.legs())
        turns = [(leg, near) for leg in legs if leg[0] == 0]
        turns += [(leg, self.at >= 0) for leg in legs if leg[0] == 1]
        turns += [(leg, jnp.logical_not(near)) for leg in legs if leg[0] == 0]
        for (way, j, d, end, beyond), now in turns:
            landing = self.forth if way == 0 else self.back

            @pl.when(now & beyond & (self.at != end))
            def _(way=way, j=j, d=d, landing=landing):
                self.copy(way, j, d).wait_recv()
                self.own[d] = (self.own[d].astype(F32) + landing[j].astype(F32)).astype(BF16)
                self.copy(way, j, d).start()

    def total(self, out_refs):
        last = self.count - 1
        for way, end, j in ((0, 0, last - self.at), (1, last, self.at)):
            landing = self.forth if way == 0 else self.back

            @pl.when(self.at != end)
            def _(way=way, j=j, landing=landing):
                self.copy(way, j, 0).wait_recv()
                self.own[self.at] = (
                    self.own[self.at].astype(F32) + landing[j].astype(F32)
                ).astype(BF16)

        result = (self.own[self.at].astype(F32) * (1.0 / self.count)).astype(BF16)
        at = 0
        for out in out_refs:
            out[...] = result[:, at : at + out.shape[1]]
            at += out.shape[1]

    def finish(self):
        for way, j, d, end, beyond in self.legs():

            @pl.when(beyond)
            def _(way=way, j=j, d=d):
                self.copy(way, j, d).wait_send()


def learn_kernel(
    kv_count, count, aligned,
    cut_ref, output_ref, query_ref, key_ref, value_ref, context_ref, weights_ref, normed_ref,
    far_normed, far_context, cosine_ref, sine_ref, *refs,
):
    if not aligned:
        near_cut, give_cut, near_normed, refs = refs[0], refs[1], refs[2], refs[3:]
    query_out, key_out, value_out, output_out = refs[:4]
    (
        pulled, pair, key_turn, value_pair, weight_grad, score_grad, query_grad, shared_grad,
        far_cut, far_query, far_shared,
        output_own, output_forth, output_back, shared_own, shared_forth, shared_back,
        query_own, query_forth, query_back,
        cut_sems, core_sems, give_sems, output_sems, shared_sems, query_sems,
    ) = refs[4:]
    length = cut_ref.shape[0]
    rows = far_cut.shape[2]
    client, group = lax.axis_index("client"), lax.axis_index("sdata")
    tensor_at = lax.axis_index("tensor")
    core = lax.rem(tensor_at, CORES)
    sibling = {"tensor": tensor_at + 1 - 2 * core}
    across = {"sdata": 1 - group}
    ahead = {"client": lax.rem(client + 1, count)}
    behind = {"client": lax.rem(client + count - 1, count)}
    greet([sibling, across, ahead, behind])
    order = []
    for j in range((count + 1) // 2):
        order += [count - 1 - j, j]

    def columns(d, side):
        return pl.ds(pl.multiple_of((2 * d + side) * rows, rows), rows)

    def cut_copy(n, d):
        source = cut_ref.at[:, columns(d, 1 - group)] if aligned else give_cut.at[d]
        return pltpu.make_async_remote_copy(
            src_ref=source, dst_ref=far_cut.at[d],
            send_sem=cut_sems.at[0, n], recv_sem=cut_sems.at[1, n],
            device_id=across, device_id_type=MESH,
        )

    def core_copy(n, d):
        return pltpu.make_async_remote_copy(
            src_ref=far_cut.at[d], dst_ref=far_cut.at[d],
            send_sem=core_sems.at[0, n], recv_sem=core_sems.at[1, n],
            device_id=sibling, device_id_type=MESH,
        )

    halves = count // CORES
    picks = [order[CORES * n] + core * (order[CORES * n + 1] - order[CORES * n]) for n in range(halves)]
    others = [
        order[CORES * n + 1] + core * (order[CORES * n] - order[CORES * n + 1]) for n in range(halves)
    ]
    for n in range(halves):
        cut_copy(n, picks[n]).start()

    width = 2 * LANES if query_ref.shape[1] % (2 * LANES) == 0 else LANES
    for at in range(0, query_ref.shape[1], width):
        pulled[:, at : at + width] = jnp.dot(
            cut_ref[...], output_ref[:, at : at + width], preferred_element_type=F32
        ).astype(BF16)
    keys_float, values_float = key_ref[...].astype(F32), value_ref[...].astype(F32)
    keys_turned = keys_float.T.astype(BF16)
    key_turn[...] = jnp.zeros_like(key_turn)
    score_grad[...] = jnp.zeros_like(score_grad)
    for g in range(kv_count):
        value_pair[g, :length], value_pair[g, length:] = paired(values_float, g)
        mine = keys_turned[g * HEAD_DIM : (g + 1) * HEAD_DIM]
        key_turn[g, :HEAD_DIM, :length] = mine
        key_turn[g, HEAD_DIM:, length:] = mine

    def unturn(tile):
        return tile * cosine_ref[...] - swap_halves(tile) * sine_ref[...]

    tiles = query_ref.shape[1] // LANES
    low = lane_tile() < HEAD_DIM
    key_sum, value_sum = [None] * kv_count, [None] * kv_count
    for t in range(tiles):
        g = t * kv_count // tiles
        span = slice(t * LANES, (t + 1) * LANES)
        weight_grad[...] = lax.dot_general(
            value_pair[g], pulled[:, span], CROSSED, preferred_element_type=F32
        )
        for head in range(2):
            base = head * length
            for i in range(0, length, LANES):
                deep = i + LANES
                grad = weight_grad[base : base + deep, i : i + LANES].astype(BF16).astype(F32)
                weight = weights_ref[t, base : base + deep, i : i + LANES].astype(F32)
                both = grad * weight
                drift = jnp.sum(both, 0, keepdims=True)
                score_grad[base : base + deep, i : i + LANES] = (
                    (both - weight * drift) * HEAD_DIM ** (-0.5)
                ).astype(BF16)
        back_query = jnp.dot(key_turn[g], score_grad[...], preferred_element_type=F32)
        query_grad[:, span] = unturn(back_query.T.astype(BF16).astype(F32)).astype(BF16)
        back_key = jnp.dot(score_grad[...], query_ref[:, span], preferred_element_type=F32)
        back_value = jnp.dot(weights_ref[t], pulled[:, span], preferred_element_type=F32)
        first = key_sum[g] is None
        key_sum[g] = back_key if first else key_sum[g] + back_key
        value_sum[g] = back_value if first else value_sum[g] + back_value

    def folded(sums):
        whole = None
        for g, both in enumerate(sums):
            upper, lower = both[:length], both[length:]
            if g == 0:
                whole = upper + pltpu.roll(lower, HEAD_DIM, 1)
            else:
                whole = jnp.where(low, whole, pltpu.roll(upper, HEAD_DIM, 1) + lower)
        return whole.astype(BF16)

    shared_grad[:, :LANES] = unturn(folded(key_sum).astype(F32)).astype(BF16)
    shared_grad[:, LANES:] = folded(value_sum)

    def give(source, target, i):
        return pltpu.make_async_remote_copy(
            src_ref=source, dst_ref=target, send_sem=give_sems.at[0, i], recv_sem=give_sems.at[1, i],
            device_id=across, device_id_type=MESH,
        )

    gifts = [give(shared_grad, far_shared, 0), give(query_grad, far_query, 1)]
    for gift in gifts:
        gift.start()
    chains = [
        Chain(output_own, output_forth, output_back, output_sems, count),
        Chain(shared_own, shared_forth, shared_back, shared_sems, count),
        Chain(query_own, query_forth, query_back, query_sems, count),
    ]

    def near(d, from_cut):
        if aligned:
            return (cut_ref if from_cut else normed_ref)[:, columns(d, group)]
        return near_cut[d] if from_cut else near_normed[d]

    def product(chain, d, left, right, far_left, far_right):
        chain.own[d] = (
            lax.dot_general(left, right, TALL, preferred_element_type=F32)
            + lax.dot_general(far_left, far_right, TALL, preferred_element_type=F32)
        ).astype(BF16)

    for n in range(halves):
        cut_copy(n, picks[n]).wait_recv()
        core_copy(n, picks[n]).start()
        core_copy(n, others[n]).wait_recv()
        for i in range(CORES):
            d = order[CORES * n + i]
            product(chains[0], d, near(d, True), context_ref[...], far_cut[d], far_context[...])
            for way in (0, 1):
                chains[0].open(d, way)

    def spread(chain, grad, far_grad):
        for d in order:
            product(chain, d, near(d, False), grad[...], far_normed[d], far_grad[...])
            for way in (0, 1):
                chain.open(d, way)

    gifts[0].wait_recv()
    spread(chains[1], shared_grad, far_shared)
    chains[0].relay()
    gifts[1].wait_recv()
    spread(chains[2], query_grad, far_query)
    chains[1].relay()
    chains[2].relay()
    chains[0].total([output_out])
    chains[1].total([key_out, value_out])
    chains[2].total([query_out])
    for n in range(halves):
        cut_copy(n, picks[n]).wait_send()
        core_copy(n, picks[n]).wait_send()
    for gift in gifts:
        gift.wait_send()
    for chain in chains:
        chain.finish()


def learn(cut_grad, output_matrix, saved, normed, far_normed, far_context, tables, kv_count):
    unused, count, group_count = axis_counts()
    queries, keys, values, context, weights = saved
    length, breadth = cut_grad.shape
    features = queries.shape[1]
    rows = breadth // (count * group_count)
    aligned = rows % LANES == 0
    dma = pltpu.SemaphoreType.DMA
    shape = lambda *sizes: jax.ShapeDtypeStruct(sizes, BF16)
    vmem = lambda *sizes: pltpu.VMEM(sizes, BF16)
    operands = [cut_grad, output_matrix, queries, keys, values, context, weights, normed]
    operands += [far_normed, far_context, *tables]
    if not aligned:
        group = lax.axis_index("sdata")
        operands += [
            half_of(cut_grad, count, group), half_of(cut_grad, count, 1 - group),
            half_of(normed, count, group),
        ]
    chain = lambda wide: [
        vmem(count, rows, wide), vmem(count - 1, rows, wide), vmem(count - 1, rows, wide)
    ]
    return pl.pallas_call(
        partial(learn_kernel, kv_count, count, aligned),
        out_shape=(
            shape(rows, features), shape(rows, LANES), shape(rows, LANES), shape(rows, features)
        ),
        in_specs=[VMEM_SPEC] * len(operands),
        out_specs=(VMEM_SPEC,) * 4,
        scratch_shapes=[
            vmem(length, features), vmem(16, LANES), vmem(kv_count, LANES, 2 * length),
            vmem(kv_count, 2 * length, LANES), pltpu.VMEM((2 * length, length), F32),
            vmem(2 * length, length), vmem(length, features), vmem(length, 2 * LANES),
            vmem(count, length, rows), vmem(length, features), vmem(length, 2 * LANES),
        ]
        + chain(features) + chain(2 * LANES) + chain(features)
        + [dma((2, count // CORES)), dma((2, count // CORES)), dma((2, 2))]
        + [dma((4, count - 1))] * 3,
        compiler_params=params(3),
        name="learn",
    )(*operands)


def half_of(array, count, side):
    blocks = array.reshape(array.shape[0], count, 2, -1)
    return lax.dynamic_index_in_dim(blocks, side, 2, False).transpose(1, 0, 2)


def across_groups(array):
    count = lax.axis_size("sdata")
    return lax.ppermute(array, "sdata", [(g, (g + 1) % count) for g in range(count)])


def tables_of(length):
    halfway = HEAD_DIM // 2
    lanes = jnp.arange(LANES) % HEAD_DIM
    frequencies = jnp.exp(-math.log(500000.0) * (2.0 / HEAD_DIM) * (lanes % halfway).astype(F32))
    angles = jnp.arange(length).astype(F32)[:, None] * frequencies[None, :]
    sign = jnp.where(lanes < halfway, -1.0, 1.0)
    return jnp.cos(angles), jnp.sin(angles) * sign[None, :]


def widened(matrix):
    return jnp.pad(matrix, ((0, 0), (0, LANES - matrix.shape[1])))


def relay_out(order, attended, rows_in, up_at):
    chips, client_count, group_count = axis_counts()
    length, breadth = rows_in.shape
    chunk, width = length // client_count, breadth // (CORES * chips)
    share = client_count // group_count
    parts = len(parts_of(chunk))
    full = (client_count, chunk, breadth)
    own = (client_count, chunk, width)
    dma = pltpu.SemaphoreType.DMA
    vmem = lambda shape: pltpu.VMEM(shape, BF16)
    cut, up_own = pl.pallas_call(
        partial(out_kernel, chips, client_count, group_count),
        out_shape=(jax.ShapeDtypeStruct(full, BF16), jax.ShapeDtypeStruct(own, BF16)),
        in_specs=[SMEM_SPEC, VMEM_SPEC, VMEM_SPEC, VMEM_SPEC],
        out_specs=(VMEM_SPEC,) * 2,
        scratch_shapes=[
            vmem((chips,) + own), vmem((chips,) + own), vmem((chips,) + own), vmem(own),
            vmem((group_count, share, chunk, width)), vmem((group_count, share, chunk, width)),
            vmem(own),
            dma((4, chips, parts * client_count)), dma((2, parts, client_count)),
            dma((2, parts, group_count, share)), dma((2, group_count, share)),
            dma((4, chips, parts * client_count)),
        ]
        + [vmem((client_count, chunk // parts, width))] * parts,
        compiler_params=params(1),
        name="relay_out",
    )(order, attended.reshape(full), rows_in.reshape(full), up_at)
    return cut.reshape(length, breadth), up_own


def relay_back(inverse, pulled, up_own):
    chips, client_count, group_count = axis_counts()
    length, breadth = pulled.shape
    chunk, width = length // client_count, breadth // (CORES * chips)
    share = client_count // group_count
    parts = len(parts_of(chunk))
    full = (client_count, chunk, breadth)
    own = (client_count, chunk, width)
    dma = pltpu.SemaphoreType.DMA
    vmem = lambda shape: pltpu.VMEM(shape, BF16)
    grad = pl.pallas_call(
        partial(back_kernel, chips, client_count, group_count),
        out_shape=jax.ShapeDtypeStruct(full, BF16),
        in_specs=[SMEM_SPEC, VMEM_SPEC, VMEM_SPEC],
        out_specs=VMEM_SPEC,
        scratch_shapes=[
            vmem((chips,) + own), vmem((chips,) + own), vmem((chips,) + own),
            vmem((group_count, share, chunk, width)), vmem(own), vmem(own),
            dma((4, chips, parts * client_count)), dma((2, parts, group_count, share)),
            dma((2, parts, client_count)), dma((4, chips, parts * client_count)),
        ]
        + [vmem((client_count, chunk // parts, width))] * parts,
        compiler_params=params(2),
        name="relay_back",
    )(inverse, pulled.reshape(full), up_own)
    return grad.reshape(length, breadth)


def local(
    client_input,
    client_gain,
    query_weight,
    key_weight,
    client_value_weight,
    output_weight,
    server_gain,
    server_gate,
    server_up,
    server_down,
    upstream,
    assignment,
):
    client_count = lax.axis_size("client")
    shared = key_weight.shape[2]
    kv_count = shared // HEAD_DIM
    tables = tables_of(client_input.shape[0])
    matrices = [
        query_weight[0], widened(key_weight[0]), widened(client_value_weight[0]), output_weight[0]
    ]
    normed, half, *saved, attended, up_at = forward(
        client_input, client_gain, tables, upstream, matrices, kv_count
    )
    ids = jnp.arange(client_count).astype(jnp.int32)
    ahead = (assignment[None, :] < assignment[:, None]) | (
        (assignment[None, :] == assignment[:, None]) & (ids[None, :] < ids[:, None])
    )
    inverse = jnp.sum(ahead.astype(jnp.int32), 1)
    group_order = jnp.sum(jnp.where(inverse[None, :] == ids[:, None], ids[None, :], 0), 1)
    cut_rows, up_own = relay_out(group_order, attended, client_input, up_at)
    pulled, far_context, far_normed = server_pull(
        cut_rows, up_own, server_gain[0], saved[3], half,
        server_gate[0], server_up[0], server_down[0],
    )
    if half.ndim == 2:
        far_normed = across_groups(half_of(normed, client_count, 1 - lax.axis_index("sdata")))
    arriving_grad = relay_back(inverse, pulled, up_own)
    query_update, key_update, value_update, output_update = learn(
        arriving_grad, output_weight[0], saved, normed, far_normed, far_context, tables, kv_count
    )
    return (query_update, key_update[:, :shared], value_update[:, :shared], output_update)


def solution(mesh):
    placed = (
        P(("client", "sdata"), None),
        P("client", None),
        P("client", None, "tensor"),
        P("client", None, "tensor"),
        P("client", None, "tensor"),
        P("client", None, "tensor"),
        P("sdata", None),
        P("sdata", None, "tensor"),
        P("sdata", None, "tensor"),
        P("sdata", "tensor", None),
        P(("client", "sdata"), None),
        P(),
    )
    return jax.shard_map(
        local,
        mesh=mesh,
        in_specs=placed,
        out_specs=(
            P(("client", "sdata"), "tensor"),
            P(("client", "sdata"), "tensor"),
            P(("client", "sdata"), "tensor"),
            P(("client", "sdata"), "tensor"),
        ),
        check_vma=False,
    )
```

```python
from functools import partial
import math

import jax
import jax.numpy as jnp
import numpy as np
from jax import lax
from jax.experimental import pallas as pl
from jax.experimental.pallas import tpu as pltpu
from jax.sharding import PartitionSpec as P

HEAD_DIM = 64
MESH = pl.DeviceIdType.MESH
CORES = 2
LANES = 128
BF16 = jnp.bfloat16
F32 = jnp.float32


def lane_tile(flag_ref=None):
    return lax.broadcasted_iota(jnp.int32, (1, LANES), 1)


def swap_halves(tile):
    low = lax.rem(lane_tile(), HEAD_DIM) < HEAD_DIM // 2
    ahead = pltpu.roll(tile, LANES - HEAD_DIM // 2, 1)
    behind = pltpu.roll(tile, HEAD_DIM // 2, 1)
    return jnp.where(low, ahead, behind)


def unfold(table, cosine_ref, sine_ref):
    low = lane_tile() < HEAD_DIM
    moved = pltpu.roll(table, HEAD_DIM, 1)
    cosine_ref[...] = jnp.where(low, table, moved)
    sine_ref[...] = jnp.where(low, moved, table)


def paired(tile, at):
    low = lane_tile() < HEAD_DIM
    moved = pltpu.roll(tile, HEAD_DIM, 1)
    first, second = (tile, moved) if at == 0 else (moved, tile)
    zero = jnp.zeros_like(tile)
    return jnp.where(low, first, zero).astype(BF16), jnp.where(low, zero, second).astype(BF16)


CROSSED = (((1,), (1,)), ((), ()))
TALL = (((0,), (0,)), ((), ()))


VMEM_SPEC = pl.BlockSpec(memory_space=pltpu.VMEM)
HBM_SPEC = pl.BlockSpec(memory_space=pltpu.HBM)
SMEM_SPEC = pl.BlockSpec(memory_space=pltpu.SMEM)


def params(number, mebibytes):
    return pltpu.CompilerParams(
        collective_id=number, has_side_effects=True, vmem_limit_bytes=mebibytes * 2**20
    )


def axis_counts():
    return lax.axis_size("tensor") // CORES, lax.axis_size("client"), lax.axis_size("sdata")


def greet(others):
    barrier = pltpu.get_barrier_semaphore()
    for other in others:
        pl.semaphore_signal(barrier, inc=1, device_id=other, device_id_type=MESH)
    pl.semaphore_wait(barrier, len(others))


def send(source, target, send_sem, recv_sem, device):
    copy = pltpu.make_async_remote_copy(
        src_ref=source,
        dst_ref=target,
        send_sem=send_sem,
        recv_sem=recv_sem,
        device_id=device,
        device_id_type=MESH,
    )
    copy.start()
    return copy


def place():
    tensor_at = lax.axis_index("tensor")
    return tensor_at // CORES, lax.rem(tensor_at, CORES)


def turned(index, step, count):
    return lax.rem(index + step, count)


def columns_of(chip, core, width):
    return pl.ds(pl.multiple_of((chip * CORES + core) * width, width), width)


def partners(chips, client_count, group_count):
    chip, core = place()
    client, group = lax.axis_index("client"), lax.axis_index("sdata")
    others = [{"tensor": chip * CORES + 1 - core}]
    others += [{"tensor": turned(chip, k, chips) * CORES + core} for k in range(1, chips)]
    others += [{"client": turned(client, k, client_count)} for k in range(1, client_count)]
    others += [{"sdata": turned(group, k, group_count)} for k in range(1, group_count)]
    return others


class ShareSum:
    def __init__(self, part, pair, relay, landed, sems, pieces, chips):
        self.part, self.pair, self.relay, self.landed = part, pair, relay, landed
        self.pair_send, self.pair_recv, self.chip_send, self.chip_recv = sems
        self.chips, self.width = chips, part.shape[-1] // (CORES * chips)
        self.chip, self.core = place()
        self.pair_copies = {}
        self.chip_copies = {}
        for n, (q, rows) in enumerate(pieces):
            for k in list(range(1, chips)) + [0]:
                to = turned(self.chip, k, chips)
                self.pair_copies[k, n] = send(
                    part.at[q, rows, columns_of(to, 1 - self.core, self.width)],
                    pair.at[k, q, rows],
                    self.pair_send.at[k, n],
                    self.pair_recv.at[k, n],
                    {"tensor": self.chip * CORES + 1 - self.core},
                )
        for n, (q, rows) in enumerate(pieces):
            for k in range(1, chips):
                to = turned(self.chip, k, chips)
                self.pair_copies[k, n].wait_recv()
                relay[k, q, rows] = (
                    part[q, rows, columns_of(to, self.core, self.width)].astype(F32)
                    + pair[k, q, rows].astype(F32)
                ).astype(BF16)
                self.chip_copies[k, n] = send(
                    relay.at[k, q, rows],
                    landed.at[k, q, rows],
                    self.chip_send.at[k, n],
                    self.chip_recv.at[k, n],
                    {"tensor": to * CORES + self.core},
                )

    def get(self, n, piece):
        q, rows = piece
        self.pair_copies[0, n].wait_recv()
        total = self.part[q, rows, columns_of(self.chip, self.core, self.width)].astype(
            F32
        ) + self.pair[0, q, rows].astype(F32)
        for k in range(1, self.chips):
            self.chip_copies[k, n].wait_recv()
            total = total + self.landed[k, q, rows].astype(F32)
        return total

    def finish(self):
        for copy in list(self.pair_copies.values()) + list(self.chip_copies.values()):
            copy.wait_send()


class Widen:
    def __init__(self, out, sems, chips):
        self.out, self.chips = out, chips
        self.chip_send, self.chip_recv, self.pair_send, self.pair_recv = sems
        self.chip, self.core = place()
        self.width = out.shape[-1] // (CORES * chips)
        self.forwarded, self.chip_copies = [], {}

    def spot(self, piece, k):
        q, rows = piece
        at = turned(self.chip, self.chips - k, self.chips)
        return q, rows, columns_of(at, self.core, self.width)

    def pair_copy(self, source, k, n, piece):
        self.forwarded.append(
            send(
                source,
                self.out.at[self.spot(piece, k)],
                self.pair_send.at[k, n],
                self.pair_recv.at[k, n],
                {"tensor": self.chip * CORES + 1 - self.core},
            )
        )

    def start(self, source, n, piece):
        spot = self.spot(piece, 0)
        for k in range(1, self.chips):
            self.chip_copies[k, n] = send(
                source,
                self.out.at[spot],
                self.chip_send.at[k, n],
                self.chip_recv.at[k, n],
                {"tensor": turned(self.chip, k, self.chips) * CORES + self.core},
            )
        self.pair_copy(source, 0, n, piece)
        self.out[spot] = source[...]

    def forward(self, n, piece):
        for k in range(1, self.chips):
            self.chip_copies[k, n].wait_recv()
            self.pair_copy(self.out.at[self.spot(piece, k)], k, n, piece)

    def finish(self):
        for copy in self.forwarded:
            copy.wait_recv()
        for copy in self.forwarded + list(self.chip_copies.values()):
            copy.wait_send()


PARTS = 2


def parts_of(chunk):
    parts = PARTS if chunk % (16 * PARTS) == 0 else 1
    return [slice(p * chunk // parts, (p + 1) * chunk // parts) for p in range(parts)]


def out_kernel(
    chips, client_count, group_count,
    order, sent, part, inputs, up_at,
    cut_out, up_own, up_all,
    pair, relay, landed, cut_from, up_put, cut_put, cut_own,
    tp_sems, z_sems, y_sems, up_sems, wide_sems, kept_sems, *cut_at,
):
    client, group = lax.axis_index("client"), lax.axis_index("sdata")
    share = client_count // group_count
    chunk = part.shape[1]
    parts = parts_of(chunk)
    steps = list(range(1, client_count)) + [0]
    pieces = [(turned(client, k, client_count), rows) for rows in parts for k in steps]
    sums = ShareSum(part, pair, relay, landed, [tp_sems.at[i] for i in range(4)], pieces, chips)
    for copy in sent:
        copy.wait_recv()
    up_copies = []
    for d in range(1, group_count):
        to = turned(group, d, group_count)
        for i in range(share):
            up_put[d, i] = up_at[order(to * share + i)]
            up_copies.append(
                send(
                    up_put.at[d, i], up_own.at[group * share + i],
                    up_sems.at[0, d, i], up_sems.at[1, d, i], {"sdata": to},
                )
            )
    kept = Widen(up_all, [kept_sems.at[i] for i in range(4)], chips)
    for i in range(share):
        q = group * share + i
        up_own[q] = up_at[order(q)]
        kept.start(up_own.at[q], i, (q, slice(None)))
    cut_z = []
    for n, piece in enumerate(pieces):
        p, k = n // client_count, steps[n % client_count]
        to, rows = piece
        block = (sums.get(n, piece) + inputs[to, rows].astype(F32)).astype(BF16)
        if k == 0:
            cut_at[p][client] = block
        else:
            cut_from[k, rows] = block
            cut_z.append(
                (
                    p,
                    send(
                        cut_from.at[k, rows], cut_at[p].at[client],
                        z_sems.at[0, p, k], z_sems.at[1, p, k], {"client": to},
                    ),
                )
            )
    widen = Widen(cut_out, [wide_sems.at[i] for i in range(4)], chips)
    rounds, y_copies = [], []

    def widen_piece(q, rows):
        widen.start(cut_own.at[q, rows], len(rounds), (q, rows))
        rounds.append((q, rows))

    for p, rows in enumerate(parts):
        for which, copy in cut_z:
            if which == p:
                copy.wait_recv()
        for d in range(1, group_count):
            to = turned(group, d, group_count)
            for i in range(share):
                cut_put[d, i, rows] = cut_at[p][order(to * share + i)]
                y_copies.append(
                    (
                        send(
                            cut_put.at[d, i, rows], cut_own.at[group * share + i, rows],
                            y_sems.at[0, p, d, i], y_sems.at[1, p, d, i], {"sdata": to},
                        ),
                        turned(group, group_count - d, group_count) * share + i,
                        rows,
                    )
                )
        for i in range(share):
            q = group * share + i
            cut_own[q, rows] = cut_at[p][order(group * share + i)]
            widen_piece(q, rows)
    for copy, q, rows in y_copies:
        copy.wait_recv()
        widen_piece(q, rows)
    for i in range(share):
        kept.forward(i, (group * share + i, slice(None)))
    for n, piece in enumerate(rounds):
        widen.forward(n, piece)
    widen.finish()
    kept.finish()
    sums.finish()
    for copy in up_copies:
        copy.wait_recv()
    for copy in sent + up_copies + [c for unused, c in cut_z] + [c for c, unused, also in y_copies]:
        copy.wait_send()


def ranked(assigned, c, at):
    total = 0
    for j in range(c):
        before = (assigned[j] < assigned[at]) | ((assigned[j] == assigned[at]) & (j < at))
        total = total + jnp.where(before, 1, 0)
    return total


def depart_kernel(kv_count, sends_half, chips, count, groups, assigned, *refs):
    ins, outs = refs[:9], refs[9:16]
    cut_out, up_own, up_all = refs[16:19]
    attended, up_at, inputs = refs[19:22]
    fore, rest = refs[22:38], refs[38:]
    sent = forward_kernel(
        kv_count, sends_half, chips, count, *ins, *outs, attended, up_at, inputs, *fore
    )
    ranks = [ranked(assigned, count, c) for c in range(count)]

    def order(at):
        return sum(jnp.where(rank == at, c, 0) for c, rank in enumerate(ranks))

    out_kernel(
        chips, count, groups, order, sent, attended, inputs, up_at, cut_out, up_own, up_all, *rest
    )


def depart(assigned, rows_in, gain, table, upstream, matrices, kv_count):
    chips, count, groups = axis_counts()
    length, breadth = rows_in.shape
    features, shared = matrices[0].shape[1], matrices[1].shape[1]
    tiles = features // LANES
    rows = breadth // (2 * count)
    sends_half = rows % LANES == 0
    shape = lambda *sizes: jax.ShapeDtypeStruct(sizes, BF16)
    half = (count // CORES, length, rows) if sends_half else (16, LANES)
    chunk, width = length // count, breadth // (CORES * chips)
    share, parts = count // groups, len(parts_of(chunk))
    full, own = (count, chunk, breadth), (count, chunk, width)
    dma = pltpu.SemaphoreType.DMA
    vmem = lambda sizes: pltpu.VMEM(sizes, BF16)
    return pl.pallas_call(
        partial(depart_kernel, kv_count, sends_half, chips, count, groups),
        out_shape=(
            shape(length, breadth), shape(*half), shape(length, features), shape(length, shared),
            shape(length, shared), shape(length, features), shape(tiles, 2 * length, length),
            shape(*full), shape(*own), shape(*full),
        ),
        in_specs=[SMEM_SPEC] + [HBM_SPEC] * 9,
        out_specs=(VMEM_SPEC,) * 10,
        scratch_shapes=[vmem(full), vmem(own), vmem(own), vmem(rows_in.shape), vmem(gain.shape)]
        + [pltpu.VMEM(table.shape, F32)] * 3
        + [vmem(m.shape) for m in matrices]
        + [
            pltpu.VMEM((2, 2 * length, length), F32), vmem((kv_count, 2 * length, LANES)),
            vmem((kv_count, LANES, 2 * length)), vmem(half),
            dma((9,)), dma((2, count)), dma((2, count)),
            vmem((chips,) + own), vmem((chips,) + own), vmem((chips,) + own), vmem(own),
            vmem((groups, share, chunk, width)), vmem((groups, share, chunk, width)), vmem(own),
            dma((4, chips, parts * count)), dma((2, parts, count)),
            dma((2, parts, groups, share)), dma((2, groups, share)),
            dma((4, chips, parts * count)), dma((4, chips, share)),
        ]
        + [vmem((count, chunk // parts, width))] * parts,
        compiler_params=params(1, 52),
        name="depart",
    )(
        assigned, rows_in, gain, table, upstream.reshape(full), rows_in.reshape(full), *matrices
    )


def back_kernel(
    chips, client_count, group_count,
    assigned, part, up_own,
    grad_out,
    pair, relay, landed, y_from, z_from, own,
    tp_sems, y_sems, z_sems, wide_sems, *y_at,
):
    client, group = lax.axis_index("client"), lax.axis_index("sdata")
    share = client_count // group_count
    greet(partners(chips, client_count, group_count))
    parts = parts_of(part.shape[1])
    steps = [(d, i) for d in list(range(1, group_count)) + [0] for i in range(share)]
    pieces = [
        (turned(group, d, group_count) * share + i, rows) for rows in parts for d, i in steps
    ]
    sums = ShareSum(part, pair, relay, landed, [tp_sems.at[i] for i in range(4)], pieces, chips)
    widen = Widen(grad_out, [wide_sems.at[i] for i in range(4)], chips)
    y_copies, z_copies, rounds = [], [], []

    def widen_piece(q, rows):
        widen.start(own.at[q, rows], len(rounds), (q, rows))
        rounds.append((q, rows))

    for p, rows in enumerate(parts):
        arrivals = []
        for at, (d, i) in enumerate(steps):
            n = p * len(steps) + at
            q = pieces[n][0]
            block = (sums.get(n, (q, rows)) + up_own[q, rows].astype(F32)).astype(BF16)
            if d == 0:
                y_at[p][group * share + i] = block
            else:
                y_from[d, i, rows] = block
                arrivals.append(
                    send(
                        y_from.at[d, i, rows], y_at[p].at[group * share + i],
                        y_sems.at[0, p, d, i], y_sems.at[1, p, d, i],
                        {"sdata": turned(group, d, group_count)},
                    )
                )
        for copy in arrivals:
            copy.wait_recv()
        y_copies += arrivals
        for k in range(1, client_count):
            to = turned(client, k, client_count)
            z_from[k, rows] = y_at[p][ranked(assigned, client_count, to)]
            z_copies.append(
                (
                    send(
                        z_from.at[k, rows], own.at[client, rows],
                        z_sems.at[0, p, k], z_sems.at[1, p, k], {"client": to},
                    ),
                    turned(client, client_count - k, client_count),
                    rows,
                )
            )
        own[client, rows] = y_at[p][ranked(assigned, client_count, client)]
        widen_piece(client, rows)
    for copy, source, rows in z_copies:
        copy.wait_recv()
        widen_piece(source, rows)
    for n, piece in enumerate(rounds):
        widen.forward(n, piece)
    widen.finish()
    sums.finish()
    for copy in y_copies + [c for c, unused, also in z_copies]:
        copy.wait_send()


def forward_kernel(
    kv_count, sends_half, chips, count,
    rows_hbm, gain_hbm, table_hbm, upstream_hbm, inputs_hbm,
    query_hbm, key_hbm, value_hbm, output_hbm,
    normed_out, far_out, query_out, key_out, value_out, context_out, weights_out,
    attended_out, up_out, inputs_out,
    rows_ref, gain_ref, table_ref, cosine_ref, sine_ref,
    query_mat, key_mat, value_mat, output_mat, scores, key_pair, value_turn, theirs,
    sems, z_sems, y_sems,
):
    length = rows_ref.shape[0]
    client, group = lax.axis_index("client"), lax.axis_index("sdata")
    chip, core = place()
    chunk, width = up_out.shape[1:]
    moves = (
        (rows_hbm, rows_ref), (table_hbm, table_ref), (gain_hbm, gain_ref),
        (query_hbm, query_mat), (key_hbm, key_mat), (value_hbm, value_mat), (output_hbm, output_mat),
        (upstream_hbm.at[client, :, columns_of(chip, core, width)], up_out.at[client]),
        (inputs_hbm.at[:, :, columns_of(chip, core, width)], inputs_out),
    )
    copies = []
    for i, (source, target) in enumerate(moves):
        copies.append(pltpu.make_async_copy(source, target, sems.at[i]))
        copies[-1].start()
    greet(partners(chips, count, lax.axis_size("sdata")))
    sent = []
    for k in range(1, count):
        to = turned(client, k, count)
        sent.append(
            send(
                upstream_hbm.at[to, :, columns_of(chip, core, width)], up_out.at[client],
                z_sems.at[0, k], z_sems.at[1, k], {"client": to},
            )
        )
    copies[0].wait()
    copies[2].wait()
    rows_float = rows_ref[...].astype(F32)
    inv_rms = lax.rsqrt(jnp.mean(rows_float * rows_float, -1, keepdims=True) + 1e-05)
    normed_out[...] = (rows_float * inv_rms * gain_ref[...].astype(F32)).astype(BF16)
    if sends_half:
        wide = far_out.shape[2]
        for n in range(count // CORES):
            d = CORES * n + core
            at = pl.ds(pl.multiple_of((2 * d + 1 - group) * wide, wide), wide)
            theirs[n] = normed_out[:, at]
            sent.append(
                send(
                    theirs.at[n], far_out.at[n], y_sems.at[0, n], y_sems.at[1, n],
                    {"sdata": 1 - group},
                )
            )
    normed = normed_out[...]
    copies[1].wait()
    unfold(table_ref[...], cosine_ref, sine_ref)

    def turn(tile):
        return tile * cosine_ref[...] + swap_halves(tile) * sine_ref[...]

    copies[3].wait()
    wide = 2 * LANES
    for at in range(0, query_mat.shape[1], wide):
        part = jnp.dot(normed, query_mat[:, at : at + wide], preferred_element_type=F32)
        for side in (0, LANES):
            query_out[:, at + side : at + side + LANES] = turn(part[:, side : side + LANES]).astype(BF16)
    copies[4].wait()
    keys = turn(jnp.dot(normed, key_mat[...], preferred_element_type=F32)).astype(BF16)
    key_out[...] = keys
    copies[5].wait()
    values = jnp.dot(normed, value_mat[...], preferred_element_type=F32).astype(BF16)
    value_out[...] = values
    keys_float, values_float = keys.astype(F32), values.astype(F32)
    values_turned = values_float.T.astype(BF16)
    value_turn[...] = jnp.zeros_like(value_turn)
    for g in range(kv_count):
        key_pair[g, :length], key_pair[g, length:] = paired(keys_float, g)
        mine = values_turned[g * HEAD_DIM : (g + 1) * HEAD_DIM]
        value_turn[g, :HEAD_DIM, :length] = mine
        value_turn[g, HEAD_DIM:, length:] = mine
    tiles = query_mat.shape[1] // LANES
    step = LANES
    for t in range(tiles):
        g = t * kv_count // tiles
        scores[t % 2] = lax.dot_general(
            key_pair[g], query_out[:, t * LANES : (t + 1) * LANES], CROSSED, preferred_element_type=F32
        )
        for head in range(2):
            base = head * length
            for i in range(0, length, step):
                deep = i + step
                block = scores[t % 2, base : base + deep, i : i + step] * HEAD_DIM ** (-0.5)
                key_ids = lax.broadcasted_iota(jnp.int32, (deep, step), 0)
                query_ids = lax.broadcasted_iota(jnp.int32, (deep, step), 1) + i
                block = jnp.where(key_ids <= query_ids, block, -1e30)
                exponent = jnp.exp(block - jnp.max(block, 0, keepdims=True))
                share = 1.0 / jnp.sum(exponent, 0, keepdims=True)
                weights_out[t, base : base + deep, i : i + step] = (exponent * share).astype(BF16)
                if deep < length:
                    weights_out[t, base + deep : base + length, i : i + step] = jnp.zeros(
                        (length - deep, step), BF16
                    )
        turned_context = jnp.dot(value_turn[g], weights_out[t], preferred_element_type=F32)
        context_out[:, t * LANES : (t + 1) * LANES] = turned_context.T.astype(BF16)
    copies[6].wait()
    context = context_out[...]
    breadth = attended_out.shape[2]
    wide = next(b for b in (512, 256, 128) if breadth % b == 0)
    for at in range(0, breadth, wide):
        attended_out[:, :, at : at + wide] = (
            lax.dot_general(
                context, output_mat[at : at + wide, :], CROSSED, preferred_element_type=F32
            )
            .reshape(count, chunk, wide)
            .astype(BF16)
        )
    copies[7].wait()
    copies[8].wait()
    return sent


def server_kernel(
    chips, groups, shares,
    rows_ref, own_ref, part_ref, gain_hbm, context_ref, half_ref, gate_hbm, up_hbm, down_hbm,
    out_ref, far_context, far_normed,
    up_all, normed_ref, gate_value, up_value, gate_grad, up_grad, weighted_ref,
    gain_ref, gate_ref, up_ref, down_ref, load_sems, wide_sems, far_sems, core_sems, local_sems,
):
    length, breadth = rows_ref.shape
    hidden = gate_ref.shape[1]
    block = next(b for b in (512, 256, 128, hidden) if hidden % b == 0)
    spans = [slice(at, at + block) for at in range(0, hidden, block)]

    def loads(i, which):
        source, target = ((gate_hbm, gate_ref), (up_hbm, up_ref), (down_hbm, down_ref))[which]
        at = (spans[i], slice(None)) if which == 2 else (slice(None), spans[i])
        return pltpu.make_async_copy(source.at[at], target.at[at], load_sems.at[which, i])

    gain_load = pltpu.make_async_copy(gain_hbm, gain_ref, load_sems.at[3, 0])
    gain_load.start()
    for which in range(3):
        for i in range(len(spans)):
            loads(i, which).start()
    group = lax.axis_index("sdata")
    chip, core = place()
    sibling = {"tensor": chip * CORES + 1 - core}
    greet(
        [sibling, {"sdata": 1 - group}]
        + [{"tensor": turned(chip, k, chips) * CORES + core} for k in range(1, chips)]
    )
    widen = Widen(up_all, [wide_sems.at[i] for i in range(4)], chips)
    count = own_ref.shape[0]
    share = count // groups
    missing = [
        (turned(group, d, groups) * share + i, slice(None))
        for d in range(1, groups)
        for i in range(share)
    ]
    for n, piece in enumerate(missing):
        widen.start(own_ref.at[piece[0]], n, piece)
    others = [
        send(context_ref, far_context, far_sems.at[0], far_sems.at[1], {"sdata": 1 - group})
    ]
    kept = []
    for n in range(shares):
        d = CORES * n + core
        others.append(
            send(half_ref.at[n], far_normed.at[d], core_sems.at[0, n], core_sems.at[1, n], sibling)
        )
        kept.append(pltpu.make_async_copy(half_ref.at[n], far_normed.at[d], local_sems.at[n]))
        kept[-1].start()
    rows_float = rows_ref[...].astype(F32)
    gain_load.wait()
    gain = gain_ref[...].astype(F32)
    inv_rms = lax.rsqrt(jnp.mean(rows_float * rows_float, -1, keepdims=True) + 1e-05)
    normed_ref[...] = (rows_float * inv_rms * gain).astype(BF16)
    for i, span in enumerate(spans):
        loads(i, 0).wait()
        gate_value[:, span] = jnp.dot(normed_ref[...], gate_ref[:, span], preferred_element_type=F32)
        loads(i, 1).wait()
        up_value[:, span] = jnp.dot(normed_ref[...], up_ref[:, span], preferred_element_type=F32)
    for i in range(share):
        up_all[group * share + i] = part_ref[group * share + i]
    for n, piece in enumerate(missing):
        widen.forward(n, piece)
    widen.finish()
    upstream = up_all[...].reshape(length, breadth)
    for i, span in enumerate(spans):
        loads(i, 2).wait()
        pulled = lax.dot_general(upstream, down_ref[span], CROSSED, preferred_element_type=F32)
        gate, up = gate_value[:, span], up_value[:, span]
        sigmoid_gate = jax.nn.sigmoid(gate)
        gate_grad[:, span] = (
            pulled * up * sigmoid_gate * (1.0 + gate * (1.0 - sigmoid_gate))
        ).astype(BF16)
        up_grad[:, span] = (pulled * gate * sigmoid_gate).astype(BF16)
    step = next(b for b in (256, 128, breadth) if breadth % b == 0)
    lean = jnp.zeros((length, 1), F32)
    for at in range(0, breadth, step):
        span = slice(at, at + step)
        weighted = (
            lax.dot_general(gate_grad[...], gate_ref[span], CROSSED, preferred_element_type=F32)
            + lax.dot_general(up_grad[...], up_ref[span], CROSSED, preferred_element_type=F32)
        ) * gain_ref[:, span].astype(F32)
        weighted_ref[:, span] = weighted
        lean = lean + jnp.sum(weighted * rows_ref[:, span].astype(F32), -1, keepdims=True)
    pull = inv_rms**3 * (lean * (1.0 / breadth))
    out_ref[...] = (inv_rms * weighted_ref[...] - rows_ref[...].astype(F32) * pull).astype(BF16)
    for copy in others:
        copy.wait_recv()
    for copy in others:
        copy.wait_send()
    for copy in kept:
        copy.wait()


def server_pull(rows_in, up_own, up_part, gain, context, half, gate_matrix, up_matrix, down_matrix):
    chips, count, groups = axis_counts()
    length, breadth = rows_in.shape
    hidden = gate_matrix.shape[1]
    shares = half.shape[0] if half.ndim == 3 else 0
    full = (count,) + half.shape[1:] if shares else half.shape
    dma = pltpu.SemaphoreType.DMA
    vmem = lambda *sizes: pltpu.VMEM(sizes, BF16)
    wide = lambda *sizes: pltpu.VMEM(sizes, F32)
    return pl.pallas_call(
        partial(server_kernel, chips, groups, shares),
        out_shape=(
            jax.ShapeDtypeStruct((length, breadth), BF16),
            jax.ShapeDtypeStruct(context.shape, BF16),
            jax.ShapeDtypeStruct(full, BF16),
        ),
        in_specs=[VMEM_SPEC] * 3 + [HBM_SPEC] + [VMEM_SPEC] * 2 + [HBM_SPEC] * 3,
        out_specs=(VMEM_SPEC,) * 3,
        scratch_shapes=[
            vmem(count, length // count, breadth), vmem(length, breadth),
            wide(length, hidden), wide(length, hidden), vmem(length, hidden), vmem(length, hidden),
            wide(length, breadth),
            vmem(1, breadth), vmem(breadth, hidden), vmem(breadth, hidden), vmem(hidden, breadth),
            dma((4, hidden // LANES)), dma((4, chips, count)), dma((2,)), dma((2, count)),
            dma((count,)),
        ],
        compiler_params=params(5, 50),
        name="server_pull",
    )(rows_in, up_own, up_part, gain[None], context, half, gate_matrix, up_matrix, down_matrix)


class Chain:
    def __init__(self, own, forth, back, sems, count):
        self.own, self.forth, self.back, self.count = own, forth, back, count
        self.sems = sems
        self.at = lax.axis_index("client")

    def copy(self, way, j, d):
        landing = self.forth if way == 0 else self.back
        to = self.at + 1 if way == 0 else self.at - 1
        return pltpu.make_async_remote_copy(
            src_ref=self.own.at[d],
            dst_ref=landing.at[j],
            send_sem=self.sems.at[2 * way, j],
            recv_sem=self.sems.at[2 * way + 1, j],
            device_id={"client": lax.rem(to + self.count, self.count)},
            device_id_type=MESH,
        )

    def legs(self):
        for j in range(self.count - 1):
            for way in (0, 1):
                d = self.count - 1 - j if way == 0 else j
                end = 0 if way == 0 else self.count - 1
                beyond = self.at < d if way == 0 else self.at > d
                yield way, j, d, end, beyond

    def open(self, d, way):
        j = self.count - 1 - d if way == 0 else d
        end = 0 if way == 0 else self.count - 1
        if abs(d - end) > 1:

            @pl.when(self.at == end)
            def _():
                self.copy(way, j, d).start()

    def add(self, way, j, d):
        landing = self.forth if way == 0 else self.back
        self.copy(way, j, d).wait_recv()
        self.own[d] = (self.own[d].astype(F32) + landing[j].astype(F32)).astype(BF16)

    def relay(self):
        near = self.at < self.count // 2
        legs = list(self.legs())
        turns = [(leg, near) for leg in legs if leg[0] == 0]
        turns += [(leg, self.at >= 0) for leg in legs if leg[0] == 1]
        turns += [(leg, jnp.logical_not(near)) for leg in legs if leg[0] == 0]
        for (way, j, d, end, beyond), now in turns:
            if abs(d - end) < 3:
                continue
            far = self.at < d - 1 if way == 0 else self.at > d + 1

            @pl.when(now & far & (self.at != end))
            def _(way=way, j=j, d=d):
                self.add(way, j, d)
                self.copy(way, j, d).start()

    def close(self, ends):
        last = self.count - 1
        for way, end, d in ((0, 0, self.at + 1), (1, last, self.at - 1)):
            j = last - d if way == 0 else d
            if ends:

                @pl.when(self.at == end)
                def _(way=way, j=j, d=d):
                    self.copy(way, j, d).start()

            else:

                @pl.when((self.at > 0) & (self.at < last))
                def _(way=way, j=j, d=d):
                    self.add(way, j, d)
                    self.copy(way, j, d).start()

    def total(self, out_refs):
        last = self.count - 1
        for way, end, j in ((0, 0, last - self.at), (1, last, self.at)):
            landing = self.forth if way == 0 else self.back

            @pl.when(self.at != end)
            def _(way=way, j=j, landing=landing):
                self.copy(way, j, 0).wait_recv()
                self.own[self.at] = (
                    self.own[self.at].astype(F32) + landing[j].astype(F32)
                ).astype(BF16)

        result = (self.own[self.at].astype(F32) * (1.0 / self.count)).astype(BF16)
        at = 0
        for out in out_refs:
            out[...] = result[:, at : at + out.shape[1]]
            at += out.shape[1]

    def finish(self):
        for way, j, d, end, beyond in self.legs():

            @pl.when(beyond)
            def _(way=way, j=j, d=d):
                self.copy(way, j, d).wait_send()


def learn_kernel(
    kv_count, count, aligned,
    cut_ref, output_ref, query_ref, key_ref, value_ref, context_ref, weights_ref, normed_ref,
    far_normed, far_context, table_ref, *refs,
):
    if not aligned:
        near_cut, give_cut, near_normed, refs = refs[0], refs[1], refs[2], refs[3:]
    query_out, key_out, value_out, output_out = refs[:4]
    (
        pulled, pair, key_turn, value_pair, weight_grad, score_grad, query_grad, shared_grad,
        far_cut, far_query, far_shared,
        output_own, output_forth, output_back, shared_own, shared_forth, shared_back,
        query_own, query_forth, query_back,
        cosine_ref, sine_ref,
        cut_sems, core_sems, give_sems, output_sems, shared_sems, query_sems,
    ) = refs[4:]
    length = cut_ref.shape[0]
    rows = far_cut.shape[2]
    client, group = lax.axis_index("client"), lax.axis_index("sdata")
    tensor_at = lax.axis_index("tensor")
    core = lax.rem(tensor_at, CORES)
    sibling = {"tensor": tensor_at + 1 - 2 * core}
    across = {"sdata": 1 - group}
    ahead = {"client": lax.rem(client + 1, count)}
    behind = {"client": lax.rem(client + count - 1, count)}
    greet([sibling, across, ahead, behind])
    order = []
    for j in range((count + 1) // 2):
        order += [count - 1 - j, j]

    def columns(d, side):
        return pl.ds(pl.multiple_of((2 * d + side) * rows, rows), rows)

    def cut_copy(n, d):
        source = cut_ref.at[:, columns(d, 1 - group)] if aligned else give_cut.at[d]
        return pltpu.make_async_remote_copy(
            src_ref=source, dst_ref=far_cut.at[d],
            send_sem=cut_sems.at[0, n], recv_sem=cut_sems.at[1, n],
            device_id=across, device_id_type=MESH,
        )

    def core_copy(n, d):
        return pltpu.make_async_remote_copy(
            src_ref=far_cut.at[d], dst_ref=far_cut.at[d],
            send_sem=core_sems.at[0, n], recv_sem=core_sems.at[1, n],
            device_id=sibling, device_id_type=MESH,
        )

    halves = count // CORES
    picks = [order[CORES * n] + core * (order[CORES * n + 1] - order[CORES * n]) for n in range(halves)]
    others = [
        order[CORES * n + 1] + core * (order[CORES * n] - order[CORES * n + 1]) for n in range(halves)
    ]
    for n in range(halves):
        cut_copy(n, picks[n]).start()

    width = 2 * LANES if query_ref.shape[1] % (2 * LANES) == 0 else LANES
    for at in range(0, query_ref.shape[1], width):
        pulled[:, at : at + width] = jnp.dot(
            cut_ref[...], output_ref[:, at : at + width], preferred_element_type=F32
        ).astype(BF16)
    keys_float, values_float = key_ref[...].astype(F32), value_ref[...].astype(F32)
    keys_turned = keys_float.T.astype(BF16)
    key_turn[...] = jnp.zeros_like(key_turn)
    score_grad[...] = jnp.zeros_like(score_grad)
    for g in range(kv_count):
        value_pair[g, :length], value_pair[g, length:] = paired(values_float, g)
        mine = keys_turned[g * HEAD_DIM : (g + 1) * HEAD_DIM]
        key_turn[g, :HEAD_DIM, :length] = mine
        key_turn[g, HEAD_DIM:, length:] = mine

    unfold(table_ref[...], cosine_ref, sine_ref)

    def unturn(tile):
        return tile * cosine_ref[...] - swap_halves(tile) * sine_ref[...]

    tiles = query_ref.shape[1] // LANES
    low = lane_tile() < HEAD_DIM
    key_sum, value_sum = [None] * kv_count, [None] * kv_count
    for t in range(tiles):
        g = t * kv_count // tiles
        span = slice(t * LANES, (t + 1) * LANES)
        weight_grad[t % 2] = lax.dot_general(
            value_pair[g], pulled[:, span], CROSSED, preferred_element_type=F32
        )
        for head in range(2):
            base = head * length
            for i in range(0, length, LANES):
                deep = i + LANES
                grad = weight_grad[t % 2, base : base + deep, i : i + LANES].astype(BF16).astype(F32)
                weight = weights_ref[t, base : base + deep, i : i + LANES].astype(F32)
                both = grad * weight
                drift = jnp.sum(both, 0, keepdims=True)
                score_grad[t % 2, base : base + deep, i : i + LANES] = (
                    (both - weight * drift) * HEAD_DIM ** (-0.5)
                ).astype(BF16)
        back_query = jnp.dot(key_turn[g], score_grad[t % 2], preferred_element_type=F32)
        query_grad[:, span] = unturn(back_query.T.astype(BF16).astype(F32)).astype(BF16)
        back_key = jnp.dot(score_grad[t % 2], query_ref[:, span], preferred_element_type=F32)
        back_value = jnp.dot(weights_ref[t], pulled[:, span], preferred_element_type=F32)
        first = key_sum[g] is None
        key_sum[g] = back_key if first else key_sum[g] + back_key
        value_sum[g] = back_value if first else value_sum[g] + back_value

    def folded(sums):
        whole = None
        for g, both in enumerate(sums):
            upper, lower = both[:length], both[length:]
            if g == 0:
                whole = upper + pltpu.roll(lower, HEAD_DIM, 1)
            else:
                whole = jnp.where(low, whole, pltpu.roll(upper, HEAD_DIM, 1) + lower)
        return whole.astype(BF16)

    shared_grad[:, :LANES] = unturn(folded(key_sum).astype(F32)).astype(BF16)
    shared_grad[:, LANES:] = folded(value_sum)

    def give(source, target, i):
        return pltpu.make_async_remote_copy(
            src_ref=source, dst_ref=target, send_sem=give_sems.at[0, i], recv_sem=give_sems.at[1, i],
            device_id=across, device_id_type=MESH,
        )

    gifts = [give(shared_grad, far_shared, 0), give(query_grad, far_query, 1)]
    for gift in gifts:
        gift.start()
    chains = [
        Chain(output_own, output_forth, output_back, output_sems, count),
        Chain(shared_own, shared_forth, shared_back, shared_sems, count),
        Chain(query_own, query_forth, query_back, query_sems, count),
    ]

    def near(d, from_cut):
        if aligned:
            return (cut_ref if from_cut else normed_ref)[:, columns(d, group)]
        return near_cut[d] if from_cut else near_normed[d]

    def product(chain, d, left, right, far_left, far_right):
        chain.own[d] = (
            lax.dot_general(left, right, TALL, preferred_element_type=F32)
            + lax.dot_general(far_left, far_right, TALL, preferred_element_type=F32)
        ).astype(BF16)

    for n in range(halves):
        cut_copy(n, picks[n]).wait_recv()
        core_copy(n, picks[n]).start()
        core_copy(n, others[n]).wait_recv()
        for i in range(CORES):
            d = order[CORES * n + i]
            product(chains[0], d, near(d, True), context_ref[...], far_cut[d], far_context[...])
            for way in (0, 1):
                chains[0].open(d, way)

    def spread(chain, grad, far_grad):
        for d in order:
            product(chain, d, near(d, False), grad[...], far_normed[d], far_grad[...])
            for way in (0, 1):
                chain.open(d, way)

    gifts[0].wait_recv()
    spread(chains[1], shared_grad, far_shared)
    chains[0].relay()
    gifts[1].wait_recv()
    spread(chains[2], query_grad, far_query)
    for chain in chains:
        chain.close(True)
    chains[0].close(False)
    for chain in chains[1:]:
        chain.relay()
        chain.close(False)
    chains[0].total([output_out])
    chains[1].total([key_out, value_out])
    chains[2].total([query_out])
    for n in range(halves):
        cut_copy(n, picks[n]).wait_send()
        core_copy(n, picks[n]).wait_send()
    for gift in gifts:
        gift.wait_send()
    for chain in chains:
        chain.finish()


def learn(cut_grad, output_matrix, saved, normed, far_normed, far_context, table, kv_count):
    unused, count, group_count = axis_counts()
    queries, keys, values, context, weights = saved
    length, breadth = cut_grad.shape
    features = queries.shape[1]
    rows = breadth // (count * group_count)
    aligned = rows % LANES == 0
    dma = pltpu.SemaphoreType.DMA
    shape = lambda *sizes: jax.ShapeDtypeStruct(sizes, BF16)
    vmem = lambda *sizes: pltpu.VMEM(sizes, BF16)
    operands = [cut_grad, output_matrix, queries, keys, values, context, weights, normed]
    operands += [far_normed, far_context, table]
    if not aligned:
        group = lax.axis_index("sdata")
        operands += [
            half_of(cut_grad, count, group), half_of(cut_grad, count, 1 - group),
            half_of(normed, count, group),
        ]
    chain = lambda wide: [
        vmem(count, rows, wide), vmem(count - 1, rows, wide), vmem(count - 1, rows, wide)
    ]
    return pl.pallas_call(
        partial(learn_kernel, kv_count, count, aligned),
        out_shape=(
            shape(rows, features), shape(rows, LANES), shape(rows, LANES), shape(rows, features)
        ),
        in_specs=[VMEM_SPEC] * len(operands),
        out_specs=(VMEM_SPEC,) * 4,
        scratch_shapes=[
            vmem(length, features), vmem(16, LANES), vmem(kv_count, LANES, 2 * length),
            vmem(kv_count, 2 * length, LANES), pltpu.VMEM((2, 2 * length, length), F32),
            vmem(2, 2 * length, length), vmem(length, features), vmem(length, 2 * LANES),
            vmem(count, length, rows), vmem(length, features), vmem(length, 2 * LANES),
        ]
        + chain(features) + chain(2 * LANES) + chain(features)
        + [pltpu.VMEM(table.shape, F32)] * 2
        + [dma((2, count // CORES)), dma((2, count // CORES)), dma((2, 2))]
        + [dma((4, count - 1))] * 3,
        compiler_params=params(3, 28),
        name="learn",
    )(*operands)


def emit_kernel(count, *refs):
    sems = refs[2 * count]
    copies = [
        pltpu.make_async_copy(refs[i], refs[count + i], sems.at[i]) for i in range(count)
    ]
    for copy in copies:
        copy.start()
    for copy in copies:
        copy.wait()


def emit(*arrays):
    count = len(arrays)
    return pl.pallas_call(
        partial(emit_kernel, count),
        out_shape=tuple(jax.ShapeDtypeStruct(a.shape, a.dtype) for a in arrays),
        in_specs=[VMEM_SPEC] * count,
        out_specs=(HBM_SPEC,) * count,
        scratch_shapes=[pltpu.SemaphoreType.DMA((count,))],
        compiler_params=pltpu.CompilerParams(vmem_limit_bytes=4 * 2**20),
        name="emit",
    )(*arrays)


def half_of(array, count, side):
    blocks = array.reshape(array.shape[0], count, 2, -1)
    return lax.dynamic_index_in_dim(blocks, side, 2, False).transpose(1, 0, 2)


def across_groups(array):
    count = lax.axis_size("sdata")
    return lax.ppermute(array, "sdata", [(g, (g + 1) % count) for g in range(count)])


def table_of(length):
    halfway = HEAD_DIM // 2
    lanes = np.arange(HEAD_DIM)
    frequencies = np.exp(-math.log(500000.0) * (2.0 / HEAD_DIM) * (lanes % halfway))
    angles = np.arange(length)[:, None] * frequencies[None, :]
    sign = np.where(lanes < halfway, -1.0, 1.0)
    return jnp.asarray(np.concatenate([np.cos(angles), np.sin(angles) * sign], 1), F32)


def widened(matrix):
    return jnp.pad(matrix, ((0, 0), (0, LANES - matrix.shape[1])))


def relay_back(assigned, pulled, up_own):
    chips, client_count, group_count = axis_counts()
    length, breadth = pulled.shape
    chunk, width = length // client_count, breadth // (CORES * chips)
    share = client_count // group_count
    parts = len(parts_of(chunk))
    full = (client_count, chunk, breadth)
    own = (client_count, chunk, width)
    dma = pltpu.SemaphoreType.DMA
    vmem = lambda shape: pltpu.VMEM(shape, BF16)
    grad = pl.pallas_call(
        partial(back_kernel, chips, client_count, group_count),
        out_shape=jax.ShapeDtypeStruct(full, BF16),
        in_specs=[SMEM_SPEC, VMEM_SPEC, VMEM_SPEC],
        out_specs=VMEM_SPEC,
        scratch_shapes=[
            vmem((chips,) + own), vmem((chips,) + own), vmem((chips,) + own),
            vmem((group_count, share, chunk, width)), vmem(own), vmem(own),
            dma((4, chips, parts * client_count)), dma((2, parts, group_count, share)),
            dma((2, parts, client_count)), dma((4, chips, parts * client_count)),
        ]
        + [vmem((client_count, chunk // parts, width))] * parts,
        compiler_params=params(2, 14),
        name="relay_back",
    )(assigned, pulled.reshape(full), up_own)
    return grad.reshape(length, breadth)


def local(
    client_input,
    client_gain,
    query_weight,
    key_weight,
    client_value_weight,
    output_weight,
    server_gain,
    server_gate,
    server_up,
    server_down,
    upstream,
    assignment,
):
    client_count = lax.axis_size("client")
    shared = key_weight.shape[2]
    kv_count = shared // HEAD_DIM
    table = table_of(client_input.shape[0])
    matrices = [
        query_weight[0], widened(key_weight[0]), widened(client_value_weight[0]), output_weight[0]
    ]
    normed, half, *saved, cut_rows, up_own, up_part = depart(
        assignment, client_input, client_gain, table, upstream, matrices, kv_count
    )
    cut_rows = cut_rows.reshape(client_input.shape)
    pulled, far_context, far_normed = server_pull(
        cut_rows, up_own, up_part, server_gain[0], saved[3], half,
        server_gate[0], server_up[0], server_down[0],
    )
    if half.ndim == 2:
        far_normed = across_groups(half_of(normed, client_count, 1 - lax.axis_index("sdata")))
    arriving_grad = relay_back(assignment, pulled, up_own)
    query_update, key_update, value_update, output_update = emit(
        *learn(
            arriving_grad, output_weight[0], saved, normed, far_normed, far_context, table,
            kv_count,
        )
    )
    return (query_update, key_update[:, :shared], value_update[:, :shared], output_update)


def solution(mesh):
    placed = (
        P(("client", "sdata"), None),
        P("client", None),
        P("client", None, "tensor"),
        P("client", None, "tensor"),
        P("client", None, "tensor"),
        P("client", None, "tensor"),
        P("sdata", None),
        P("sdata", None, "tensor"),
        P("sdata", None, "tensor"),
        P("sdata", "tensor", None),
        P(("client", "sdata"), None),
        P(),
    )
    return jax.shard_map(
        local,
        mesh=mesh,
        in_specs=placed,
        out_specs=(
            P(("client", "sdata"), "tensor"),
            P(("client", "sdata"), "tensor"),
            P(("client", "sdata"), "tensor"),
            P(("client", "sdata"), "tensor"),
        ),
        check_vma=False,
    )
```

```python
from functools import partial
import math

import jax
import jax.numpy as jnp
import numpy as np
from jax import lax
from jax.experimental import pallas as pl
from jax.experimental.pallas import tpu as pltpu
from jax.sharding import PartitionSpec as P

HEAD_DIM = 64
MESH = pl.DeviceIdType.MESH
CORES = 2
LANES = 128
BF16 = jnp.bfloat16
F32 = jnp.float32


def lane_tile(flag_ref=None):
    return lax.broadcasted_iota(jnp.int32, (1, LANES), 1)


def swap_halves(tile):
    low = lax.rem(lane_tile(), HEAD_DIM) < HEAD_DIM // 2
    ahead = pltpu.roll(tile, LANES - HEAD_DIM // 2, 1)
    behind = pltpu.roll(tile, HEAD_DIM // 2, 1)
    return jnp.where(low, ahead, behind)


def unfold(table, cosine_ref, sine_ref):
    low = lane_tile() < HEAD_DIM
    moved = pltpu.roll(table, HEAD_DIM, 1)
    cosine_ref[...] = jnp.where(low, table, moved)
    sine_ref[...] = jnp.where(low, moved, table)


def paired(tile, at):
    low = lane_tile() < HEAD_DIM
    moved = pltpu.roll(tile, HEAD_DIM, 1)
    first, second = (tile, moved) if at == 0 else (moved, tile)
    zero = jnp.zeros_like(tile)
    return jnp.where(low, first, zero).astype(BF16), jnp.where(low, zero, second).astype(BF16)


CROSSED = (((1,), (1,)), ((), ()))
TALL = (((0,), (0,)), ((), ()))


VMEM_SPEC = pl.BlockSpec(memory_space=pltpu.VMEM)
HBM_SPEC = pl.BlockSpec(memory_space=pltpu.HBM)
SMEM_SPEC = pl.BlockSpec(memory_space=pltpu.SMEM)


def params(number, mebibytes):
    return pltpu.CompilerParams(
        collective_id=number, has_side_effects=True, vmem_limit_bytes=mebibytes * 2**20
    )


def axis_counts():
    return lax.axis_size("tensor") // CORES, lax.axis_size("client"), lax.axis_size("sdata")


def greet(others):
    barrier = pltpu.get_barrier_semaphore()
    for other in others:
        pl.semaphore_signal(barrier, inc=1, device_id=other, device_id_type=MESH)
    pl.semaphore_wait(barrier, len(others))


def send(source, target, send_sem, recv_sem, device):
    copy = pltpu.make_async_remote_copy(
        src_ref=source,
        dst_ref=target,
        send_sem=send_sem,
        recv_sem=recv_sem,
        device_id=device,
        device_id_type=MESH,
    )
    copy.start()
    return copy


def place():
    tensor_at = lax.axis_index("tensor")
    return tensor_at // CORES, lax.rem(tensor_at, CORES)


def turned(index, step, count):
    return lax.rem(index + step, count)


def columns_of(chip, core, width):
    return pl.ds(pl.multiple_of((chip * CORES + core) * width, width), width)


def partners(chips, client_count, group_count):
    chip, core = place()
    client, group = lax.axis_index("client"), lax.axis_index("sdata")
    others = [{"tensor": chip * CORES + 1 - core}]
    others += [{"tensor": turned(chip, k, chips) * CORES + core} for k in range(1, chips)]
    others += [{"client": turned(client, k, client_count)} for k in range(1, client_count)]
    others += [{"sdata": turned(group, k, group_count)} for k in range(1, group_count)]
    return others


class ShareSum:
    def __init__(self, part, pair, relay, landed, sems, pieces, chips):
        self.part, self.pair, self.relay, self.landed = part, pair, relay, landed
        self.pair_send, self.pair_recv, self.chip_send, self.chip_recv = sems
        self.chips, self.width = chips, part.shape[-1] // (CORES * chips)
        self.chip, self.core = place()
        self.pair_copies = {}
        self.chip_copies = {}
        self.pieces = pieces

    def give(self, k):
        to = turned(self.chip, k, self.chips)
        for n, (q, rows) in enumerate(self.pieces):
            self.pair_copies[k, n] = send(
                self.part.at[q, rows, columns_of(to, 1 - self.core, self.width)],
                self.pair.at[k, q, rows],
                self.pair_send.at[k, n],
                self.pair_recv.at[k, n],
                {"tensor": self.chip * CORES + 1 - self.core},
            )

    def hand_on(self, k):
        to = turned(self.chip, k, self.chips)
        for n, (q, rows) in enumerate(self.pieces):
            self.pair_copies[k, n].wait_recv()
            self.relay[k, q, rows] = (
                self.part[q, rows, columns_of(to, self.core, self.width)].astype(F32)
                + self.pair[k, q, rows].astype(F32)
            ).astype(BF16)
            self.chip_copies[k, n] = send(
                self.relay.at[k, q, rows],
                self.landed.at[k, q, rows],
                self.chip_send.at[k, n],
                self.chip_recv.at[k, n],
                {"tensor": to * CORES + self.core},
            )

    def fill(self, make):
        for k in range(1, self.chips):
            make(turned(self.chip, k, self.chips), 1 - self.core)
            self.give(k)
        for k in range(1, self.chips):
            make(turned(self.chip, k, self.chips), self.core)
            self.hand_on(k)
        make(self.chip, 1 - self.core)
        self.give(0)
        make(self.chip, self.core)

    def get(self, n, piece):
        q, rows = piece
        self.pair_copies[0, n].wait_recv()
        total = self.part[q, rows, columns_of(self.chip, self.core, self.width)].astype(
            F32
        ) + self.pair[0, q, rows].astype(F32)
        for k in range(1, self.chips):
            self.chip_copies[k, n].wait_recv()
            total = total + self.landed[k, q, rows].astype(F32)
        return total

    def finish(self):
        for copy in list(self.pair_copies.values()) + list(self.chip_copies.values()):
            copy.wait_send()


class Widen:
    def __init__(self, out, sems, chips):
        self.out, self.chips = out, chips
        self.chip_send, self.chip_recv, self.pair_send, self.pair_recv = sems
        self.chip, self.core = place()
        self.width = out.shape[-1] // (CORES * chips)
        self.forwarded, self.chip_copies = [], {}

    def spot(self, piece, k):
        q, rows = piece
        at = turned(self.chip, self.chips - k, self.chips)
        return q, rows, columns_of(at, self.core, self.width)

    def pair_copy(self, source, k, n, piece):
        self.forwarded.append(
            send(
                source,
                self.out.at[self.spot(piece, k)],
                self.pair_send.at[k, n],
                self.pair_recv.at[k, n],
                {"tensor": self.chip * CORES + 1 - self.core},
            )
        )

    def start(self, source, n, piece):
        spot = self.spot(piece, 0)
        for k in range(1, self.chips):
            self.chip_copies[k, n] = send(
                source,
                self.out.at[spot],
                self.chip_send.at[k, n],
                self.chip_recv.at[k, n],
                {"tensor": turned(self.chip, k, self.chips) * CORES + self.core},
            )
        self.pair_copy(source, 0, n, piece)
        self.out[spot] = source[...]

    def forward(self, n, piece):
        for k in range(1, self.chips):
            self.chip_copies[k, n].wait_recv()
            self.pair_copy(self.out.at[self.spot(piece, k)], k, n, piece)

    def finish(self):
        for copy in self.forwarded:
            copy.wait_recv()
        for copy in self.forwarded + list(self.chip_copies.values()):
            copy.wait_send()


PARTS = 2


def parts_of(chunk):
    parts = PARTS if chunk % (16 * PARTS) == 0 else 1
    return [slice(p * chunk // parts, (p + 1) * chunk // parts) for p in range(parts)]


def out_kernel(
    chips, client_count, group_count,
    order, sent, copies, project, part, inputs, up_at,
    cut_out, up_own, up_all,
    pair, relay, landed, cut_from, up_put, cut_put, cut_own,
    tp_sems, z_sems, y_sems, up_sems, wide_sems, kept_sems, *cut_at,
):
    client, group = lax.axis_index("client"), lax.axis_index("sdata")
    share = client_count // group_count
    chunk = part.shape[1]
    parts = parts_of(chunk)
    steps = list(range(1, client_count)) + [0]
    pieces = [(turned(client, k, client_count), rows) for rows in parts for k in steps]
    sums = ShareSum(part, pair, relay, landed, [tp_sems.at[i] for i in range(4)], pieces, chips)
    sums.fill(project)
    for copy in copies:
        copy.wait()
    for copy in sent:
        copy.wait_recv()
    up_copies = []
    for d in range(1, group_count):
        to = turned(group, d, group_count)
        for i in range(share):
            up_put[d, i] = up_at[order(to * share + i)]
            up_copies.append(
                send(
                    up_put.at[d, i], up_own.at[group * share + i],
                    up_sems.at[0, d, i], up_sems.at[1, d, i], {"sdata": to},
                )
            )
    kept = Widen(up_all, [kept_sems.at[i] for i in range(4)], chips)
    for i in range(share):
        q = group * share + i
        up_own[q] = up_at[order(q)]
        kept.start(up_own.at[q], i, (q, slice(None)))
    cut_z = []
    for n, piece in enumerate(pieces):
        p, k = n // client_count, steps[n % client_count]
        to, rows = piece
        block = (sums.get(n, piece) + inputs[to, rows].astype(F32)).astype(BF16)
        if k == 0:
            cut_at[p][client] = block
        else:
            cut_from[k, rows] = block
            cut_z.append(
                (
                    p,
                    send(
                        cut_from.at[k, rows], cut_at[p].at[client],
                        z_sems.at[0, p, k], z_sems.at[1, p, k], {"client": to},
                    ),
                )
            )
    widen = Widen(cut_out, [wide_sems.at[i] for i in range(4)], chips)
    rounds, y_copies = [], []

    def widen_piece(q, rows):
        widen.start(cut_own.at[q, rows], len(rounds), (q, rows))
        rounds.append((q, rows))

    for p, rows in enumerate(parts):
        for which, copy in cut_z:
            if which == p:
                copy.wait_recv()
        for d in range(1, group_count):
            to = turned(group, d, group_count)
            for i in range(share):
                cut_put[d, i, rows] = cut_at[p][order(to * share + i)]
                y_copies.append(
                    (
                        send(
                            cut_put.at[d, i, rows], cut_own.at[group * share + i, rows],
                            y_sems.at[0, p, d, i], y_sems.at[1, p, d, i], {"sdata": to},
                        ),
                        turned(group, group_count - d, group_count) * share + i,
                        rows,
                    )
                )
        for i in range(share):
            q = group * share + i
            cut_own[q, rows] = cut_at[p][order(group * share + i)]
            widen_piece(q, rows)
    for copy, q, rows in y_copies:
        copy.wait_recv()
        widen_piece(q, rows)
    for i in range(share):
        kept.forward(i, (group * share + i, slice(None)))
    for n, piece in enumerate(rounds):
        widen.forward(n, piece)
    widen.finish()
    kept.finish()
    sums.finish()
    for copy in up_copies:
        copy.wait_recv()
    for copy in sent + up_copies + [c for unused, c in cut_z] + [c for c, unused, also in y_copies]:
        copy.wait_send()


def ranked(assigned, c, at):
    total = 0
    for j in range(c):
        before = (assigned[j] < assigned[at]) | ((assigned[j] == assigned[at]) & (j < at))
        total = total + jnp.where(before, 1, 0)
    return total


def depart_kernel(kv_count, sends_half, chips, count, groups, assigned, *refs):
    ins, outs = refs[:9], refs[9:16]
    cut_out, up_own, up_all = refs[16:19]
    attended, up_at, inputs = refs[19:22]
    fore, rest = refs[22:38], refs[38:]
    sent, copies, project = forward_kernel(
        kv_count, sends_half, chips, count, *ins, *outs, attended, up_at, inputs, *fore
    )
    ranks = [ranked(assigned, count, c) for c in range(count)]

    def order(at):
        return sum(jnp.where(rank == at, c, 0) for c, rank in enumerate(ranks))

    out_kernel(
        chips, count, groups, order, sent, copies, project, attended, inputs, up_at, cut_out, up_own, up_all, *rest
    )


def depart(assigned, rows_in, gain, table, upstream, matrices, kv_count):
    chips, count, groups = axis_counts()
    length, breadth = rows_in.shape
    features, shared = matrices[0].shape[1], matrices[1].shape[1]
    tiles = features // LANES
    rows = breadth // (2 * count)
    sends_half = rows % LANES == 0
    shape = lambda *sizes: jax.ShapeDtypeStruct(sizes, BF16)
    half = (count // CORES, length, rows) if sends_half else (16, LANES)
    chunk, width = length // count, breadth // (CORES * chips)
    share, parts = count // groups, len(parts_of(chunk))
    full, own = (count, chunk, breadth), (count, chunk, width)
    dma = pltpu.SemaphoreType.DMA
    vmem = lambda sizes: pltpu.VMEM(sizes, BF16)
    return pl.pallas_call(
        partial(depart_kernel, kv_count, sends_half, chips, count, groups),
        out_shape=(
            shape(length, breadth), shape(*half), shape(length, features), shape(length, shared),
            shape(length, shared), shape(length, features), shape(tiles, 2 * length, length),
            shape(*full), shape(*own), shape(*full),
        ),
        in_specs=[SMEM_SPEC] + [HBM_SPEC] * 9,
        out_specs=(VMEM_SPEC,) * 10,
        scratch_shapes=[vmem(full), vmem(own), vmem(own), vmem(rows_in.shape), vmem(gain.shape)]
        + [pltpu.VMEM(table.shape, F32)] * 3
        + [vmem(m.shape) for m in matrices]
        + [
            pltpu.VMEM((2, 2 * length, length), F32), vmem((kv_count, 2 * length, LANES)),
            vmem((kv_count, LANES, 2 * length)), vmem(half),
            dma((9,)), dma((2, count)), dma((2, count)),
            vmem((chips,) + own), vmem((chips,) + own), vmem((chips,) + own), vmem(own),
            vmem((groups, share, chunk, width)), vmem((groups, share, chunk, width)), vmem(own),
            dma((4, chips, parts * count)), dma((2, parts, count)),
            dma((2, parts, groups, share)), dma((2, groups, share)),
            dma((4, chips, parts * count)), dma((4, chips, share)),
        ]
        + [vmem((count, chunk // parts, width))] * parts,
        compiler_params=params(1, 52),
        name="depart",
    )(
        assigned, rows_in, gain, table, upstream.reshape(full), rows_in.reshape(full), *matrices
    )


def back_kernel(
    chips, client_count, group_count, pull,
    assigned, part, up_own,
    grad_out,
    pair, relay, landed, y_from, z_from, own,
    tp_sems, y_sems, z_sems, wide_sems, *y_at,
):
    client, group = lax.axis_index("client"), lax.axis_index("sdata")
    share = client_count // group_count
    parts = parts_of(part.shape[1])
    steps = [(d, i) for d in list(range(1, group_count)) + [0] for i in range(share)]
    pieces = [
        (turned(group, d, group_count) * share + i, rows) for rows in parts for d, i in steps
    ]
    sums = ShareSum(part, pair, relay, landed, [tp_sems.at[i] for i in range(4)], pieces, chips)
    sums.fill(pull)
    widen = Widen(grad_out, [wide_sems.at[i] for i in range(4)], chips)
    y_copies, z_copies, rounds = [], [], []

    def widen_piece(q, rows):
        widen.start(own.at[q, rows], len(rounds), (q, rows))
        rounds.append((q, rows))

    for p, rows in enumerate(parts):
        arrivals = []
        for at, (d, i) in enumerate(steps):
            n = p * len(steps) + at
            q = pieces[n][0]
            block = (sums.get(n, (q, rows)) + up_own[q, rows].astype(F32)).astype(BF16)
            if d == 0:
                y_at[p][group * share + i] = block
            else:
                y_from[d, i, rows] = block
                arrivals.append(
                    send(
                        y_from.at[d, i, rows], y_at[p].at[group * share + i],
                        y_sems.at[0, p, d, i], y_sems.at[1, p, d, i],
                        {"sdata": turned(group, d, group_count)},
                    )
                )
        for copy in arrivals:
            copy.wait_recv()
        y_copies += arrivals
        for k in range(1, client_count):
            to = turned(client, k, client_count)
            z_from[k, rows] = y_at[p][ranked(assigned, client_count, to)]
            z_copies.append(
                (
                    send(
                        z_from.at[k, rows], own.at[client, rows],
                        z_sems.at[0, p, k], z_sems.at[1, p, k], {"client": to},
                    ),
                    turned(client, client_count - k, client_count),
                    rows,
                )
            )
        own[client, rows] = y_at[p][ranked(assigned, client_count, client)]
        widen_piece(client, rows)
    for copy, source, rows in z_copies:
        copy.wait_recv()
        widen_piece(source, rows)
    for n, piece in enumerate(rounds):
        widen.forward(n, piece)
    widen.finish()
    sums.finish()
    for copy in y_copies + [c for c, unused, also in z_copies]:
        copy.wait_send()


def forward_kernel(
    kv_count, sends_half, chips, count,
    rows_hbm, gain_hbm, table_hbm, upstream_hbm, inputs_hbm,
    query_hbm, key_hbm, value_hbm, output_hbm,
    normed_out, far_out, query_out, key_out, value_out, context_out, weights_out,
    attended_out, up_out, inputs_out,
    rows_ref, gain_ref, table_ref, cosine_ref, sine_ref,
    query_mat, key_mat, value_mat, output_mat, scores, key_pair, value_turn, theirs,
    sems, z_sems, y_sems,
):
    length = rows_ref.shape[0]
    client, group = lax.axis_index("client"), lax.axis_index("sdata")
    chip, core = place()
    chunk, width = up_out.shape[1:]
    moves = (
        (rows_hbm, rows_ref), (table_hbm, table_ref), (gain_hbm, gain_ref),
        (query_hbm, query_mat), (key_hbm, key_mat), (value_hbm, value_mat), (output_hbm, output_mat),
        (upstream_hbm.at[client, :, columns_of(chip, core, width)], up_out.at[client]),
        (inputs_hbm.at[:, :, columns_of(chip, core, width)], inputs_out),
    )
    copies = []
    for i, (source, target) in enumerate(moves):
        copies.append(pltpu.make_async_copy(source, target, sems.at[i]))
        copies[-1].start()
    greet(partners(chips, count, lax.axis_size("sdata")))
    sent = []
    for k in range(1, count):
        to = turned(client, k, count)
        sent.append(
            send(
                upstream_hbm.at[to, :, columns_of(chip, core, width)], up_out.at[client],
                z_sems.at[0, k], z_sems.at[1, k], {"client": to},
            )
        )
    copies[0].wait()
    copies[2].wait()
    rows_float = rows_ref[...].astype(F32)
    inv_rms = lax.rsqrt(jnp.mean(rows_float * rows_float, -1, keepdims=True) + 1e-05)
    normed_out[...] = (rows_float * inv_rms * gain_ref[...].astype(F32)).astype(BF16)
    if sends_half:
        wide = far_out.shape[2]
        for n in range(count // CORES):
            d = CORES * n + core
            at = pl.ds(pl.multiple_of((2 * d + 1 - group) * wide, wide), wide)
            theirs[n] = normed_out[:, at]
            sent.append(
                send(
                    theirs.at[n], far_out.at[n], y_sems.at[0, n], y_sems.at[1, n],
                    {"sdata": 1 - group},
                )
            )
    normed = normed_out[...]
    copies[1].wait()
    unfold(table_ref[...], cosine_ref, sine_ref)

    def turn(tile):
        return tile * cosine_ref[...] + swap_halves(tile) * sine_ref[...]

    copies[3].wait()
    wide = 2 * LANES
    for at in range(0, query_mat.shape[1], wide):
        part = jnp.dot(normed, query_mat[:, at : at + wide], preferred_element_type=F32)
        for side in (0, LANES):
            query_out[:, at + side : at + side + LANES] = turn(part[:, side : side + LANES]).astype(BF16)
    copies[4].wait()
    keys = turn(jnp.dot(normed, key_mat[...], preferred_element_type=F32)).astype(BF16)
    key_out[...] = keys
    copies[5].wait()
    values = jnp.dot(normed, value_mat[...], preferred_element_type=F32).astype(BF16)
    value_out[...] = values
    keys_float, values_float = keys.astype(F32), values.astype(F32)
    values_turned = values_float.T.astype(BF16)
    value_turn[...] = jnp.zeros_like(value_turn)
    for g in range(kv_count):
        key_pair[g, :length], key_pair[g, length:] = paired(keys_float, g)
        mine = values_turned[g * HEAD_DIM : (g + 1) * HEAD_DIM]
        value_turn[g, :HEAD_DIM, :length] = mine
        value_turn[g, HEAD_DIM:, length:] = mine
    tiles = query_mat.shape[1] // LANES
    step = LANES
    for t in range(tiles):
        g = t * kv_count // tiles
        scores[t % 2] = lax.dot_general(
            key_pair[g], query_out[:, t * LANES : (t + 1) * LANES], CROSSED, preferred_element_type=F32
        )
        for head in range(2):
            base = head * length
            for i in range(0, length, step):
                deep = i + step
                block = scores[t % 2, base : base + deep, i : i + step] * HEAD_DIM ** (-0.5)
                key_ids = lax.broadcasted_iota(jnp.int32, (deep, step), 0)
                query_ids = lax.broadcasted_iota(jnp.int32, (deep, step), 1) + i
                block = jnp.where(key_ids <= query_ids, block, -1e30)
                exponent = jnp.exp(block - jnp.max(block, 0, keepdims=True))
                share = 1.0 / jnp.sum(exponent, 0, keepdims=True)
                weights_out[t, base : base + deep, i : i + step] = (exponent * share).astype(BF16)
                if deep < length:
                    weights_out[t, base + deep : base + length, i : i + step] = jnp.zeros(
                        (length - deep, step), BF16
                    )
        turned_context = jnp.dot(value_turn[g], weights_out[t], preferred_element_type=F32)
        context_out[:, t * LANES : (t + 1) * LANES] = turned_context.T.astype(BF16)
    copies[6].wait()
    context = context_out[...]

    def project(to, side):
        cols = columns_of(to, side, width)
        attended_out[:, :, cols] = (
            lax.dot_general(context, output_mat[cols, :], CROSSED, preferred_element_type=F32)
            .reshape(count, chunk, width)
            .astype(BF16)
        )

    return sent, copies[7:], project


def server_kernel(
    chips, groups, shares,
    rows_ref, own_ref, part_ref, gain_hbm, context_ref, half_ref, gate_hbm, up_hbm, down_hbm,
    assigned, grad_out, far_context, far_normed,
    up_all, normed_ref, gate_value, up_value, gate_grad, up_grad, pulled_ref,
    gain_ref, gate_ref, up_ref, down_ref, load_sems, wide_sems, far_sems, core_sems, local_sems, *rest,
):
    length, breadth = rows_ref.shape
    hidden = gate_ref.shape[1]
    block = next(b for b in (512, 256, 128, hidden) if hidden % b == 0)
    spans = [slice(at, at + block) for at in range(0, hidden, block)]

    def loads(i, which):
        source, target = ((gate_hbm, gate_ref), (up_hbm, up_ref), (down_hbm, down_ref))[which]
        at = (spans[i], slice(None)) if which == 2 else (slice(None), spans[i])
        return pltpu.make_async_copy(source.at[at], target.at[at], load_sems.at[which, i])

    gain_load = pltpu.make_async_copy(gain_hbm, gain_ref, load_sems.at[3, 0])
    gain_load.start()
    for which in range(3):
        for i in range(len(spans)):
            loads(i, which).start()
    group = lax.axis_index("sdata")
    chip, core = place()
    sibling = {"tensor": chip * CORES + 1 - core}
    greet(partners(chips, lax.axis_size("client"), groups))
    widen = Widen(up_all, [wide_sems.at[i] for i in range(4)], chips)
    count = own_ref.shape[0]
    share = count // groups
    missing = [
        (turned(group, d, groups) * share + i, slice(None))
        for d in range(1, groups)
        for i in range(share)
    ]
    for n, piece in enumerate(missing):
        widen.start(own_ref.at[piece[0]], n, piece)
    others = [
        send(context_ref, far_context, far_sems.at[0], far_sems.at[1], {"sdata": 1 - group})
    ]
    kept = []
    for n in range(shares):
        d = CORES * n + core
        others.append(
            send(half_ref.at[n], far_normed.at[d], core_sems.at[0, n], core_sems.at[1, n], sibling)
        )
        kept.append(pltpu.make_async_copy(half_ref.at[n], far_normed.at[d], local_sems.at[n]))
        kept[-1].start()
    rows_float = rows_ref[...].astype(F32)
    gain_load.wait()
    gain = gain_ref[...].astype(F32)
    inv_rms = lax.rsqrt(jnp.mean(rows_float * rows_float, -1, keepdims=True) + 1e-05)
    normed_ref[...] = (rows_float * inv_rms * gain).astype(BF16)
    for i, span in enumerate(spans):
        loads(i, 0).wait()
        gate_value[:, span] = jnp.dot(normed_ref[...], gate_ref[:, span], preferred_element_type=F32)
        loads(i, 1).wait()
        up_value[:, span] = jnp.dot(normed_ref[...], up_ref[:, span], preferred_element_type=F32)
    for i in range(share):
        up_all[group * share + i] = part_ref[group * share + i]
    for n, piece in enumerate(missing):
        widen.forward(n, piece)
    widen.finish()
    upstream = up_all[...].reshape(length, breadth)
    lean = jnp.zeros((length, 1), F32)
    for i, span in enumerate(spans):
        loads(i, 2).wait()
        pulled = lax.dot_general(upstream, down_ref[span], CROSSED, preferred_element_type=F32)
        gate, up = gate_value[:, span], up_value[:, span]
        sigmoid_gate = jax.nn.sigmoid(gate)
        gate_part = (
            pulled * up * sigmoid_gate * (1.0 + gate * (1.0 - sigmoid_gate))
        ).astype(BF16)
        up_part = (pulled * gate * sigmoid_gate).astype(BF16)
        gate_grad[:, span], up_grad[:, span] = gate_part, up_part
        lean = lean + jnp.sum(
            gate_part.astype(F32) * gate + up_part.astype(F32) * up, -1, keepdims=True
        )
    lean = inv_rms**2 * (lean * (1.0 / breadth))
    width = own_ref.shape[2]
    chunk = own_ref.shape[1]
    step = min(256, width)

    def pull(to, side):
        for at in range(0, width, step):
            span = pl.ds(pl.multiple_of((to * CORES + side) * width + at, step), step)
            weighted = (
                lax.dot_general(gate_grad[...], gate_ref[span, :], CROSSED, preferred_element_type=F32)
                + lax.dot_general(up_grad[...], up_ref[span, :], CROSSED, preferred_element_type=F32)
            ) * gain_ref[:, span].astype(F32)
            mine = inv_rms * weighted - rows_ref[:, span].astype(F32) * lean
            pulled_ref[:, :, span] = mine.reshape(count, chunk, step).astype(BF16)

    back_kernel(
        chips, lax.axis_size("client"), groups, pull, assigned, pulled_ref, own_ref, grad_out, *rest
    )
    for copy in others:
        copy.wait_recv()
    for copy in others:
        copy.wait_send()
    for copy in kept:
        copy.wait()


def serve(assigned, rows_in, up_own, up_part, gain, context, half, gate_matrix, up_matrix, down_matrix):
    chips, count, groups = axis_counts()
    length, breadth = rows_in.shape
    hidden = gate_matrix.shape[1]
    shares = half.shape[0] if half.ndim == 3 else 0
    far = (count,) + half.shape[1:] if shares else half.shape
    chunk, width = length // count, breadth // (CORES * chips)
    share, parts = count // groups, len(parts_of(chunk))
    full, own = (count, chunk, breadth), (count, chunk, width)
    dma = pltpu.SemaphoreType.DMA
    vmem = lambda *sizes: pltpu.VMEM(sizes, BF16)
    wide = lambda *sizes: pltpu.VMEM(sizes, F32)
    return pl.pallas_call(
        partial(server_kernel, chips, groups, shares),
        out_shape=(
            jax.ShapeDtypeStruct(full, BF16),
            jax.ShapeDtypeStruct(context.shape, BF16),
            jax.ShapeDtypeStruct(far, BF16),
        ),
        in_specs=[VMEM_SPEC] * 3 + [HBM_SPEC] + [VMEM_SPEC] * 2 + [HBM_SPEC] * 3 + [SMEM_SPEC],
        out_specs=(VMEM_SPEC,) * 3,
        scratch_shapes=[
            vmem(*full), vmem(length, breadth),
            wide(length, hidden), wide(length, hidden), vmem(length, hidden), vmem(length, hidden),
            vmem(*full),
            vmem(1, breadth), vmem(breadth, hidden), vmem(breadth, hidden), vmem(hidden, breadth),
            dma((4, hidden // LANES)), dma((4, chips, count)), dma((2,)), dma((2, count)),
            dma((count,)),
            vmem(chips, *own), vmem(chips, *own), vmem(chips, *own),
            vmem(groups, share, chunk, width), vmem(*own), vmem(*own),
            dma((4, chips, parts * count)), dma((2, parts, groups, share)),
            dma((2, parts, count)), dma((4, chips, parts * count)),
        ]
        + [vmem(count, chunk // parts, width)] * parts,
        compiler_params=params(5, 50),
        name="serve",
    )(
        rows_in, up_own, up_part, gain[None], context, half, gate_matrix, up_matrix, down_matrix,
        assigned,
    )


class Chain:
    def __init__(self, own, forth, back, sems, count):
        self.own, self.forth, self.back, self.count = own, forth, back, count
        self.sems = sems
        self.at = lax.axis_index("client")

    def copy(self, way, j, d):
        landing = self.forth if way == 0 else self.back
        to = self.at + 1 if way == 0 else self.at - 1
        return pltpu.make_async_remote_copy(
            src_ref=self.own.at[d],
            dst_ref=landing.at[j],
            send_sem=self.sems.at[2 * way, j],
            recv_sem=self.sems.at[2 * way + 1, j],
            device_id={"client": lax.rem(to + self.count, self.count)},
            device_id_type=MESH,
        )

    def legs(self):
        for j in range(self.count - 1):
            for way in (0, 1):
                d = self.count - 1 - j if way == 0 else j
                end = 0 if way == 0 else self.count - 1
                beyond = self.at < d if way == 0 else self.at > d
                yield way, j, d, end, beyond

    def open(self, d, way):
        j = self.count - 1 - d if way == 0 else d
        end = 0 if way == 0 else self.count - 1
        if abs(d - end) > 1:

            @pl.when(self.at == end)
            def _():
                self.copy(way, j, d).start()

    def add(self, way, j, d):
        landing = self.forth if way == 0 else self.back
        self.copy(way, j, d).wait_recv()
        self.own[d] = (self.own[d].astype(F32) + landing[j].astype(F32)).astype(BF16)

    def relay(self):
        near = self.at < self.count // 2
        legs = list(self.legs())
        turns = [(leg, near) for leg in legs if leg[0] == 0]
        turns += [(leg, self.at >= 0) for leg in legs if leg[0] == 1]
        turns += [(leg, jnp.logical_not(near)) for leg in legs if leg[0] == 0]
        for (way, j, d, end, beyond), now in turns:
            if abs(d - end) < 3:
                continue
            far = self.at < d - 1 if way == 0 else self.at > d + 1

            @pl.when(now & far & (self.at != end))
            def _(way=way, j=j, d=d):
                self.add(way, j, d)
                self.copy(way, j, d).start()

    def close(self, ends):
        last = self.count - 1
        for way, end, d in ((0, 0, self.at + 1), (1, last, self.at - 1)):
            j = last - d if way == 0 else d
            if ends:

                @pl.when(self.at == end)
                def _(way=way, j=j, d=d):
                    self.copy(way, j, d).start()

            else:

                @pl.when((self.at > 0) & (self.at < last))
                def _(way=way, j=j, d=d):
                    self.add(way, j, d)
                    self.copy(way, j, d).start()

    def total(self, out_refs):
        last = self.count - 1
        for way, end, j in ((0, 0, last - self.at), (1, last, self.at)):
            landing = self.forth if way == 0 else self.back

            @pl.when(self.at != end)
            def _(way=way, j=j, landing=landing):
                self.copy(way, j, 0).wait_recv()
                self.own[self.at] = (
                    self.own[self.at].astype(F32) + landing[j].astype(F32)
                ).astype(BF16)

        result = (self.own[self.at].astype(F32) * (1.0 / self.count)).astype(BF16)
        at = 0
        for out in out_refs:
            out[...] = result[:, at : at + out.shape[1]]
            at += out.shape[1]

    def finish(self):
        for way, j, d, end, beyond in self.legs():

            @pl.when(beyond)
            def _(way=way, j=j, d=d):
                self.copy(way, j, d).wait_send()


def learn_kernel(
    kv_count, count, aligned,
    cut_ref, output_ref, query_ref, key_ref, value_ref, context_ref, weights_ref, normed_ref,
    far_normed, far_context, table_ref, *refs,
):
    if not aligned:
        near_cut, give_cut, near_normed, refs = refs[0], refs[1], refs[2], refs[3:]
    query_out, key_out, value_out, output_out = refs[:4]
    (
        pulled, pair, key_turn, value_pair, weight_grad, score_grad, query_grad, shared_grad,
        far_cut, far_query, far_shared,
        output_own, output_forth, output_back, shared_own, shared_forth, shared_back,
        query_own, query_forth, query_back,
        cosine_ref, sine_ref,
        cut_sems, core_sems, give_sems, output_sems, shared_sems, query_sems,
    ) = refs[4:]
    length = cut_ref.shape[0]
    rows = far_cut.shape[2]
    client, group = lax.axis_index("client"), lax.axis_index("sdata")
    tensor_at = lax.axis_index("tensor")
    core = lax.rem(tensor_at, CORES)
    sibling = {"tensor": tensor_at + 1 - 2 * core}
    across = {"sdata": 1 - group}
    ahead = {"client": lax.rem(client + 1, count)}
    behind = {"client": lax.rem(client + count - 1, count)}
    greet([sibling, across, ahead, behind])
    order = []
    for j in range((count + 1) // 2):
        order += [count - 1 - j, j]

    def columns(d, side):
        return pl.ds(pl.multiple_of((2 * d + side) * rows, rows), rows)

    def cut_copy(n, d):
        source = cut_ref.at[:, columns(d, 1 - group)] if aligned else give_cut.at[d]
        return pltpu.make_async_remote_copy(
            src_ref=source, dst_ref=far_cut.at[d],
            send_sem=cut_sems.at[0, n], recv_sem=cut_sems.at[1, n],
            device_id=across, device_id_type=MESH,
        )

    def core_copy(n, d):
        return pltpu.make_async_remote_copy(
            src_ref=far_cut.at[d], dst_ref=far_cut.at[d],
            send_sem=core_sems.at[0, n], recv_sem=core_sems.at[1, n],
            device_id=sibling, device_id_type=MESH,
        )

    halves = count // CORES
    picks = [order[CORES * n] + core * (order[CORES * n + 1] - order[CORES * n]) for n in range(halves)]
    others = [
        order[CORES * n + 1] + core * (order[CORES * n] - order[CORES * n + 1]) for n in range(halves)
    ]
    for n in range(halves):
        cut_copy(n, picks[n]).start()

    width = 2 * LANES if query_ref.shape[1] % (2 * LANES) == 0 else LANES
    for at in range(0, query_ref.shape[1], width):
        pulled[:, at : at + width] = jnp.dot(
            cut_ref[...], output_ref[:, at : at + width], preferred_element_type=F32
        ).astype(BF16)
    keys_float, values_float = key_ref[...].astype(F32), value_ref[...].astype(F32)
    keys_turned = keys_float.T.astype(BF16)
    key_turn[...] = jnp.zeros_like(key_turn)
    score_grad[...] = jnp.zeros_like(score_grad)
    for g in range(kv_count):
        value_pair[g, :length], value_pair[g, length:] = paired(values_float, g)
        mine = keys_turned[g * HEAD_DIM : (g + 1) * HEAD_DIM]
        key_turn[g, :HEAD_DIM, :length] = mine
        key_turn[g, HEAD_DIM:, length:] = mine

    unfold(table_ref[...], cosine_ref, sine_ref)

    def unturn(tile):
        return tile * cosine_ref[...] - swap_halves(tile) * sine_ref[...]

    tiles = query_ref.shape[1] // LANES
    low = lane_tile() < HEAD_DIM
    key_sum, value_sum = [None] * kv_count, [None] * kv_count
    for t in range(tiles):
        g = t * kv_count // tiles
        span = slice(t * LANES, (t + 1) * LANES)
        weight_grad[t % 2] = lax.dot_general(
            value_pair[g], pulled[:, span], CROSSED, preferred_element_type=F32
        )
        for head in range(2):
            base = head * length
            for i in range(0, length, LANES):
                deep = i + LANES
                grad = weight_grad[t % 2, base : base + deep, i : i + LANES].astype(BF16).astype(F32)
                weight = weights_ref[t, base : base + deep, i : i + LANES].astype(F32)
                both = grad * weight
                drift = jnp.sum(both, 0, keepdims=True)
                score_grad[t % 2, base : base + deep, i : i + LANES] = (
                    (both - weight * drift) * HEAD_DIM ** (-0.5)
                ).astype(BF16)
        back_query = jnp.dot(key_turn[g], score_grad[t % 2], preferred_element_type=F32)
        query_grad[:, span] = unturn(back_query.T.astype(BF16).astype(F32)).astype(BF16)
        back_key = jnp.dot(score_grad[t % 2], query_ref[:, span], preferred_element_type=F32)
        back_value = jnp.dot(weights_ref[t], pulled[:, span], preferred_element_type=F32)
        first = key_sum[g] is None
        key_sum[g] = back_key if first else key_sum[g] + back_key
        value_sum[g] = back_value if first else value_sum[g] + back_value

    def folded(sums):
        whole = None
        for g, both in enumerate(sums):
            upper, lower = both[:length], both[length:]
            if g == 0:
                whole = upper + pltpu.roll(lower, HEAD_DIM, 1)
            else:
                whole = jnp.where(low, whole, pltpu.roll(upper, HEAD_DIM, 1) + lower)
        return whole.astype(BF16)

    shared_grad[:, :LANES] = unturn(folded(key_sum).astype(F32)).astype(BF16)
    shared_grad[:, LANES:] = folded(value_sum)

    def give(source, target, i):
        return pltpu.make_async_remote_copy(
            src_ref=source, dst_ref=target, send_sem=give_sems.at[0, i], recv_sem=give_sems.at[1, i],
            device_id=across, device_id_type=MESH,
        )

    gifts = [give(shared_grad, far_shared, 0), give(query_grad, far_query, 1)]
    for gift in gifts:
        gift.start()
    chains = [
        Chain(output_own, output_forth, output_back, output_sems, count),
        Chain(shared_own, shared_forth, shared_back, shared_sems, count),
        Chain(query_own, query_forth, query_back, query_sems, count),
    ]

    def near(d, from_cut):
        if aligned:
            return (cut_ref if from_cut else normed_ref)[:, columns(d, group)]
        return near_cut[d] if from_cut else near_normed[d]

    def product(chain, d, left, right, far_left, far_right):
        chain.own[d] = (
            lax.dot_general(left, right, TALL, preferred_element_type=F32)
            + lax.dot_general(far_left, far_right, TALL, preferred_element_type=F32)
        ).astype(BF16)

    for n in range(halves):
        cut_copy(n, picks[n]).wait_recv()
        core_copy(n, picks[n]).start()
        core_copy(n, others[n]).wait_recv()
        for i in range(CORES):
            d = order[CORES * n + i]
            product(chains[0], d, near(d, True), context_ref[...], far_cut[d], far_context[...])
            for way in (0, 1):
                chains[0].open(d, way)

    def spread(chain, grad, far_grad):
        for d in order:
            product(chain, d, near(d, False), grad[...], far_normed[d], far_grad[...])
            for way in (0, 1):
                chain.open(d, way)

    gifts[0].wait_recv()
    spread(chains[1], shared_grad, far_shared)
    chains[0].relay()
    gifts[1].wait_recv()
    spread(chains[2], query_grad, far_query)
    for chain in chains:
        chain.close(True)
    chains[0].close(False)
    for chain in chains[1:]:
        chain.relay()
        chain.close(False)
    chains[0].total([output_out])
    chains[1].total([key_out, value_out])
    chains[2].total([query_out])
    for n in range(halves):
        cut_copy(n, picks[n]).wait_send()
        core_copy(n, picks[n]).wait_send()
    for gift in gifts:
        gift.wait_send()
    for chain in chains:
        chain.finish()


def learn(cut_grad, output_matrix, saved, normed, far_normed, far_context, table, kv_count):
    unused, count, group_count = axis_counts()
    queries, keys, values, context, weights = saved
    length, breadth = cut_grad.shape
    features = queries.shape[1]
    rows = breadth // (count * group_count)
    aligned = rows % LANES == 0
    dma = pltpu.SemaphoreType.DMA
    shape = lambda *sizes: jax.ShapeDtypeStruct(sizes, BF16)
    vmem = lambda *sizes: pltpu.VMEM(sizes, BF16)
    operands = [cut_grad, output_matrix, queries, keys, values, context, weights, normed]
    operands += [far_normed, far_context, table]
    if not aligned:
        group = lax.axis_index("sdata")
        operands += [
            half_of(cut_grad, count, group), half_of(cut_grad, count, 1 - group),
            half_of(normed, count, group),
        ]
    chain = lambda wide: [
        vmem(count, rows, wide), vmem(count - 1, rows, wide), vmem(count - 1, rows, wide)
    ]
    return pl.pallas_call(
        partial(learn_kernel, kv_count, count, aligned),
        out_shape=(
            shape(rows, features), shape(rows, LANES), shape(rows, LANES), shape(rows, features)
        ),
        in_specs=[VMEM_SPEC] * len(operands),
        out_specs=(VMEM_SPEC,) * 4,
        scratch_shapes=[
            vmem(length, features), vmem(16, LANES), vmem(kv_count, LANES, 2 * length),
            vmem(kv_count, 2 * length, LANES), pltpu.VMEM((2, 2 * length, length), F32),
            vmem(2, 2 * length, length), vmem(length, features), vmem(length, 2 * LANES),
            vmem(count, length, rows), vmem(length, features), vmem(length, 2 * LANES),
        ]
        + chain(features) + chain(2 * LANES) + chain(features)
        + [pltpu.VMEM(table.shape, F32)] * 2
        + [dma((2, count // CORES)), dma((2, count // CORES)), dma((2, 2))]
        + [dma((4, count - 1))] * 3,
        compiler_params=params(3, 28),
        name="learn",
    )(*operands)


def emit_kernel(count, *refs):
    sems = refs[2 * count]
    copies = [
        pltpu.make_async_copy(refs[i], refs[count + i], sems.at[i]) for i in range(count)
    ]
    for copy in copies:
        copy.start()
    for copy in copies:
        copy.wait()


def emit(*arrays):
    count = len(arrays)
    return pl.pallas_call(
        partial(emit_kernel, count),
        out_shape=tuple(jax.ShapeDtypeStruct(a.shape, a.dtype) for a in arrays),
        in_specs=[VMEM_SPEC] * count,
        out_specs=(HBM_SPEC,) * count,
        scratch_shapes=[pltpu.SemaphoreType.DMA((count,))],
        compiler_params=pltpu.CompilerParams(vmem_limit_bytes=4 * 2**20),
        name="emit",
    )(*arrays)


def half_of(array, count, side):
    blocks = array.reshape(array.shape[0], count, 2, -1)
    return lax.dynamic_index_in_dim(blocks, side, 2, False).transpose(1, 0, 2)


def across_groups(array):
    count = lax.axis_size("sdata")
    return lax.ppermute(array, "sdata", [(g, (g + 1) % count) for g in range(count)])


def table_of(length):
    halfway = HEAD_DIM // 2
    lanes = np.arange(HEAD_DIM)
    frequencies = np.exp(-math.log(500000.0) * (2.0 / HEAD_DIM) * (lanes % halfway))
    angles = np.arange(length)[:, None] * frequencies[None, :]
    sign = np.where(lanes < halfway, -1.0, 1.0)
    return jnp.asarray(np.concatenate([np.cos(angles), np.sin(angles) * sign], 1), F32)


def widened(matrix):
    return jnp.pad(matrix, ((0, 0), (0, LANES - matrix.shape[1])))


def local(
    client_input,
    client_gain,
    query_weight,
    key_weight,
    client_value_weight,
    output_weight,
    server_gain,
    server_gate,
    server_up,
    server_down,
    upstream,
    assignment,
):
    client_count = lax.axis_size("client")
    shared = key_weight.shape[2]
    kv_count = shared // HEAD_DIM
    table = table_of(client_input.shape[0])
    matrices = [
        query_weight[0], widened(key_weight[0]), widened(client_value_weight[0]), output_weight[0]
    ]
    normed, half, *saved, cut_rows, up_own, up_part = depart(
        assignment, client_input, client_gain, table, upstream, matrices, kv_count
    )
    cut_rows = cut_rows.reshape(client_input.shape)
    arriving_grad, far_context, far_normed = serve(
        assignment, cut_rows, up_own, up_part, server_gain[0], saved[3], half,
        server_gate[0], server_up[0], server_down[0],
    )
    arriving_grad = arriving_grad.reshape(client_input.shape)
    if half.ndim == 2:
        far_normed = across_groups(half_of(normed, client_count, 1 - lax.axis_index("sdata")))
    query_update, key_update, value_update, output_update = emit(
        *learn(
            arriving_grad, output_weight[0], saved, normed, far_normed, far_context, table,
            kv_count,
        )
    )
    return (query_update, key_update[:, :shared], value_update[:, :shared], output_update)


def solution(mesh):
    placed = (
        P(("client", "sdata"), None),
        P("client", None),
        P("client", None, "tensor"),
        P("client", None, "tensor"),
        P("client", None, "tensor"),
        P("client", None, "tensor"),
        P("sdata", None),
        P("sdata", None, "tensor"),
        P("sdata", None, "tensor"),
        P("sdata", "tensor", None),
        P(("client", "sdata"), None),
        P(),
    )
    return jax.shard_map(
        local,
        mesh=mesh,
        in_specs=placed,
        out_specs=(
            P(("client", "sdata"), "tensor"),
            P(("client", "sdata"), "tensor"),
            P(("client", "sdata"), "tensor"),
            P(("client", "sdata"), "tensor"),
        ),
        check_vma=False,
    )
```

```python
from functools import partial
import math

import jax
import jax.numpy as jnp
import numpy as np
from jax import lax
from jax.experimental import pallas as pl
from jax.experimental.pallas import tpu as pltpu
from jax.sharding import PartitionSpec as P

HEAD_DIM = 64
MESH = pl.DeviceIdType.MESH
CORES = 2
LANES = 128
BF16 = jnp.bfloat16
F32 = jnp.float32


def lane_tile(flag_ref=None):
    return lax.broadcasted_iota(jnp.int32, (1, LANES), 1)


def swap_halves(tile):
    low = lax.rem(lane_tile(), HEAD_DIM) < HEAD_DIM // 2
    ahead = pltpu.roll(tile, LANES - HEAD_DIM // 2, 1)
    behind = pltpu.roll(tile, HEAD_DIM // 2, 1)
    return jnp.where(low, ahead, behind)


def unfold(table, cosine_ref, sine_ref):
    low = lane_tile() < HEAD_DIM
    moved = pltpu.roll(table, HEAD_DIM, 1)
    cosine_ref[...] = jnp.where(low, table, moved)
    sine_ref[...] = jnp.where(low, moved, table)


def paired(tile, at):
    low = lane_tile() < HEAD_DIM
    moved = pltpu.roll(tile, HEAD_DIM, 1)
    first, second = (tile, moved) if at == 0 else (moved, tile)
    zero = jnp.zeros_like(tile)
    return jnp.where(low, first, zero).astype(BF16), jnp.where(low, zero, second).astype(BF16)


CROSSED = (((1,), (1,)), ((), ()))
TALL = (((0,), (0,)), ((), ()))


VMEM_SPEC = pl.BlockSpec(memory_space=pltpu.VMEM)
HBM_SPEC = pl.BlockSpec(memory_space=pltpu.HBM)
SMEM_SPEC = pl.BlockSpec(memory_space=pltpu.SMEM)


def params(number, mebibytes):
    return pltpu.CompilerParams(
        collective_id=number, has_side_effects=True, vmem_limit_bytes=mebibytes * 2**20
    )


def axis_counts():
    return lax.axis_size("tensor") // CORES, lax.axis_size("client"), lax.axis_size("sdata")


def greet(others):
    barrier = pltpu.get_barrier_semaphore()
    for other in others:
        pl.semaphore_signal(barrier, inc=1, device_id=other, device_id_type=MESH)
    pl.semaphore_wait(barrier, len(others))


def send(source, target, send_sem, recv_sem, device):
    copy = pltpu.make_async_remote_copy(
        src_ref=source,
        dst_ref=target,
        send_sem=send_sem,
        recv_sem=recv_sem,
        device_id=device,
        device_id_type=MESH,
    )
    copy.start()
    return copy


def place():
    tensor_at = lax.axis_index("tensor")
    return tensor_at // CORES, lax.rem(tensor_at, CORES)


def turned(index, step, count):
    return lax.rem(index + step, count)


def columns_of(chip, core, width):
    return pl.ds(pl.multiple_of((chip * CORES + core) * width, width), width)


def partners(chips, client_count, group_count):
    chip, core = place()
    client, group = lax.axis_index("client"), lax.axis_index("sdata")
    others = [{"tensor": chip * CORES + 1 - core}]
    others += [{"tensor": turned(chip, k, chips) * CORES + core} for k in range(1, chips)]
    others += [{"client": turned(client, k, client_count)} for k in range(1, client_count)]
    others += [{"sdata": turned(group, k, group_count)} for k in range(1, group_count)]
    return others


class ShareSum:
    def __init__(self, part, pair, relay, landed, sems, pieces, chips):
        self.part, self.pair, self.relay, self.landed = part, pair, relay, landed
        self.pair_send, self.pair_recv, self.chip_send, self.chip_recv = sems
        self.chips, self.width = chips, part.shape[-1] // (CORES * chips)
        self.chip, self.core = place()
        self.pair_copies = {}
        self.chip_copies = {}
        self.pieces = pieces

    def give(self, k):
        to = turned(self.chip, k, self.chips)
        for n, (q, rows) in enumerate(self.pieces):
            self.pair_copies[k, n] = send(
                self.part.at[q, rows, columns_of(to, 1 - self.core, self.width)],
                self.pair.at[k, q, rows],
                self.pair_send.at[k, n],
                self.pair_recv.at[k, n],
                {"tensor": self.chip * CORES + 1 - self.core},
            )

    def hand_on(self, k):
        to = turned(self.chip, k, self.chips)
        for n, (q, rows) in enumerate(self.pieces):
            self.pair_copies[k, n].wait_recv()
            self.relay[k, q, rows] = (
                self.part[q, rows, columns_of(to, self.core, self.width)].astype(F32)
                + self.pair[k, q, rows].astype(F32)
            ).astype(BF16)
            self.chip_copies[k, n] = send(
                self.relay.at[k, q, rows],
                self.landed.at[k, q, rows],
                self.chip_send.at[k, n],
                self.chip_recv.at[k, n],
                {"tensor": to * CORES + self.core},
            )

    def fill(self, make):
        for k in range(1, self.chips):
            make(turned(self.chip, k, self.chips), 1 - self.core)
            self.give(k)
        for k in range(1, self.chips):
            make(turned(self.chip, k, self.chips), self.core)
            self.hand_on(k)
        make(self.chip, 1 - self.core)
        self.give(0)
        make(self.chip, self.core)

    def get(self, n, piece):
        q, rows = piece
        self.pair_copies[0, n].wait_recv()
        total = self.part[q, rows, columns_of(self.chip, self.core, self.width)].astype(
            F32
        ) + self.pair[0, q, rows].astype(F32)
        for k in range(1, self.chips):
            self.chip_copies[k, n].wait_recv()
            total = total + self.landed[k, q, rows].astype(F32)
        return total

    def finish(self):
        for copy in list(self.pair_copies.values()) + list(self.chip_copies.values()):
            copy.wait_send()


class Widen:
    def __init__(self, out, sems, chips):
        self.out, self.chips = out, chips
        self.chip_send, self.chip_recv, self.pair_send, self.pair_recv = sems
        self.chip, self.core = place()
        self.width = out.shape[-1] // (CORES * chips)
        self.forwarded, self.chip_copies = [], {}

    def spot(self, piece, k):
        q, rows = piece
        at = turned(self.chip, self.chips - k, self.chips)
        return q, rows, columns_of(at, self.core, self.width)

    def pair_copy(self, source, k, n, piece):
        self.forwarded.append(
            send(
                source,
                self.out.at[self.spot(piece, k)],
                self.pair_send.at[k, n],
                self.pair_recv.at[k, n],
                {"tensor": self.chip * CORES + 1 - self.core},
            )
        )

    def start(self, source, n, piece):
        spot = self.spot(piece, 0)
        for k in range(1, self.chips):
            self.chip_copies[k, n] = send(
                source,
                self.out.at[spot],
                self.chip_send.at[k, n],
                self.chip_recv.at[k, n],
                {"tensor": turned(self.chip, k, self.chips) * CORES + self.core},
            )
        self.pair_copy(source, 0, n, piece)
        self.out[spot] = source[...]

    def forward(self, n, piece):
        for k in range(1, self.chips):
            self.chip_copies[k, n].wait_recv()
            self.pair_copy(self.out.at[self.spot(piece, k)], k, n, piece)

    def finish(self):
        for copy in self.forwarded:
            copy.wait_recv()
        for copy in self.forwarded + list(self.chip_copies.values()):
            copy.wait_send()


PARTS = 2


def parts_of(chunk):
    parts = PARTS if chunk % (16 * PARTS) == 0 else 1
    return [slice(p * chunk // parts, (p + 1) * chunk // parts) for p in range(parts)]


def out_kernel(
    chips, client_count, group_count,
    order, sent, copies, project, part, inputs, up_at,
    cut_out, up_own, up_all,
    pair, relay, landed, cut_from, up_put, cut_put, cut_own,
    tp_sems, z_sems, y_sems, up_sems, wide_sems, kept_sems, *cut_at,
):
    client, group = lax.axis_index("client"), lax.axis_index("sdata")
    share = client_count // group_count
    chunk = part.shape[1]
    parts = parts_of(chunk)
    steps = list(range(1, client_count)) + [0]
    pieces = [(turned(client, k, client_count), rows) for rows in parts for k in steps]
    sums = ShareSum(part, pair, relay, landed, [tp_sems.at[i] for i in range(4)], pieces, chips)
    sums.fill(project)
    for copy in copies:
        copy.wait()
    for copy in sent:
        copy.wait_recv()
    up_copies = []
    for d in range(1, group_count):
        to = turned(group, d, group_count)
        for i in range(share):
            up_put[d, i] = up_at[order(to * share + i)]
            up_copies.append(
                send(
                    up_put.at[d, i], up_own.at[group * share + i],
                    up_sems.at[0, d, i], up_sems.at[1, d, i], {"sdata": to},
                )
            )
    kept = Widen(up_all, [kept_sems.at[i] for i in range(4)], chips)
    for i in range(share):
        q = group * share + i
        up_own[q] = up_at[order(q)]
        kept.start(up_own.at[q], i, (q, slice(None)))
    cut_z = []
    for n, piece in enumerate(pieces):
        p, k = n // client_count, steps[n % client_count]
        to, rows = piece
        block = (sums.get(n, piece) + inputs[to, rows].astype(F32)).astype(BF16)
        if k == 0:
            cut_at[p][client] = block
        else:
            cut_from[k, rows] = block
            cut_z.append(
                (
                    p,
                    send(
                        cut_from.at[k, rows], cut_at[p].at[client],
                        z_sems.at[0, p, k], z_sems.at[1, p, k], {"client": to},
                    ),
                )
            )
    widen = Widen(cut_out, [wide_sems.at[i] for i in range(4)], chips)
    rounds, y_copies = [], []

    def widen_piece(q, rows):
        widen.start(cut_own.at[q, rows], len(rounds), (q, rows))
        rounds.append((q, rows))

    for p, rows in enumerate(parts):
        for which, copy in cut_z:
            if which == p:
                copy.wait_recv()
        for d in range(1, group_count):
            to = turned(group, d, group_count)
            for i in range(share):
                cut_put[d, i, rows] = cut_at[p][order(to * share + i)]
                y_copies.append(
                    (
                        send(
                            cut_put.at[d, i, rows], cut_own.at[group * share + i, rows],
                            y_sems.at[0, p, d, i], y_sems.at[1, p, d, i], {"sdata": to},
                        ),
                        turned(group, group_count - d, group_count) * share + i,
                        rows,
                    )
                )
        for i in range(share):
            q = group * share + i
            cut_own[q, rows] = cut_at[p][order(group * share + i)]
            widen_piece(q, rows)
    for copy, q, rows in y_copies:
        copy.wait_recv()
        widen_piece(q, rows)
    for i in range(share):
        kept.forward(i, (group * share + i, slice(None)))
    for n, piece in enumerate(rounds):
        widen.forward(n, piece)
    widen.finish()
    kept.finish()
    sums.finish()
    for copy in up_copies:
        copy.wait_recv()
    for copy in sent + up_copies + [c for unused, c in cut_z] + [c for c, unused, also in y_copies]:
        copy.wait_send()


def ranked(assigned, c, at):
    total = 0
    for j in range(c):
        before = (assigned[j] < assigned[at]) | ((assigned[j] == assigned[at]) & (j < at))
        total = total + jnp.where(before, 1, 0)
    return total


def depart_kernel(kv_count, sends_half, chips, count, groups, assigned, *refs):
    ins, outs = refs[:9], refs[9:16]
    cut_out, up_own, up_all = refs[16:19]
    attended, up_at, inputs = refs[19:22]
    fore, rest = refs[22:38], refs[38:]
    sent, copies, project = forward_kernel(
        kv_count, sends_half, chips, count, *ins, *outs, attended, up_at, inputs, *fore
    )
    ranks = [ranked(assigned, count, c) for c in range(count)]

    def order(at):
        return sum(jnp.where(rank == at, c, 0) for c, rank in enumerate(ranks))

    out_kernel(
        chips, count, groups, order, sent, copies, project, attended, inputs, up_at, cut_out, up_own, up_all, *rest
    )


def depart(assigned, rows_in, gain, table, upstream, matrices, kv_count):
    chips, count, groups = axis_counts()
    length, breadth = rows_in.shape
    features, shared = matrices[0].shape[1], matrices[1].shape[1]
    tiles = features // LANES
    rows = breadth // (2 * count)
    sends_half = rows % LANES == 0
    shape = lambda *sizes: jax.ShapeDtypeStruct(sizes, BF16)
    half = (count // CORES, length, rows) if sends_half else (16, LANES)
    chunk, width = length // count, breadth // (CORES * chips)
    share, parts = count // groups, len(parts_of(chunk))
    full, own = (count, chunk, breadth), (count, chunk, width)
    dma = pltpu.SemaphoreType.DMA
    vmem = lambda sizes: pltpu.VMEM(sizes, BF16)
    return pl.pallas_call(
        partial(depart_kernel, kv_count, sends_half, chips, count, groups),
        out_shape=(
            shape(length, breadth), shape(*half), shape(length, features), shape(length, shared),
            shape(length, shared), shape(length, features), shape(tiles, 2 * length, length),
            shape(*full), shape(*own), shape(*full),
        ),
        in_specs=[SMEM_SPEC] + [HBM_SPEC] * 9,
        out_specs=(VMEM_SPEC,) * 10,
        scratch_shapes=[vmem(full), vmem(own), vmem(own), vmem(rows_in.shape), vmem(gain.shape)]
        + [pltpu.VMEM(table.shape, F32)] * 3
        + [vmem(m.shape) for m in matrices]
        + [
            pltpu.VMEM((2, 2 * length, length), F32), vmem((kv_count, 2 * length, LANES)),
            vmem((kv_count, LANES, 2 * length)), vmem(half),
            dma((9,)), dma((2, count)), dma((2, count)),
            vmem((chips,) + own), vmem((chips,) + own), vmem((chips,) + own), vmem(own),
            vmem((groups, share, chunk, width)), vmem((groups, share, chunk, width)), vmem(own),
            dma((4, chips, parts * count)), dma((2, parts, count)),
            dma((2, parts, groups, share)), dma((2, groups, share)),
            dma((4, chips, parts * count)), dma((4, chips, share)),
        ]
        + [vmem((count, chunk // parts, width))] * parts,
        compiler_params=params(1, 52),
        name="depart",
    )(
        assigned, rows_in, gain, table, upstream.reshape(full), rows_in.reshape(full), *matrices
    )


def back_kernel(
    chips, client_count, group_count, pull,
    assigned, part, up_own,
    grad_out,
    pair, relay, landed, y_from, z_from, own,
    tp_sems, y_sems, z_sems, wide_sems, *y_at,
):
    client, group = lax.axis_index("client"), lax.axis_index("sdata")
    share = client_count // group_count
    parts = parts_of(part.shape[1])
    steps = [(d, i) for d in list(range(1, group_count)) + [0] for i in range(share)]
    pieces = [
        (turned(group, d, group_count) * share + i, rows) for rows in parts for d, i in steps
    ]
    sums = ShareSum(part, pair, relay, landed, [tp_sems.at[i] for i in range(4)], pieces, chips)
    sums.fill(pull)
    widen = Widen(grad_out, [wide_sems.at[i] for i in range(4)], chips)
    y_copies, z_copies, rounds = [], [], []

    def widen_piece(q, rows):
        widen.start(own.at[q, rows], len(rounds), (q, rows))
        rounds.append((q, rows))

    for p, rows in enumerate(parts):
        arrivals = []
        for at, (d, i) in enumerate(steps):
            n = p * len(steps) + at
            q = pieces[n][0]
            block = (sums.get(n, (q, rows)) + up_own[q, rows].astype(F32)).astype(BF16)
            if d == 0:
                y_at[p][group * share + i] = block
            else:
                y_from[d, i, rows] = block
                arrivals.append(
                    send(
                        y_from.at[d, i, rows], y_at[p].at[group * share + i],
                        y_sems.at[0, p, d, i], y_sems.at[1, p, d, i],
                        {"sdata": turned(group, d, group_count)},
                    )
                )
        for copy in arrivals:
            copy.wait_recv()
        y_copies += arrivals
        for k in range(1, client_count):
            to = turned(client, k, client_count)
            z_from[k, rows] = y_at[p][ranked(assigned, client_count, to)]
            z_copies.append(
                (
                    send(
                        z_from.at[k, rows], own.at[client, rows],
                        z_sems.at[0, p, k], z_sems.at[1, p, k], {"client": to},
                    ),
                    turned(client, client_count - k, client_count),
                    rows,
                )
            )
        own[client, rows] = y_at[p][ranked(assigned, client_count, client)]
        widen_piece(client, rows)
    for copy, source, rows in z_copies:
        copy.wait_recv()
        widen_piece(source, rows)
    for n, piece in enumerate(rounds):
        widen.forward(n, piece)
    widen.finish()
    sums.finish()
    for copy in y_copies + [c for c, unused, also in z_copies]:
        copy.wait_send()


def forward_kernel(
    kv_count, sends_half, chips, count,
    rows_hbm, gain_hbm, table_hbm, upstream_hbm, inputs_hbm,
    query_hbm, key_hbm, value_hbm, output_hbm,
    normed_out, far_out, query_out, key_out, value_out, context_out, weights_out,
    attended_out, up_out, inputs_out,
    rows_ref, gain_ref, table_ref, cosine_ref, sine_ref,
    query_mat, key_mat, value_mat, output_mat, scores, key_pair, value_turn, theirs,
    sems, z_sems, y_sems,
):
    length = rows_ref.shape[0]
    client, group = lax.axis_index("client"), lax.axis_index("sdata")
    chip, core = place()
    chunk, width = up_out.shape[1:]
    moves = (
        (rows_hbm, rows_ref), (table_hbm, table_ref), (gain_hbm, gain_ref),
        (query_hbm, query_mat), (key_hbm, key_mat), (value_hbm, value_mat), (output_hbm, output_mat),
        (upstream_hbm.at[client, :, columns_of(chip, core, width)], up_out.at[client]),
        (inputs_hbm.at[:, :, columns_of(chip, core, width)], inputs_out),
    )
    copies = []
    for i, (source, target) in enumerate(moves):
        copies.append(pltpu.make_async_copy(source, target, sems.at[i]))
        copies[-1].start()
    greet(partners(chips, count, lax.axis_size("sdata")))
    sent = []
    for k in range(1, count):
        to = turned(client, k, count)
        sent.append(
            send(
                upstream_hbm.at[to, :, columns_of(chip, core, width)], up_out.at[client],
                z_sems.at[0, k], z_sems.at[1, k], {"client": to},
            )
        )
    copies[0].wait()
    copies[2].wait()
    rows_float = rows_ref[...].astype(F32)
    inv_rms = lax.rsqrt(jnp.mean(rows_float * rows_float, -1, keepdims=True) + 1e-05)
    normed_out[...] = (rows_float * inv_rms * gain_ref[...].astype(F32)).astype(BF16)
    if sends_half:
        wide = far_out.shape[2]
        for n in range(count // CORES):
            d = CORES * n + core
            at = pl.ds(pl.multiple_of((2 * d + 1 - group) * wide, wide), wide)
            theirs[n] = normed_out[:, at]
            sent.append(
                send(
                    theirs.at[n], far_out.at[n], y_sems.at[0, n], y_sems.at[1, n],
                    {"sdata": 1 - group},
                )
            )
    normed = normed_out[...]
    copies[1].wait()
    unfold(table_ref[...], cosine_ref, sine_ref)

    def turn(tile):
        return tile * cosine_ref[...] + swap_halves(tile) * sine_ref[...]

    copies[3].wait()
    wide = 2 * LANES
    for at in range(0, query_mat.shape[1], wide):
        part = jnp.dot(normed, query_mat[:, at : at + wide], preferred_element_type=F32)
        for side in (0, LANES):
            query_out[:, at + side : at + side + LANES] = turn(part[:, side : side + LANES]).astype(BF16)
    copies[4].wait()
    keys = turn(jnp.dot(normed, key_mat[...], preferred_element_type=F32)).astype(BF16)
    key_out[...] = keys
    copies[5].wait()
    values = jnp.dot(normed, value_mat[...], preferred_element_type=F32).astype(BF16)
    value_out[...] = values
    keys_float, values_float = keys.astype(F32), values.astype(F32)
    values_turned = values_float.T.astype(BF16)
    value_turn[...] = jnp.zeros_like(value_turn)
    for g in range(kv_count):
        key_pair[g, :length], key_pair[g, length:] = paired(keys_float, g)
        mine = values_turned[g * HEAD_DIM : (g + 1) * HEAD_DIM]
        value_turn[g, :HEAD_DIM, :length] = mine
        value_turn[g, HEAD_DIM:, length:] = mine
    tiles = query_mat.shape[1] // LANES
    step = LANES
    for t in range(tiles):
        g = t * kv_count // tiles
        scores[t % 2] = lax.dot_general(
            key_pair[g], query_out[:, t * LANES : (t + 1) * LANES], CROSSED, preferred_element_type=F32
        )
        for head in range(2):
            base = head * length
            for i in range(0, length, step):
                deep = i + step
                block = scores[t % 2, base : base + deep, i : i + step] * HEAD_DIM ** (-0.5)
                key_ids = lax.broadcasted_iota(jnp.int32, (deep, step), 0)
                query_ids = lax.broadcasted_iota(jnp.int32, (deep, step), 1) + i
                block = jnp.where(key_ids <= query_ids, block, -1e30)
                exponent = jnp.exp(block - jnp.max(block, 0, keepdims=True))
                share = 1.0 / jnp.sum(exponent, 0, keepdims=True)
                weights_out[t, base : base + deep, i : i + step] = (exponent * share).astype(BF16)
                if deep < length:
                    weights_out[t, base + deep : base + length, i : i + step] = jnp.zeros(
                        (length - deep, step), BF16
                    )
        turned_context = jnp.dot(value_turn[g], weights_out[t], preferred_element_type=F32)
        context_out[:, t * LANES : (t + 1) * LANES] = turned_context.T.astype(BF16)
    copies[6].wait()
    context = context_out[...]

    def project(to, side):
        cols = columns_of(to, side, width)
        attended_out[:, :, cols] = (
            lax.dot_general(context, output_mat[cols, :], CROSSED, preferred_element_type=F32)
            .reshape(count, chunk, width)
            .astype(BF16)
        )

    return sent, copies[7:], project


def server_kernel(
    chips, groups, shares,
    rows_ref, own_ref, part_ref, gain_hbm, context_ref, half_ref, gate_hbm, up_hbm, down_hbm,
    assigned, grad_out, far_context, far_normed,
    up_all, normed_ref, gate_value, up_value, gate_grad, up_grad, pulled_ref,
    gain_ref, gate_ref, up_ref, down_ref, load_sems, wide_sems, far_sems, core_sems, local_sems, *rest,
):
    length, breadth = rows_ref.shape
    hidden = gate_ref.shape[1]
    block = next(b for b in (1024, 512, 256, 128, hidden) if hidden % b == 0)
    spans = [slice(at, at + block) for at in range(0, hidden, block)]

    def loads(i, which):
        source, target = ((gate_hbm, gate_ref), (up_hbm, up_ref), (down_hbm, down_ref))[which]
        at = (spans[i], slice(None)) if which == 2 else (slice(None), spans[i])
        return pltpu.make_async_copy(source.at[at], target.at[at], load_sems.at[which, i])

    gain_load = pltpu.make_async_copy(gain_hbm, gain_ref, load_sems.at[3, 0])
    gain_load.start()
    for which in range(3):
        for i in range(len(spans)):
            loads(i, which).start()
    group = lax.axis_index("sdata")
    chip, core = place()
    sibling = {"tensor": chip * CORES + 1 - core}
    greet(partners(chips, lax.axis_size("client"), groups))
    widen = Widen(up_all, [wide_sems.at[i] for i in range(4)], chips)
    count = own_ref.shape[0]
    share = count // groups
    missing = [
        (turned(group, d, groups) * share + i, slice(None))
        for d in range(1, groups)
        for i in range(share)
    ]
    for n, piece in enumerate(missing):
        widen.start(own_ref.at[piece[0]], n, piece)
    others = [
        send(context_ref, far_context, far_sems.at[0], far_sems.at[1], {"sdata": 1 - group})
    ]
    kept = []
    for n in range(shares):
        d = CORES * n + core
        others.append(
            send(half_ref.at[n], far_normed.at[d], core_sems.at[0, n], core_sems.at[1, n], sibling)
        )
        kept.append(pltpu.make_async_copy(half_ref.at[n], far_normed.at[d], local_sems.at[n]))
        kept[-1].start()
    rows_float = rows_ref[...].astype(F32)
    gain_load.wait()
    gain = gain_ref[...].astype(F32)
    inv_rms = lax.rsqrt(jnp.mean(rows_float * rows_float, -1, keepdims=True) + 1e-05)
    normed_ref[...] = (rows_float * inv_rms * gain).astype(BF16)
    for i, span in enumerate(spans):
        loads(i, 0).wait()
        gate_value[:, span] = jnp.dot(normed_ref[...], gate_ref[:, span], preferred_element_type=F32)
        loads(i, 1).wait()
        up_value[:, span] = jnp.dot(normed_ref[...], up_ref[:, span], preferred_element_type=F32)
    for i in range(share):
        up_all[group * share + i] = part_ref[group * share + i]
    for n, piece in enumerate(missing):
        widen.forward(n, piece)
    widen.finish()
    upstream = up_all[...].reshape(length, breadth)
    lean = jnp.zeros((length, 1), F32)
    for i, span in enumerate(spans):
        loads(i, 2).wait()
        pulled = lax.dot_general(upstream, down_ref[span], CROSSED, preferred_element_type=F32)
        gate, up = gate_value[:, span], up_value[:, span]
        sigmoid_gate = jax.nn.sigmoid(gate)
        gate_part = (
            pulled * up * sigmoid_gate * (1.0 + gate * (1.0 - sigmoid_gate))
        ).astype(BF16)
        up_part = (pulled * gate * sigmoid_gate).astype(BF16)
        gate_grad[:, span], up_grad[:, span] = gate_part, up_part
        lean = lean + jnp.sum(
            gate_part.astype(F32) * gate + up_part.astype(F32) * up, -1, keepdims=True
        )
    lean = inv_rms**2 * (lean * (1.0 / breadth))
    width = own_ref.shape[2]
    chunk = own_ref.shape[1]
    step = min(256, width)

    def pull(to, side):
        for at in range(0, width, step):
            span = pl.ds(pl.multiple_of((to * CORES + side) * width + at, step), step)
            weighted = (
                lax.dot_general(gate_grad[...], gate_ref[span, :], CROSSED, preferred_element_type=F32)
                + lax.dot_general(up_grad[...], up_ref[span, :], CROSSED, preferred_element_type=F32)
            ) * gain_ref[:, span].astype(F32)
            mine = inv_rms * weighted - rows_ref[:, span].astype(F32) * lean
            pulled_ref[:, :, span] = mine.reshape(count, chunk, step).astype(BF16)

    back_kernel(
        chips, lax.axis_size("client"), groups, pull, assigned, pulled_ref, own_ref, grad_out, *rest
    )
    for copy in others:
        copy.wait_recv()
    for copy in others:
        copy.wait_send()
    for copy in kept:
        copy.wait()


def serve(assigned, rows_in, up_own, up_part, gain, context, half, gate_matrix, up_matrix, down_matrix):
    chips, count, groups = axis_counts()
    length, breadth = rows_in.shape
    hidden = gate_matrix.shape[1]
    shares = half.shape[0] if half.ndim == 3 else 0
    far = (count,) + half.shape[1:] if shares else half.shape
    chunk, width = length // count, breadth // (CORES * chips)
    share, parts = count // groups, len(parts_of(chunk))
    full, own = (count, chunk, breadth), (count, chunk, width)
    dma = pltpu.SemaphoreType.DMA
    vmem = lambda *sizes: pltpu.VMEM(sizes, BF16)
    wide = lambda *sizes: pltpu.VMEM(sizes, F32)
    return pl.pallas_call(
        partial(server_kernel, chips, groups, shares),
        out_shape=(
            jax.ShapeDtypeStruct(full, BF16),
            jax.ShapeDtypeStruct(context.shape, BF16),
            jax.ShapeDtypeStruct(far, BF16),
        ),
        in_specs=[VMEM_SPEC] * 3 + [HBM_SPEC] + [VMEM_SPEC] * 2 + [HBM_SPEC] * 3 + [SMEM_SPEC],
        out_specs=(VMEM_SPEC,) * 3,
        scratch_shapes=[
            vmem(*full), vmem(length, breadth),
            wide(length, hidden), wide(length, hidden), vmem(length, hidden), vmem(length, hidden),
            vmem(*full),
            vmem(1, breadth), vmem(breadth, hidden), vmem(breadth, hidden), vmem(hidden, breadth),
            dma((4, hidden // LANES)), dma((4, chips, count)), dma((2,)), dma((2, count)),
            dma((count,)),
            vmem(chips, *own), vmem(chips, *own), vmem(chips, *own),
            vmem(groups, share, chunk, width), vmem(*own), vmem(*own),
            dma((4, chips, parts * count)), dma((2, parts, groups, share)),
            dma((2, parts, count)), dma((4, chips, parts * count)),
        ]
        + [vmem(count, chunk // parts, width)] * parts,
        compiler_params=params(5, 50),
        name="serve",
    )(
        rows_in, up_own, up_part, gain[None], context, half, gate_matrix, up_matrix, down_matrix,
        assigned,
    )


class Chain:
    def __init__(self, own, forth, back, sems, count):
        self.own, self.forth, self.back, self.count = own, forth, back, count
        self.sems = sems
        self.at = lax.axis_index("client")

    def copy(self, way, j, d):
        landing = self.forth if way == 0 else self.back
        to = self.at + 1 if way == 0 else self.at - 1
        return pltpu.make_async_remote_copy(
            src_ref=self.own.at[d],
            dst_ref=landing.at[j],
            send_sem=self.sems.at[2 * way, j],
            recv_sem=self.sems.at[2 * way + 1, j],
            device_id={"client": lax.rem(to + self.count, self.count)},
            device_id_type=MESH,
        )

    def legs(self):
        for j in range(self.count - 1):
            for way in (0, 1):
                d = self.count - 1 - j if way == 0 else j
                end = 0 if way == 0 else self.count - 1
                beyond = self.at < d if way == 0 else self.at > d
                yield way, j, d, end, beyond

    def open(self, d, way):
        j = self.count - 1 - d if way == 0 else d
        end = 0 if way == 0 else self.count - 1
        if abs(d - end) > 1:

            @pl.when(self.at == end)
            def _():
                self.copy(way, j, d).start()

    def add(self, way, j, d):
        landing = self.forth if way == 0 else self.back
        self.copy(way, j, d).wait_recv()
        self.own[d] = (self.own[d].astype(F32) + landing[j].astype(F32)).astype(BF16)

    def relay(self):
        near = self.at < self.count // 2
        legs = list(self.legs())
        turns = [(leg, near) for leg in legs if leg[0] == 0]
        turns += [(leg, self.at >= 0) for leg in legs if leg[0] == 1]
        turns += [(leg, jnp.logical_not(near)) for leg in legs if leg[0] == 0]
        for (way, j, d, end, beyond), now in turns:
            if abs(d - end) < 3:
                continue
            far = self.at < d - 1 if way == 0 else self.at > d + 1

            @pl.when(now & far & (self.at != end))
            def _(way=way, j=j, d=d):
                self.add(way, j, d)
                self.copy(way, j, d).start()

    def close(self, ends):
        last = self.count - 1
        for way, end, d in ((0, 0, self.at + 1), (1, last, self.at - 1)):
            j = last - d if way == 0 else d
            if ends:

                @pl.when(self.at == end)
                def _(way=way, j=j, d=d):
                    self.copy(way, j, d).start()

            else:

                @pl.when((self.at > 0) & (self.at < last))
                def _(way=way, j=j, d=d):
                    self.add(way, j, d)
                    self.copy(way, j, d).start()

    def total(self, out_refs):
        last = self.count - 1
        for way, end, j in ((0, 0, last - self.at), (1, last, self.at)):
            landing = self.forth if way == 0 else self.back

            @pl.when(self.at != end)
            def _(way=way, j=j, landing=landing):
                self.copy(way, j, 0).wait_recv()
                self.own[self.at] = (
                    self.own[self.at].astype(F32) + landing[j].astype(F32)
                ).astype(BF16)

        result = (self.own[self.at].astype(F32) * (1.0 / self.count)).astype(BF16)
        at = 0
        for out in out_refs:
            out[...] = result[:, at : at + out.shape[1]]
            at += out.shape[1]

    def finish(self):
        for way, j, d, end, beyond in self.legs():

            @pl.when(beyond)
            def _(way=way, j=j, d=d):
                self.copy(way, j, d).wait_send()


def learn_kernel(
    kv_count, count, aligned,
    cut_ref, output_ref, query_ref, key_ref, value_ref, context_ref, weights_ref, normed_ref,
    far_normed, far_context, table_ref, *refs,
):
    if not aligned:
        near_cut, give_cut, near_normed, refs = refs[0], refs[1], refs[2], refs[3:]
    query_out, key_out, value_out, output_out = refs[:4]
    (
        pulled, pair, key_turn, value_pair, weight_grad, score_grad, query_grad, shared_grad,
        far_cut, far_query, far_shared,
        output_own, output_forth, output_back, shared_own, shared_forth, shared_back,
        query_own, query_forth, query_back,
        cosine_ref, sine_ref,
        cut_sems, core_sems, give_sems, output_sems, shared_sems, query_sems,
    ) = refs[4:]
    length = cut_ref.shape[0]
    rows = far_cut.shape[2]
    client, group = lax.axis_index("client"), lax.axis_index("sdata")
    tensor_at = lax.axis_index("tensor")
    core = lax.rem(tensor_at, CORES)
    sibling = {"tensor": tensor_at + 1 - 2 * core}
    across = {"sdata": 1 - group}
    ahead = {"client": lax.rem(client + 1, count)}
    behind = {"client": lax.rem(client + count - 1, count)}
    greet([sibling, across, ahead, behind])
    order = []
    for j in range((count + 1) // 2):
        order += [count - 1 - j, j]

    def columns(d, side):
        return pl.ds(pl.multiple_of((2 * d + side) * rows, rows), rows)

    def cut_copy(n, d):
        source = cut_ref.at[:, columns(d, 1 - group)] if aligned else give_cut.at[d]
        return pltpu.make_async_remote_copy(
            src_ref=source, dst_ref=far_cut.at[d],
            send_sem=cut_sems.at[0, n], recv_sem=cut_sems.at[1, n],
            device_id=across, device_id_type=MESH,
        )

    def core_copy(n, d):
        return pltpu.make_async_remote_copy(
            src_ref=far_cut.at[d], dst_ref=far_cut.at[d],
            send_sem=core_sems.at[0, n], recv_sem=core_sems.at[1, n],
            device_id=sibling, device_id_type=MESH,
        )

    halves = count // CORES
    picks = [order[CORES * n] + core * (order[CORES * n + 1] - order[CORES * n]) for n in range(halves)]
    others = [
        order[CORES * n + 1] + core * (order[CORES * n] - order[CORES * n + 1]) for n in range(halves)
    ]
    for n in range(halves):
        cut_copy(n, picks[n]).start()

    width = 2 * LANES if query_ref.shape[1] % (2 * LANES) == 0 else LANES
    for at in range(0, query_ref.shape[1], width):
        pulled[:, at : at + width] = jnp.dot(
            cut_ref[...], output_ref[:, at : at + width], preferred_element_type=F32
        ).astype(BF16)
    keys_float, values_float = key_ref[...].astype(F32), value_ref[...].astype(F32)
    keys_turned = keys_float.T.astype(BF16)
    key_turn[...] = jnp.zeros_like(key_turn)
    score_grad[...] = jnp.zeros_like(score_grad)
    for g in range(kv_count):
        value_pair[g, :length], value_pair[g, length:] = paired(values_float, g)
        mine = keys_turned[g * HEAD_DIM : (g + 1) * HEAD_DIM]
        key_turn[g, :HEAD_DIM, :length] = mine
        key_turn[g, HEAD_DIM:, length:] = mine

    unfold(table_ref[...], cosine_ref, sine_ref)

    def unturn(tile):
        return tile * cosine_ref[...] - swap_halves(tile) * sine_ref[...]

    tiles = query_ref.shape[1] // LANES
    low = lane_tile() < HEAD_DIM
    key_sum, value_sum = [None] * kv_count, [None] * kv_count
    for t in range(tiles):
        g = t * kv_count // tiles
        span = slice(t * LANES, (t + 1) * LANES)
        weight_grad[t % 2] = lax.dot_general(
            value_pair[g], pulled[:, span], CROSSED, preferred_element_type=F32
        )
        for head in range(2):
            base = head * length
            for i in range(0, length, LANES):
                deep = i + LANES
                grad = weight_grad[t % 2, base : base + deep, i : i + LANES].astype(BF16).astype(F32)
                weight = weights_ref[t, base : base + deep, i : i + LANES].astype(F32)
                both = grad * weight
                drift = jnp.sum(both, 0, keepdims=True)
                score_grad[t % 2, base : base + deep, i : i + LANES] = (
                    (both - weight * drift) * HEAD_DIM ** (-0.5)
                ).astype(BF16)
        back_query = jnp.dot(key_turn[g], score_grad[t % 2], preferred_element_type=F32)
        query_grad[:, span] = unturn(back_query.T.astype(BF16).astype(F32)).astype(BF16)
        back_key = jnp.dot(score_grad[t % 2], query_ref[:, span], preferred_element_type=F32)
        back_value = jnp.dot(weights_ref[t], pulled[:, span], preferred_element_type=F32)
        first = key_sum[g] is None
        key_sum[g] = back_key if first else key_sum[g] + back_key
        value_sum[g] = back_value if first else value_sum[g] + back_value

    def folded(sums):
        whole = None
        for g, both in enumerate(sums):
            upper, lower = both[:length], both[length:]
            if g == 0:
                whole = upper + pltpu.roll(lower, HEAD_DIM, 1)
            else:
                whole = jnp.where(low, whole, pltpu.roll(upper, HEAD_DIM, 1) + lower)
        return whole.astype(BF16)

    shared_grad[:, :LANES] = unturn(folded(key_sum).astype(F32)).astype(BF16)
    shared_grad[:, LANES:] = folded(value_sum)

    def give(source, target, i):
        return pltpu.make_async_remote_copy(
            src_ref=source, dst_ref=target, send_sem=give_sems.at[0, i], recv_sem=give_sems.at[1, i],
            device_id=across, device_id_type=MESH,
        )

    gifts = [give(shared_grad, far_shared, 0), give(query_grad, far_query, 1)]
    for gift in gifts:
        gift.start()
    chains = [
        Chain(output_own, output_forth, output_back, output_sems, count),
        Chain(shared_own, shared_forth, shared_back, shared_sems, count),
        Chain(query_own, query_forth, query_back, query_sems, count),
    ]

    def near(d, from_cut):
        if aligned:
            return (cut_ref if from_cut else normed_ref)[:, columns(d, group)]
        return near_cut[d] if from_cut else near_normed[d]

    def product(chain, d, left, right, far_left, far_right):
        chain.own[d] = (
            lax.dot_general(left, right, TALL, preferred_element_type=F32)
            + lax.dot_general(far_left, far_right, TALL, preferred_element_type=F32)
        ).astype(BF16)

    for n in range(halves):
        cut_copy(n, picks[n]).wait_recv()
        core_copy(n, picks[n]).start()
        core_copy(n, others[n]).wait_recv()
        for i in range(CORES):
            d = order[CORES * n + i]
            product(chains[0], d, near(d, True), context_ref[...], far_cut[d], far_context[...])
            for way in (0, 1):
                chains[0].open(d, way)

    def spread(chain, grad, far_grad):
        for d in order:
            product(chain, d, near(d, False), grad[...], far_normed[d], far_grad[...])
            for way in (0, 1):
                chain.open(d, way)

    gifts[0].wait_recv()
    spread(chains[1], shared_grad, far_shared)
    chains[0].relay()
    gifts[1].wait_recv()
    spread(chains[2], query_grad, far_query)
    for chain in chains:
        chain.close(True)
    chains[0].close(False)
    for chain in chains[1:]:
        chain.relay()
        chain.close(False)
    chains[0].total([output_out])
    chains[1].total([key_out, value_out])
    chains[2].total([query_out])
    for n in range(halves):
        cut_copy(n, picks[n]).wait_send()
        core_copy(n, picks[n]).wait_send()
    for gift in gifts:
        gift.wait_send()
    for chain in chains:
        chain.finish()


def learn(cut_grad, output_matrix, saved, normed, far_normed, far_context, table, kv_count):
    unused, count, group_count = axis_counts()
    queries, keys, values, context, weights = saved
    length, breadth = cut_grad.shape
    features = queries.shape[1]
    rows = breadth // (count * group_count)
    aligned = rows % LANES == 0
    dma = pltpu.SemaphoreType.DMA
    shape = lambda *sizes: jax.ShapeDtypeStruct(sizes, BF16)
    vmem = lambda *sizes: pltpu.VMEM(sizes, BF16)
    operands = [cut_grad, output_matrix, queries, keys, values, context, weights, normed]
    operands += [far_normed, far_context, table]
    if not aligned:
        group = lax.axis_index("sdata")
        operands += [
            half_of(cut_grad, count, group), half_of(cut_grad, count, 1 - group),
            half_of(normed, count, group),
        ]
    chain = lambda wide: [
        vmem(count, rows, wide), vmem(count - 1, rows, wide), vmem(count - 1, rows, wide)
    ]
    return pl.pallas_call(
        partial(learn_kernel, kv_count, count, aligned),
        out_shape=(
            shape(rows, features), shape(rows, LANES), shape(rows, LANES), shape(rows, features)
        ),
        in_specs=[VMEM_SPEC] * len(operands),
        out_specs=(VMEM_SPEC,) * 4,
        scratch_shapes=[
            vmem(length, features), vmem(16, LANES), vmem(kv_count, LANES, 2 * length),
            vmem(kv_count, 2 * length, LANES), pltpu.VMEM((2, 2 * length, length), F32),
            vmem(2, 2 * length, length), vmem(length, features), vmem(length, 2 * LANES),
            vmem(count, length, rows), vmem(length, features), vmem(length, 2 * LANES),
        ]
        + chain(features) + chain(2 * LANES) + chain(features)
        + [pltpu.VMEM(table.shape, F32)] * 2
        + [dma((2, count // CORES)), dma((2, count // CORES)), dma((2, 2))]
        + [dma((4, count - 1))] * 3,
        compiler_params=params(3, 28),
        name="learn",
    )(*operands)


def emit_kernel(count, *refs):
    sems = refs[2 * count]
    copies = [
        pltpu.make_async_copy(refs[i], refs[count + i], sems.at[i]) for i in range(count)
    ]
    for copy in copies:
        copy.start()
    for copy in copies:
        copy.wait()


def emit(*arrays):
    count = len(arrays)
    return pl.pallas_call(
        partial(emit_kernel, count),
        out_shape=tuple(jax.ShapeDtypeStruct(a.shape, a.dtype) for a in arrays),
        in_specs=[VMEM_SPEC] * count,
        out_specs=(HBM_SPEC,) * count,
        scratch_shapes=[pltpu.SemaphoreType.DMA((count,))],
        compiler_params=pltpu.CompilerParams(vmem_limit_bytes=4 * 2**20),
        name="emit",
    )(*arrays)


def half_of(array, count, side):
    blocks = array.reshape(array.shape[0], count, 2, -1)
    return lax.dynamic_index_in_dim(blocks, side, 2, False).transpose(1, 0, 2)


def across_groups(array):
    count = lax.axis_size("sdata")
    return lax.ppermute(array, "sdata", [(g, (g + 1) % count) for g in range(count)])


def table_of(length):
    halfway = HEAD_DIM // 2
    lanes = np.arange(HEAD_DIM)
    frequencies = np.exp(-math.log(500000.0) * (2.0 / HEAD_DIM) * (lanes % halfway))
    angles = np.arange(length)[:, None] * frequencies[None, :]
    sign = np.where(lanes < halfway, -1.0, 1.0)
    return jnp.asarray(np.concatenate([np.cos(angles), np.sin(angles) * sign], 1), F32)


def widened(matrix):
    return jnp.pad(matrix, ((0, 0), (0, LANES - matrix.shape[1])))


def local(
    client_input,
    client_gain,
    query_weight,
    key_weight,
    client_value_weight,
    output_weight,
    server_gain,
    server_gate,
    server_up,
    server_down,
    upstream,
    assignment,
):
    client_count = lax.axis_size("client")
    shared = key_weight.shape[2]
    kv_count = shared // HEAD_DIM
    table = table_of(client_input.shape[0])
    matrices = [
        query_weight[0], widened(key_weight[0]), widened(client_value_weight[0]), output_weight[0]
    ]
    normed, half, *saved, cut_rows, up_own, up_part = depart(
        assignment, client_input, client_gain, table, upstream, matrices, kv_count
    )
    cut_rows = cut_rows.reshape(client_input.shape)
    arriving_grad, far_context, far_normed = serve(
        assignment, cut_rows, up_own, up_part, server_gain[0], saved[3], half,
        server_gate[0], server_up[0], server_down[0],
    )
    arriving_grad = arriving_grad.reshape(client_input.shape)
    if half.ndim == 2:
        far_normed = across_groups(half_of(normed, client_count, 1 - lax.axis_index("sdata")))
    query_update, key_update, value_update, output_update = emit(
        *learn(
            arriving_grad, output_weight[0], saved, normed, far_normed, far_context, table,
            kv_count,
        )
    )
    return (query_update, key_update[:, :shared], value_update[:, :shared], output_update)


def solution(mesh):
    placed = (
        P(("client", "sdata"), None),
        P("client", None),
        P("client", None, "tensor"),
        P("client", None, "tensor"),
        P("client", None, "tensor"),
        P("client", None, "tensor"),
        P("sdata", None),
        P("sdata", None, "tensor"),
        P("sdata", None, "tensor"),
        P("sdata", "tensor", None),
        P(("client", "sdata"), None),
        P(),
    )
    return jax.shard_map(
        local,
        mesh=mesh,
        in_specs=placed,
        out_specs=(
            P(("client", "sdata"), "tensor"),
            P(("client", "sdata"), "tensor"),
            P(("client", "sdata"), "tensor"),
            P(("client", "sdata"), "tensor"),
        ),
        check_vma=False,
    )
```
